32 devices in a mesh: dp: 2 (over x), cpo: 4 (over z), cpi: 4 (over y, core).
Axes of the slice: x: 2, y: 2, z: 4, core: 2. Of those that a mesh axis runs over, the one named last changes fastest.
Arguments:
- hidden: bfloat16 [6144, 2560], P(('dp', 'cpo', 'cpi')), parts along dimension 0
- w_q: bfloat16 [2560, 8, 256], replicated
- w_k: bfloat16 [2560, 4, 256], replicated
- w_v: bfloat16 [2560, 4, 256], replicated
- w_o: bfloat16 [8, 256, 2560], replicated
Outputs:
- output: bfloat16 [6144, 2560], P(('dp', 'cpo', 'cpi')), parts along dimension 0
There are 2 independent parts. The reference program is written for one: setup_inputs(seed, part) draws one part's arguments, and reference() takes and returns one part's arrays. A program takes and returns all parts, laid end to end along the dimension named above; an argument that names none is the same for every part.
All inputs are finite; a program needn't handle non-finite values.
Results may differ from the reference program's by a relative error of at most 0.00476169.
Values are sent between devices in bfloat16 or wider.
A program may use at most 1 GiB of HBM per device.

```python
import jax
import jax.numpy as jnp
from jax import lax

D_MODEL = 2560
HEADS_Q = 8
HEADS_KV = 4
HEAD_DIM = 256
TOK_DEV = 192
CHUNKS = 16
WINDOW = 2048
QUERY_BLOCK = 128
SEQ_LEN = CHUNKS * TOK_DEV
GROUP_SIZE = HEADS_Q // HEADS_KV
KEY_SPAN = WINDOW + QUERY_BLOCK
ROPE_BASE = 10000.0


def setup_inputs(seed: int = 0, part: int = 0) -> dict:
    root_part, root_shared = jax.random.split(jax.random.key(seed))
    key_noise, key_shift = jax.random.split(jax.random.fold_in(root_part, part))
    key_q, key_k, key_v, key_o = jax.random.split(root_shared, 4)
    noise = jax.random.normal(key_noise, (CHUNKS, TOK_DEV, D_MODEL), jnp.float32)
    shifts = jax.random.normal(key_shift, (CHUNKS, 1, D_MODEL), jnp.float32)
    hidden = (0.8 * noise + 0.8 * shifts).reshape(SEQ_LEN, D_MODEL).astype(jnp.bfloat16)
    scale_in = D_MODEL ** -0.5
    scale_out = (HEADS_Q * HEAD_DIM) ** -0.5
    w_q = (jax.random.normal(key_q, (D_MODEL, HEADS_Q, HEAD_DIM), jnp.float32) * scale_in).astype(jnp.bfloat16)
    w_k = (jax.random.normal(key_k, (D_MODEL, HEADS_KV, HEAD_DIM), jnp.float32) * scale_in).astype(jnp.bfloat16)
    w_v = (jax.random.normal(key_v, (D_MODEL, HEADS_KV, HEAD_DIM), jnp.float32) * scale_in).astype(jnp.bfloat16)
    w_o = (jax.random.normal(key_o, (HEADS_Q, HEAD_DIM, D_MODEL), jnp.float32) * scale_out).astype(jnp.bfloat16)
    return {'hidden': hidden, 'w_q': w_q, 'w_k': w_k, 'w_v': w_v, 'w_o': w_o}


def rope_rotate(vals, positions):
    half_dim = HEAD_DIM // 2
    inv_freq = ROPE_BASE ** (-jnp.arange(half_dim, dtype=jnp.float32) * 2.0 / HEAD_DIM)
    angles = positions.astype(jnp.float32)[..., None] * inv_freq
    cos_t = jnp.cos(angles)[..., None, :]
    sin_t = jnp.sin(angles)[..., None, :]
    lower_half = vals[..., :half_dim]
    upper_half = vals[..., half_dim:]
    return jnp.concatenate([lower_half * cos_t - upper_half * sin_t, upper_half * cos_t + lower_half * sin_t], axis=-1)


def reference(hidden, w_q, w_k, w_v, w_o):
    positions = jnp.arange(SEQ_LEN)
    q_proj = jnp.dot(hidden, w_q.reshape(D_MODEL, HEADS_Q * HEAD_DIM), preferred_element_type=jnp.float32)
    k_proj = jnp.dot(hidden, w_k.reshape(D_MODEL, HEADS_KV * HEAD_DIM), preferred_element_type=jnp.float32)
    v_proj = jnp.dot(hidden, w_v.reshape(D_MODEL, HEADS_KV * HEAD_DIM), preferred_element_type=jnp.float32)
    q_rot = rope_rotate(q_proj.reshape(SEQ_LEN, HEADS_Q, HEAD_DIM), positions).astype(jnp.bfloat16)
    k_rot = rope_rotate(k_proj.reshape(SEQ_LEN, HEADS_KV, HEAD_DIM), positions).astype(jnp.bfloat16)
    v_val = v_proj.reshape(SEQ_LEN, HEADS_KV, HEAD_DIM).astype(jnp.bfloat16)
    k_pad = jnp.concatenate([jnp.zeros((WINDOW, HEADS_KV, HEAD_DIM), jnp.bfloat16), k_rot], axis=0)
    v_pad = jnp.concatenate([jnp.zeros((WINDOW, HEADS_KV, HEAD_DIM), jnp.bfloat16), v_val], axis=0)
    score_scale = HEAD_DIM ** -0.5
    q_offsets = jnp.arange(QUERY_BLOCK)
    k_offsets = jnp.arange(KEY_SPAN)

    def attend_block(block_idx):
        q_start = block_idx * QUERY_BLOCK
        q_blk = lax.dynamic_slice_in_dim(q_rot, q_start, QUERY_BLOCK, 0).reshape(QUERY_BLOCK, HEADS_KV, GROUP_SIZE, HEAD_DIM)
        k_blk = lax.dynamic_slice_in_dim(k_pad, q_start, KEY_SPAN, 0)
        v_blk = lax.dynamic_slice_in_dim(v_pad, q_start, KEY_SPAN, 0)
        scores = jnp.einsum('tkgd,skd->kgts', q_blk.astype(jnp.float32), k_blk.astype(jnp.float32)) * score_scale
        pos_gap = q_offsets[:, None] + WINDOW - k_offsets[None, :]
        key_pos = q_start - WINDOW + k_offsets
        allowed = (pos_gap >= 0) & (pos_gap < WINDOW) & (key_pos[None, :] >= 0)
        scores = jnp.where(allowed, scores, -jnp.inf)
        row_max = jnp.max(scores, axis=-1, keepdims=True)
        exp_scores = jnp.exp(scores - row_max)
        exp_total = jnp.sum(exp_scores, axis=-1)
        weighted = jnp.einsum('kgts,skd->kgtd', exp_scores.astype(jnp.bfloat16).astype(jnp.float32), v_blk.astype(jnp.float32))
        return (weighted / exp_total[..., None]).astype(jnp.bfloat16)

    attended = lax.map(attend_block, jnp.arange(SEQ_LEN // QUERY_BLOCK))
    attended = jnp.transpose(attended, (0, 3, 1, 2, 4)).reshape(SEQ_LEN, HEADS_Q * HEAD_DIM)
    out_proj = jnp.dot(attended, w_o.reshape(HEADS_Q * HEAD_DIM, D_MODEL), preferred_element_type=jnp.float32)
    return out_proj.astype(jnp.bfloat16)
```

```python
import functools

import jax
import jax.numpy as jnp
from jax import lax
from jax.experimental import pallas as pl
from jax.experimental.pallas import tpu as pltpu
from jax.sharding import PartitionSpec as P

WINDOW = 2048
ROPE_BASE = 10000.0
MESH = pl.DeviceIdType.MESH
NL = 4
TOK = 192
LVL = NL * TOK
HD = 256
ROWS = 2 * TOK
CHUNK = 256
NEG = -1e30
LOG2E = 1.4426950408889634


def rope(vals, pos):
    half = vals.shape[-1] // 2
    inv_freq = ROPE_BASE ** (-jnp.arange(half, dtype=jnp.float32) * 2.0 / vals.shape[-1])
    ang = pos.astype(jnp.float32)[:, None] * inv_freq
    c, s = jnp.cos(ang)[None], jnp.sin(ang)[None]
    lo, hi = vals[..., :half], vals[..., half:]
    return jnp.concatenate([lo * c - hi * s, hi * c + lo * s], axis=-1).astype(jnp.bfloat16)


def body(q_ref, k_ref, v_ref, wo_hbm, y_ref, kb, vb, qb, ob, osend, acc, m_s, l_s, wo,
         krecv, vrecv, kfs, vfs, ksend, vsend, qsend, qrecv, os_sem, orecv, wsem):
    d, a, b = lax.axis_index("dp"), lax.axis_index("cpo"), lax.axis_index("cpi")
    shard = a * NL + b

    wcopy = pltpu.make_async_copy(wo_hbm, wo, wsem)
    wcopy.start()

    bar = pltpu.get_barrier_semaphore()
    for step in range(1, NL):
        pl.semaphore_signal(bar, inc=1, device_id=(d, a, lax.rem(b + step, NL)), device_id_type=MESH)

    @pl.when(a > 0)
    def _():
        pl.semaphore_signal(bar, inc=1, device_id=(d, a - 1, b), device_id_type=MESH)

    @pl.when(a < NL - 1)
    def _():
        pl.semaphore_signal(bar, inc=1, device_id=(d, a + 1, b), device_id_type=MESH)

    ends = (a == 0).astype(jnp.int32) + (a == NL - 1).astype(jnp.int32)
    pl.semaphore_wait(bar, NL + 1 - ends)

    def rows(s):
        return pl.ds(pl.multiple_of(s * TOK, TOK), TOK)

    def remote(src, dst, ss, rs, dev):
        return pltpu.make_async_remote_copy(src_ref=src, dst_ref=dst, send_sem=ss, recv_sem=rs,
                                            device_id=dev, device_id_type=MESH)

    def exchange(h, what):
        dev = (d, a, h)
        if what == "k":
            return remote(k_ref.at[h], kb.at[rows(shard)], ksend.at[h], krecv.at[shard], dev)
        if what == "v":
            return remote(v_ref.at[h], vb.at[rows(shard)], vsend.at[h], vrecv.at[shard], dev)
        return remote(q_ref.at[h], qb.at[b], qsend.at[h], qrecv.at[b], dev)

    for what in ("k", "v", "q"):
        for h in range(NL):
            @pl.when(b != h)
            def _():
                exchange(h, what).start()

    kb[rows(shard), :] = k_ref[b]
    vb[rows(shard), :] = v_ref[b]
    qb[b] = q_ref[b]

    def forward(s):
        dev = (d, a + 1, b)
        return (remote(kb.at[rows(s)], kb.at[rows(s)], kfs.at[s], krecv.at[s], dev),
                remote(vb.at[rows(s)], vb.at[rows(s)], vfs.at[s], vrecv.at[s], dev))

    def wait_piece(s):
        forwarded = forward(s)
        forwarded[0].wait_recv()
        forwarded[1].wait_recv()

    def needed(s, level):
        return s >= NL * level - 11

    def pass_on(s):
        @pl.when((a < NL - 1) & needed(s, a + 1))
        def _():
            for c in forward(s):
                c.start()

    pass_on(shard)
    partner = b + 1 - 2 * lax.rem(b, 2)
    far = lax.rem(b + 2, NL)
    far2 = lax.rem(partner + 2, NL)
    for j in (partner, far, far2):
        s = a * NL + j
        wait_piece(s)
        pass_on(s)

    for j in (partner, far, far2):
        remote(q_ref.at[0], qb.at[j], qsend.at[0], qrecv.at[j], (d, a, b)).wait_recv()

    def attend(i, key0, masked, first):
        q = qb[i].reshape(ROWS, HD)
        keys = pl.ds(pl.multiple_of(key0, CHUNK), CHUNK)
        s = lax.dot_general(q, kb[keys, :], (((1,), (1,)), ((), ())), preferred_element_type=jnp.float32)
        if masked:
            row = lax.broadcasted_iota(jnp.int32, (2, TOK, CHUNK), 1).reshape(ROWS, CHUNK)
            col = lax.broadcasted_iota(jnp.int32, (ROWS, CHUNK), 1)
            gap = row - col + (a * LVL + i * TOK - key0)
            s = jnp.where((gap >= 0) & (gap < WINDOW), s, NEG)
        top = jnp.max(s, axis=-1, keepdims=True)
        old = m_s[i]
        new = jnp.maximum(old, top)
        scale = HD ** -0.5 * LOG2E
        p = jnp.exp2((s - new) * scale)
        fix = jnp.exp2((old - new) * scale)
        l_s[i] = l_s[i] * fix + jnp.sum(p, axis=-1, keepdims=True)
        acc[i] = acc[i] * fix + jnp.dot(p.astype(jnp.bfloat16), vb[keys, :], preferred_element_type=jnp.float32)
        m_s[i] = new

    m_s[...] = jnp.full_like(m_s, NEG)
    l_s[...] = jnp.zeros_like(l_s)
    acc[...] = jnp.zeros_like(acc)

    def own(i, carry):
        n = lax.div(i * TOK + TOK + CHUNK - 1, CHUNK)

        def one(c, carry):
            attend(i, a * LVL + c * CHUNK, True, False)
            return carry

        return lax.fori_loop(0, n, one, carry)

    lax.fori_loop(0, NL, own, 0)

    for back in (1, 2, 3):
        @pl.when(a >= back)
        def _():
            base = (a - back) * NL
            for j in range(NL):
                @pl.when(needed(base + j, a))
                def _():
                    wait_piece(base + j)
                    pass_on(base + j)

            first = 1 if back == 3 else 0
            last = NL - 1 if back == 3 else NL

            def over(i, carry):
                def one(c, carry):
                    attend(i, base * TOK + c * CHUNK, back > 1, False)
                    return carry
                return lax.fori_loop(first, LVL // CHUNK, one, carry)

            lax.fori_loop(0, last, over, 0)

    def back_to(i):
        cols = pl.ds(pl.multiple_of(b * 2 * HD, 2 * HD), 2 * HD)
        return remote(osend.at[i], ob.at[:, cols], os_sem.at[i], orecv.at[b], (d, a, i))

    for i in range(NL):
        o = (acc[i] / l_s[i]).astype(jnp.bfloat16)
        osend[i] = jnp.concatenate([o[:TOK], o[TOK:]], axis=1)

        @pl.when(b != i)
        def _():
            back_to(i).start()

    for h in range(NL):
        cols = pl.ds(h * 2 * HD, 2 * HD)

        @pl.when(b == h)
        def _():
            ob[:, cols] = osend[h]

        @pl.when(b != h)
        def _():
            remote(osend.at[0], ob.at[:, cols], os_sem.at[0], orecv.at[h], (d, a, b)).wait_recv()

    wcopy.wait()
    y_ref[...] = jnp.dot(ob[...], wo[...], preferred_element_type=jnp.float32).astype(jnp.bfloat16)

    for i in range(NL):
        @pl.when(b != i)
        def _():
            back_to(i).wait_send()
            for what in ("k", "v", "q"):
                exchange(i, what).wait_send()

    for s in range(12):
        @pl.when((a < NL - 1) & (s < NL * (a + 1)) & needed(s, a + 1))
        def _():
            for c in forward(s):
                c.wait_send()


def solution(mesh):
    def local_fn(hidden, w_q, w_k, w_v, w_o):
        shard = lax.axis_index("cpo") * NL + lax.axis_index("cpi")
        pos = shard * TOK + jnp.arange(TOK)
        k = rope(jnp.einsum("td,dhe->hte", hidden, w_k, preferred_element_type=jnp.float32), pos)
        v = jnp.einsum("td,dhe->hte", hidden, w_v, preferred_element_type=jnp.float32).astype(jnp.bfloat16)
        q = rope(jnp.einsum("td,dhe->hte", hidden, w_q, preferred_element_type=jnp.float32), pos)
        q = q.reshape(NL, 2, TOK, HD)
        vm = pl.BlockSpec(memory_space=pltpu.VMEM)
        dma = pltpu.SemaphoreType.DMA
        bf, f32 = jnp.bfloat16, jnp.float32
        return pl.pallas_call(
            body,
            out_shape=jax.ShapeDtypeStruct((TOK, 2560), bf),
            in_specs=[vm, vm, vm, pl.BlockSpec(memory_space=pl.ANY)],
            out_specs=vm,
            scratch_shapes=[
                pltpu.VMEM((16 * TOK, HD), bf), pltpu.VMEM((16 * TOK, HD), bf),
                pltpu.VMEM((NL, 2, TOK, HD), bf), pltpu.VMEM((TOK, 8 * HD), bf),
                pltpu.VMEM((NL, TOK, 2 * HD), bf), pltpu.VMEM((NL, ROWS, HD), f32),
                pltpu.VMEM((NL, ROWS, 1), f32), pltpu.VMEM((NL, ROWS, 1), f32),
                pltpu.VMEM((8 * HD, 2560), bf),
                dma((16,)), dma((16,)), dma((16,)), dma((16,)),
                dma((NL,)), dma((NL,)), dma((NL,)), dma((NL,)), dma((NL,)), dma((NL,)), dma(()),
            ],
            compiler_params=pltpu.CompilerParams(collective_id=0, has_side_effects=True,
                                                 vmem_limit_bytes=50 * 2 ** 20),
        )(q, k, v, w_o.reshape(8 * HD, 2560))

    return jax.shard_map(local_fn, mesh=mesh,
                         in_specs=(P(("dp", "cpo", "cpi"), None), P(), P(), P(), P()),
                         out_specs=P(("dp", "cpo", "cpi"), None), check_vma=False)
```

```python
import jax
import jax.numpy as jnp
from jax import lax
from jax.experimental import pallas as pl
from jax.experimental.pallas import tpu as pltpu
from jax.sharding import PartitionSpec as P

WINDOW = 2048
ROPE_BASE = 10000.0
MESH = pl.DeviceIdType.MESH
NL = 4
TOK = 192
LVL = NL * TOK
DM = 2560
HD = 256
HALF = HD // 2
NEG = -1e30
SCALE = HD ** -0.5 * 1.4426950408889634
KCUT = 2
QCUT = 4
OWN_KEYS = (256, 384, 640, 768)
F32, BF = jnp.float32, jnp.bfloat16


def body(freq_ref, x_hbm, wq_hbm, wk_hbm, wv_hbm, wo_hbm, y_ref,
         x, wq, wk, wv, wo, ko, vo, qo, kb, vb, qb, ob, osend, acc, m_s, l_s,
         xsem, wksem, wvsem, wqsem, wosem, krecv, vrecv, kfs, vfs, ksend, vsend, qsend, qrecv,
         os_sem, orecv, go):
    d, a, b = lax.axis_index("dp"), lax.axis_index("cpo"), lax.axis_index("cpi")
    shard = a * NL + b
    odd = lax.rem(b, 2)
    even = odd == 0
    partner = b + 1 - 2 * odd
    far = lax.rem(b + 2, NL)
    far2 = lax.rem(partner + 2, NL)
    donor = (a == 3) & even
    host = (a == 2) & even
    feeds = (a < 2) | ((a == 2) & (odd == 1))

    def cut(src, dst, sem, n, c):
        r = DM // n
        return pltpu.make_async_copy(src.at[pl.ds(c * r, r)], dst.at[pl.ds(c * r, r)], sem.at[c])

    xcopy = pltpu.make_async_copy(x_hbm, x, xsem)
    xcopy.start()
    for c in range(KCUT):
        cut(wk_hbm, wk, wksem, KCUT, c).start()
    for c in range(KCUT):
        cut(wv_hbm, wv, wvsem, KCUT, c).start()

    bar = pltpu.get_barrier_semaphore()

    def greet(level, other):
        pl.semaphore_signal(bar, inc=1, device_id=(d, level, other), device_id_type=MESH)

    for j in (partner, far, far2):
        greet(a, j)

    @pl.when(a > 0)
    def _():
        greet(a - 1, b)

    @pl.when(a < NL - 1)
    def _():
        greet(a + 1, b)

    @pl.when(host)
    def _():
        for j in (partner, far, far2):
            greet(3, j)

    @pl.when(a == 3)
    def _():
        greet(2, lax.rem(b + 2 - odd, NL))

    @pl.when((a == 3) & (odd == 1))
    def _():
        greet(2, b - 1)

    def one(p):
        return p.astype(jnp.int32)

    pos = (lax.broadcasted_iota(jnp.int32, (TOK, HALF), 0) + shard * TOK).astype(F32)
    ang = pos * freq_ref[...]
    cos, sin = jnp.cos(ang), jnp.sin(ang)

    def project(w, n, copies, heads):
        total = None
        for c in range(n):
            copies[c].wait()
            r = DM // n
            part = jnp.dot(x[:, c * r:(c + 1) * r], w[pl.ds(c * r, r)].reshape(r, heads * HD),
                           preferred_element_type=F32)
            total = part if total is None else total + part
        return total

    def rotate(t, h):
        lo, hi = t[:, h * HD:h * HD + HALF], t[:, h * HD + HALF:(h + 1) * HD]
        return (lo * cos - hi * sin).astype(BF), (hi * cos + lo * sin).astype(BF)

    def rows(s):
        return pl.ds(pl.multiple_of(s * TOK, TOK), TOK)

    def remote(src, dst, ss, rs, dev):
        return pltpu.make_async_remote_copy(src_ref=src, dst_ref=dst, send_sem=ss, recv_sem=rs,
                                            device_id=dev, device_id_type=MESH)

    def holder(h):
        return jnp.minimum(a, 2) if h % 2 == 0 else a

    def mine(h):
        return (b == h) & (holder(h) == a)

    def exchange(h, what):
        dev = (d, holder(h), h)
        if what == "k":
            return remote(ko.at[h], kb.at[rows(shard)], ksend.at[h], krecv.at[shard], dev)
        if what == "v":
            return remote(vo.at[h], vb.at[rows(shard)], vsend.at[h], vrecv.at[shard], dev)
        slot = one(a == 3) if h % 2 == 0 else 0
        return remote(qo.at[h], qb.at[slot, b], qsend.at[h], qrecv.at[slot, b], dev)

    def send_all(what):
        for h in (0, 2, 1, 3):
            @pl.when(jnp.logical_not(mine(h)))
            def _():
                exchange(h, what).start()

    def up(s, what):
        dev = (d, a + 1, b)
        if what == "k":
            return remote(kb.at[rows(s)], kb.at[rows(s)], kfs.at[s], krecv.at[s], dev)
        return remote(vb.at[rows(s)], vb.at[rows(s)], vfs.at[s], vrecv.at[s], dev)

    def wait_piece(s):
        up(s, "k").wait_recv()
        up(s, "v").wait_recv()

    def needed(s, level):
        return s >= NL * level - 11

    def pass_on(s):
        @pl.when(feeds & needed(s, a + 1))
        def _():
            up(s, "k").start()
            up(s, "v").start()

    xcopy.wait()
    k_f = project(wk, KCUT, [cut(wk_hbm, wk, wksem, KCUT, c) for c in range(KCUT)], NL)
    for c in range(QCUT):
        cut(wq_hbm, wq, wqsem, QCUT, c).start()
    wo_copy = pltpu.make_async_copy(wo_hbm, wo, wosem)
    wo_copy.start()
    for h in range(NL):
        ko[h, :, :HALF], ko[h, :, HALF:] = rotate(k_f, h)

    @pl.when(jnp.logical_not(donor))
    def _():
        kb[rows(shard), :] = ko[b]

    pl.semaphore_wait(bar, 3 + one(a > 0) + one(a < NL - 1) + 3 * one(host) + one(a == 3) + one((a == 3) & (odd == 1)))
    send_all("k")
    v_f = project(wv, KCUT, [cut(wv_hbm, wv, wvsem, KCUT, c) for c in range(KCUT)], NL)
    for h in range(NL):
        vo[h] = v_f[:, h * HD:(h + 1) * HD].astype(BF)

    @pl.when(jnp.logical_not(donor))
    def _():
        vb[rows(shard), :] = vo[b]

    send_all("v")

    @pl.when(even)
    def _():
        pass_on(shard)

    q_f = project(wq, QCUT, [cut(wq_hbm, wq, wqsem, QCUT, c) for c in range(QCUT)], 2 * NL)
    for h in range(2 * NL):
        qo[h // 2, h % 2, :, :HALF], qo[h // 2, h % 2, :, HALF:] = rotate(q_f, h)

    @pl.when(jnp.logical_not(donor))
    def _():
        qb[0, b] = qo[b]

    send_all("q")

    @pl.when((odd == 1) & (a < 2))
    def _():
        pl.semaphore_wait(go, 1)

    def attend(slot, i, level, key0, n, masked, first):
        keys = pl.ds(pl.multiple_of(key0, 64), n)
        k, v = kb[keys, :], vb[keys, :]
        scores = []
        for g in range(2):
            s = lax.dot_general(qb[slot, i, g], k, (((1,), (1,)), ((), ())), preferred_element_type=F32)
            if masked:
                gap = (lax.broadcasted_iota(jnp.int32, (TOK, n), 0) - lax.broadcasted_iota(jnp.int32, (TOK, n), 1)
                       + (level * LVL + i * TOK - key0))
                s = jnp.where((gap >= 0) & (gap < WINDOW), s, NEG)
            scores.append(s)
        for g in range(2):
            s = scores[g]
            top = jnp.max(s, axis=-1, keepdims=True)
            if first:
                new = top
            else:
                old = m_s[i, g]
                new = jnp.maximum(old, top)
                fix = jnp.exp2((old - new) * SCALE)
            p = jnp.exp2((s - new) * SCALE)
            total = jnp.sum(p, axis=-1, keepdims=True)
            out = jnp.dot(p.astype(BF), v, preferred_element_type=F32)
            if not first:
                total = total + l_s[i, g] * fix
                out = out + acc[i, g] * fix
            m_s[i, g] = new
            l_s[i, g] = total
            acc[i, g] = out

    def attend_shards(lo, hi, fn):
        def step(i, carry):
            fn(i)
            return carry
        lax.fori_loop(lo, hi, step, 0)

    def back_to(slot, i):
        cols = pl.ds(pl.multiple_of(b * 2 * HD, 2 * HD), 2 * HD)
        return remote(osend.at[slot, i], ob.at[:, cols], os_sem.at[slot, i], orecv.at[b], (d, a + slot, i))

    def finish(slot, i):
        for g in range(2):
            osend[slot, i, :, g * HD:(g + 1) * HD] = (acc[i, g] / l_s[i, g]).astype(BF)

    @pl.when(jnp.logical_not(donor))
    def _():
        @pl.when(odd == 1)
        def _():
            pass_on(shard)

        for j in (partner, far, far2):
            wait_piece(a * NL + j)
            pass_on(a * NL + j)

        @pl.when(even & (a == 0))
        def _():
            pl.semaphore_signal(go, inc=1, device_id=(d, a, partner), device_id_type=MESH)

        for j in (partner, far, far2):
            remote(qo.at[0], qb.at[0, j], qsend.at[0], qrecv.at[0, j], (d, a, b)).wait_recv()

        for i in range(NL):
            attend(0, i, a, a * LVL, OWN_KEYS[i], True, True)

        for back in (1, 2, 3):
            @pl.when(a >= back)
            def _():
                base = (a - back) * NL
                near = b // 2 * 2
                away = 2 - near

                def take(s):
                    @pl.when(needed(s, a))
                    def _():
                        wait_piece(s)
                        pass_on(s)

                if back == 1:
                    for j in (b, partner, far, far2):
                        take(base + j)

                    @pl.when(even & (a == 1))
                    def _():
                        pl.semaphore_signal(go, inc=1, device_id=(d, a, partner), device_id_type=MESH)

                    attend_shards(0, NL, lambda i: attend(0, i, a, base * TOK, LVL, False, False))
                elif back == 2:
                    take(base + b)
                    take(base + partner)
                    attend_shards(0, NL, lambda i: attend(0, i, a, (base + near) * TOK, 2 * TOK, True, False))
                    take(base + far)
                    take(base + far2)
                    attend_shards(0, NL, lambda i: attend(0, i, a, (base + away) * TOK, 2 * TOK, True, False))
                else:
                    for j in (b, partner, far, far2):
                        take(base + j)
                    attend_shards(0, NL - 1, lambda i: attend(0, i, a, base * TOK + 256, 512, True, False))

        for i in range(NL):
            finish(0, i)

            @pl.when(b != i)
            def _():
                back_to(0, i).start()

            @pl.when(b == i)
            def _():
                ob[:, pl.ds(pl.multiple_of(b * 2 * HD, 2 * HD), 2 * HD)] = osend[0, i]

    @pl.when(host)
    def _():
        for j in range(NL):
            wait_piece(3 * NL + j)
        for j in range(NL):
            remote(qo.at[0], qb.at[1, j], qsend.at[0], qrecv.at[1, j], (d, a, b)).wait_recv()
        for i in range(NL):
            attend(1, i, 3, 3 * LVL, OWN_KEYS[i], True, True)
            attend(1, i, 3, 2 * LVL, LVL, False, False)
            attend(1, i, 3, LVL, LVL, True, False)
            if i < NL - 1:
                attend(1, i, 3, 256, 512, True, False)
            finish(1, i)
            back_to(1, i).start()

    def take_o(h):
        @pl.when(jnp.logical_not(mine(h)))
        def _():
            remote(osend.at[0, 0], ob.at[:, pl.ds(h * 2 * HD, 2 * HD)], os_sem.at[0, 0], orecv.at[h], (d, a, b)).wait_recv()

    def project_o(h):
        return jnp.dot(ob[:, h * 2 * HD:(h + 1) * 2 * HD], wo[pl.ds(h * 2 * HD, 2 * HD), :],
                       preferred_element_type=F32)

    take_o(0)
    take_o(2)
    wo_copy.wait()
    y = project_o(0) + project_o(2)
    take_o(1)
    take_o(3)
    y_ref[...] = (y + project_o(1) + project_o(3)).astype(BF)

    for h in range(NL):
        @pl.when(jnp.logical_not(mine(h)))
        def _():
            for what in ("k", "v", "q"):
                exchange(h, what).wait_send()

        @pl.when((b != h) & jnp.logical_not(donor))
        def _():
            back_to(0, h).wait_send()

        @pl.when(host)
        def _():
            back_to(1, h).wait_send()

    for s in range(12):
        @pl.when(feeds & (s < NL * (a + 1)) & needed(s, a + 1))
        def _():
            up(s, "k").wait_send()
            up(s, "v").wait_send()


def solution(mesh):
    def local_fn(hidden, w_q, w_k, w_v, w_o):
        freq = (ROPE_BASE ** (-jnp.arange(HALF, dtype=F32) * 2.0 / HD)).reshape(1, HALF)
        vm, hbm = pl.BlockSpec(memory_space=pltpu.VMEM), pl.BlockSpec(memory_space=pl.ANY)
        dma = pltpu.SemaphoreType.DMA
        return pl.pallas_call(
            body,
            out_shape=jax.ShapeDtypeStruct((TOK, DM), BF),
            in_specs=[vm, hbm, hbm, hbm, hbm, hbm],
            out_specs=vm,
            scratch_shapes=[
                pltpu.VMEM((TOK, DM), BF), pltpu.VMEM((DM, 2 * NL, HD), BF), pltpu.VMEM((DM, NL, HD), BF),
                pltpu.VMEM((DM, NL, HD), BF), pltpu.VMEM((2 * NL * HD, DM), BF),
                pltpu.VMEM((NL, TOK, HD), BF), pltpu.VMEM((NL, TOK, HD), BF), pltpu.VMEM((NL, 2, TOK, HD), BF),
                pltpu.VMEM((16 * TOK, HD), BF), pltpu.VMEM((16 * TOK, HD), BF),
                pltpu.VMEM((2, NL, 2, TOK, HD), BF), pltpu.VMEM((TOK, 2 * NL * HD), BF),
                pltpu.VMEM((2, NL, TOK, 2 * HD), BF), pltpu.VMEM((NL, 2, TOK, HD), F32),
                pltpu.VMEM((NL, 2, TOK, 1), F32), pltpu.VMEM((NL, 2, TOK, 1), F32),
                dma(()), dma((KCUT,)), dma((KCUT,)), dma((QCUT,)), dma(()),
                dma((16,)), dma((16,)), dma((16,)), dma((16,)),
                dma((NL,)), dma((NL,)), dma((NL,)), dma((2, NL)), dma((2, NL)), dma((NL,)),
                pltpu.SemaphoreType.REGULAR,
            ],
            compiler_params=pltpu.CompilerParams(collective_id=0, has_side_effects=True,
                                                 vmem_limit_bytes=63 * 2 ** 20),
        )(freq, hidden, w_q, w_k, w_v, w_o.reshape(2 * NL * HD, DM))

    return jax.shard_map(local_fn, mesh=mesh,
                         in_specs=(P(("dp", "cpo", "cpi"), None), P(), P(), P(), P()),
                         out_specs=P(("dp", "cpo", "cpi"), None), check_vma=False)
```

```python
import jax
import jax.numpy as jnp
import numpy as np
from jax import lax
from jax.experimental import pallas as pl
from jax.experimental.pallas import tpu as pltpu
from jax.sharding import PartitionSpec as P

WINDOW = 2048
ROPE_BASE = 10000.0
MESH = pl.DeviceIdType.MESH
NL = 4
TOK = 192
LVL = NL * TOK
DM = 2560
HD = 256
HALF = HD // 2
NEG = -1e30
SCALE = HD ** -0.5 * 1.4426950408889634
KCUT = 2
QCUT = 4
OWN_KEYS = (256, 384, 640, 768)
F32, BF = jnp.float32, jnp.bfloat16


def body(trig_hbm, base_hbm, x_hbm, wq_hbm, wk_hbm, wv_hbm, wo_hbm, y_ref,
         trig, base, x, wq, wk, wv, wo, ko, vo, qo, kb, vb, qb, ob, osend, acc, m_s, l_s,
         tsem, xsem, wksem, wvsem, wqsem, wosem, krecv, vrecv, kfs, vfs, qfs, ksend, vsend, qsend, qrecv,
         os_sem, orecv, go):
    d, a, b = lax.axis_index("dp"), lax.axis_index("cpo"), lax.axis_index("cpi")
    shard = a * NL + b
    odd = lax.rem(b, 2)
    even = odd == 0
    partner = b + 1 - 2 * odd
    far = lax.rem(b + 2, NL)
    far2 = lax.rem(partner + 2, NL)
    near0 = b - odd
    away0 = 2 - near0
    donor = (a == 3) & even
    host = (a == 2) & even
    feeds = (a < 2) | ((a == 2) & (odd == 1))

    def cut(src, dst, sem, n, c):
        r = DM // n
        return pltpu.make_async_copy(src.at[pl.ds(c * r, r)], dst.at[pl.ds(c * r, r)], sem.at[c])

    xcopy = pltpu.make_async_copy(x_hbm, x, xsem)
    xcopy.start()
    for c in range(KCUT):
        cut(wk_hbm, wk, wksem, KCUT, c).start()
    trig_copy = pltpu.make_async_copy(trig_hbm, trig, tsem.at[0])
    base_copy = pltpu.make_async_copy(base_hbm, base, tsem.at[1])
    trig_copy.start()
    base_copy.start()
    for c in range(KCUT):
        cut(wv_hbm, wv, wvsem, KCUT, c).start()

    bar = pltpu.get_barrier_semaphore()

    def greet(level, other):
        pl.semaphore_signal(bar, inc=1, device_id=(d, level, other), device_id_type=MESH)

    for j in (partner, far, far2):
        greet(a, j)

    @pl.when(a > 0)
    def _():
        greet(a - 1, b)

    @pl.when(a < NL - 1)
    def _():
        greet(a + 1, b)

    @pl.when(host)
    def _():
        for j in (partner, far, far2):
            greet(3, j)

    @pl.when(a == 3)
    def _():
        greet(2, lax.rem(b + 2 - odd, NL))

    @pl.when((a == 3) & (odd == 1))
    def _():
        greet(2, b - 1)

    def one(p):
        return p.astype(jnp.int32)

    def project(w, n, copies, heads, between):
        total = None
        for c in range(n):
            copies[c].wait()
            r = DM // n
            part = jnp.dot(x[:, c * r:(c + 1) * r], w[pl.ds(c * r, r)].reshape(r, heads * HD),
                           preferred_element_type=F32)
            total = part if total is None else total + part
            if c in between:
                between[c]()
        return total

    def rotate(t, h, cos, sin):
        lo, hi = t[:, h * HD:h * HD + HALF], t[:, h * HD + HALF:(h + 1) * HD]
        return (lo * cos - hi * sin).astype(BF), (hi * cos + lo * sin).astype(BF)

    def rows(s):
        return pl.ds(pl.multiple_of(s * TOK, TOK), TOK)

    def remote(src, dst, ss, rs, dev):
        return pltpu.make_async_remote_copy(src_ref=src, dst_ref=dst, send_sem=ss, recv_sem=rs,
                                            device_id=dev, device_id_type=MESH)

    def exchange(h, what):
        dev = (d, a, h)
        if what == "k":
            return remote(ko.at[h], kb.at[rows(shard)], ksend.at[h], krecv.at[shard], dev)
        if what == "v":
            return remote(vo.at[h], vb.at[rows(shard)], vsend.at[h], vrecv.at[shard], dev)
        return remote(qo.at[h], qb.at[0, b], qsend.at[h], qrecv.at[0, b], dev)

    def send(what, heads):
        for h in heads:
            @pl.when(b != h)
            def _():
                exchange(h, what).start()

    def hop(s, what, level):
        dev = (d, level, b)
        if what == "k":
            return remote(kb.at[rows(s)], kb.at[rows(s)], kfs.at[s], krecv.at[s], dev)
        return remote(vb.at[rows(s)], vb.at[rows(s)], vfs.at[s], vrecv.at[s], dev)

    def wait_piece(s):
        hop(s, "k", a).wait_recv()
        hop(s, "v", a).wait_recv()

    def needed(s, level):
        return s >= NL * level - 11

    def pass_on(s, whats=("k", "v")):
        @pl.when(feeds & needed(s, a + 1))
        def _():
            for what in whats:
                hop(s, what, a + 1).start()

        @pl.when(donor)
        def _():
            for what in whats:
                hop(s, what, 2).start()

    def q_down(j):
        return remote(qb.at[0, j], qb.at[1, j], qfs.at[j], qrecv.at[1, j], (d, 2, b))

    def wait_q(slot, j):
        remote(qo.at[0], qb.at[slot, j], qsend.at[0], qrecv.at[slot, j], (d, a, b)).wait_recv()

    first_user = even | (a >= 2)

    xcopy.wait()
    with jax.named_scope("k_proj"):
        k_f = project(wk, KCUT, [cut(wk_hbm, wk, wksem, KCUT, c) for c in range(KCUT)], NL, {})
    for c in range(QCUT):
        cut(wq_hbm, wq, wqsem, QCUT, c).start()
    wo_copy = pltpu.make_async_copy(wo_hbm, wo, wosem)
    wo_copy.start()
    trig_copy.wait()
    base_copy.wait()
    cb, sb = base[0, pl.ds(shard, 1), :], base[1, pl.ds(shard, 1), :]
    cos = cb * trig[0] - sb * trig[1]
    sin = sb * trig[0] + cb * trig[1]
    for h in range(NL):
        ko[h, :, :HALF], ko[h, :, HALF:] = rotate(k_f, h, cos, sin)
    kb[rows(shard), :] = ko[b]
    with jax.named_scope("barrier"):
        pl.semaphore_wait(bar, 3 + one(a > 0) + one(a < NL - 1) + 3 * one(host) + one(a == 3)
                          + one((a == 3) & (odd == 1)))
    send("k", (0, 2))

    @pl.when(first_user)
    def _():
        pass_on(shard, ("k",))

    with jax.named_scope("v_proj"):
        v_f = project(wv, KCUT, [cut(wv_hbm, wv, wvsem, KCUT, c) for c in range(KCUT)], NL, {})
    for h in range(NL):
        vo[h] = v_f[:, h * HD:(h + 1) * HD].astype(BF)
    vb[rows(shard), :] = vo[b]
    send("v", (0, 2))

    @pl.when(first_user)
    def _():
        pass_on(shard, ("v",))

    def relay_partner():
        @pl.when(even)
        def _():
            wait_piece(a * NL + partner)
            pass_on(a * NL + partner)

    with jax.named_scope("q_proj"):
        q_f = project(wq, QCUT, [cut(wq_hbm, wq, wqsem, QCUT, c) for c in range(QCUT)], 2 * NL, {1: relay_partner})
    for h in range(2 * NL):
        qo[h // 2, h % 2, :, :HALF], qo[h // 2, h % 2, :, HALF:] = rotate(q_f, h, cos, sin)
    qb[0, b] = qo[b]
    send("q", (0, 2))
    send("k", (1, 3))
    send("v", (1, 3))
    send("q", (1, 3))

    def attend(slot, shards, level, key0, n, masked, first):
        keys = pl.ds(pl.multiple_of(key0, 64), n)
        k, v = kb[keys, :], vb[keys, :]
        chains = [(i, g) for i in shards for g in range(2)]
        scores = []
        for i, g in chains:
            s = lax.dot_general(qb[slot, i, g], k, (((1,), (1,)), ((), ())), preferred_element_type=F32)
            if masked:
                gap = (lax.broadcasted_iota(jnp.int32, (TOK, n), 0) - lax.broadcasted_iota(jnp.int32, (TOK, n), 1)
                       + (level * LVL + i * TOK - key0))
                s = jnp.where((gap >= 0) & (gap < WINDOW), s, NEG)
            scores.append(s)
        for (i, g), s in zip(chains, scores):
            top = jnp.max(s, axis=-1, keepdims=True)
            if first:
                new = top
            else:
                old = m_s[i, g]
                new = jnp.maximum(old, top)
                fix = jnp.exp2((old - new) * SCALE)
            p = jnp.exp2((s - new) * SCALE)
            total = jnp.sum(p, axis=-1, keepdims=True)
            out = jnp.dot(p.astype(BF), v, preferred_element_type=F32)
            if not first:
                total = total + l_s[i, g] * fix
                out = out + acc[i, g] * fix
            m_s[i, g] = new
            l_s[i, g] = total
            acc[i, g] = out

    def loop(lo, hi, fn):
        def step(i, carry):
            fn(i)
            return carry
        lax.fori_loop(lo, hi, step, 0)

    def head_cols():
        return pl.ds(pl.multiple_of(b * 2 * HD, 2 * HD), 2 * HD)

    def back_to(slot, i):
        return remote(osend.at[slot, i], ob.at[:, head_cols()], os_sem.at[slot, i], orecv.at[b], (d, a + slot, i))

    def finish(slot, i):
        for g in range(2):
            osend[slot, i, :, g * HD:(g + 1) * HD] = (acc[i, g] / l_s[i, g]).astype(BF)
        if slot == 1:
            back_to(1, i).start()
            return

        @pl.when(b != i)
        def _():
            back_to(0, i).start()

        @pl.when(b == i)
        def _():
            ob[:, head_cols()] = osend[0, i]

    def turn(t):
        return lax.rem(away0 + t, NL)

    low = (a - 1) * NL

    def own_block(slot):
        with jax.named_scope("own_att"):
            for i in range(NL):
                attend(slot, (i,), a + slot, (a + slot) * LVL, OWN_KEYS[i], True, True)

    def take(s):
        wait_piece(s)
        pass_on(s)

    @pl.when(even)
    def _():
        with jax.named_scope("own_pieces"):
            for j in (far, far2):
                take(a * NL + j)

    @pl.when((odd == 1) & (a >= 2))
    def _():
        with jax.named_scope("own_pieces"):
            for j in (partner, far, far2):
                take(a * NL + j)

    @pl.when(even & (a == 1))
    def _():
        with jax.named_scope("take_low"):
            for j in (b, partner, far, far2):
                take(low + j)
            for s in (shard, NL + partner, NL + far, NL + far2, b, partner):
                hop(s, "k", 2).wait_send()
                hop(s, "v", 2).wait_send()

    @pl.when(even & (a < 2))
    def _():
        pl.semaphore_signal(go, inc=1, device_id=(d, a, partner), device_id_type=MESH)

    @pl.when((odd == 1) & (a < 2))
    def _():
        with jax.named_scope("go_wait"):
            pl.semaphore_wait(go, 1)
        pass_on(shard)
        for j in (partner, far, far2):
            take(a * NL + j)

        @pl.when(a == 1)
        def _():
            with jax.named_scope("take_low"):
                for j in (b, partner, far, far2):
                    take(low + j)

    with jax.named_scope("own_q"):
        for j in (partner, far, far2):
            @pl.when(jnp.logical_not(donor))
            def _():
                wait_q(0, j)

    @pl.when(donor)
    def _():
        q_down(b).start()
        for j in (partner, far, far2):
            wait_q(0, j)
            q_down(j).start()

    @pl.when(jnp.logical_not(donor))
    def _():
        own_block(0)

        @pl.when(a == 0)
        def _():
            loop(0, NL, lambda t: finish(0, turn(t)))

        @pl.when(a > 0)
        def _():
            @pl.when(a >= 2)
            def _():
                with jax.named_scope("take1"):
                    for j in (b, partner, far, far2):
                        take(low + j)

            with jax.named_scope("att1"):
                loop(0, NL, lambda i: attend(0, (i,), a, (a - 1) * LVL, LVL, False, False))

            @pl.when(a == 1)
            def _():
                loop(0, NL, lambda t: finish(0, turn(t)))

        @pl.when(host)
        def _():
            with jax.named_scope("take2"):
                for j in (b, partner, far, far2):
                    take(j)

            def last(t):
                attend(0, (turn(t),), a, 0, LVL, True, False)
                finish(0, turn(t))
            with jax.named_scope("att2"):
                loop(0, NL, last)

        @pl.when((a >= 2) & (odd == 1))
        def _():
            lvl2 = (a - 2) * NL
            with jax.named_scope("take2a"):
                for j in (b, partner):
                    take(lvl2 + j)
            with jax.named_scope("att2a"):
                loop(0, 2, lambda t: attend(0, (2 * t, 2 * t + 1), a, (lvl2 + near0) * TOK, 2 * TOK, True, False))
            with jax.named_scope("take2b"):
                for j in (far, far2):
                    take(lvl2 + j)

            def last(t):
                i = turn(2 * t)
                attend(0, (i, i + 1), a, (lvl2 + away0) * TOK, 2 * TOK, True, False)

                @pl.when(a == 2)
                def _():
                    finish(0, i)
                    finish(0, i + 1)
            with jax.named_scope("att2b"):
                loop(0, 2, last)

        @pl.when((a == 3) & (odd == 1))
        def _():
            finish(0, NL - 1)
            with jax.named_scope("take3"):
                for j in (b, partner, far, far2):
                    @pl.when(j > 0)
                    def _():
                        wait_piece(j)

            def last(t):
                @pl.when(turn(t) < NL - 1)
                def _():
                    attend(0, (turn(t),), a, 256, 512, True, False)
                    finish(0, turn(t))
            with jax.named_scope("att3"):
                loop(0, NL, last)

    @pl.when(host)
    def _():
        with jax.named_scope("host_wait"):
            for j in range(NL):
                wait_piece(3 * NL + j)
            for j in range(NL):
                wait_q(1, j)
        own_block(1)

        def each(i):
            attend(1, (i,), 3, 2 * LVL, LVL, False, False)
            attend(1, (i,), 3, LVL, LVL, True, False)

            @pl.when(i < NL - 1)
            def _():
                attend(1, (i,), 3, 256, 512, True, False)
            finish(1, i)
        with jax.named_scope("host_att"):
            loop(0, NL, each)

    def take_o(h):
        @pl.when((b != h) | ((a == 3) & (h % 2 == 0)))
        def _():
            remote(osend.at[0, 0], ob.at[:, pl.ds(h * 2 * HD, 2 * HD)], os_sem.at[0, 0], orecv.at[h], (d, a, b)).wait_recv()

    def project_o(h):
        return jnp.dot(ob[:, h * 2 * HD:(h + 1) * 2 * HD], wo[pl.ds(h * 2 * HD, 2 * HD), :],
                       preferred_element_type=F32)

    with jax.named_scope("o_even"):
        take_o(0)
        take_o(2)
    wo_copy.wait()
    y = project_o(0) + project_o(2)
    with jax.named_scope("o_odd"):
        take_o(1)
        take_o(3)
    y_ref[...] = (y + project_o(1) + project_o(3)).astype(BF)

    for h in range(NL):
        @pl.when(b != h)
        def _():
            for what in ("k", "v", "q"):
                exchange(h, what).wait_send()

        @pl.when((b != h) & jnp.logical_not(donor))
        def _():
            back_to(0, h).wait_send()

        @pl.when(host)
        def _():
            back_to(1, h).wait_send()

        @pl.when(donor)
        def _():
            q_down(h).wait_send()
            for what in ("k", "v"):
                hop(3 * NL + h, what, 2).wait_send()

    for s in range(12):
        waited = even & (a == 1) & ((s >= NL) | (s // 2 == b // 2))

        @pl.when(feeds & (s < NL * (a + 1)) & needed(s, a + 1) & jnp.logical_not(waited))
        def _():
            for what in ("k", "v"):
                hop(s, what, a + 1).wait_send()


def solution(mesh):
    def local_fn(hidden, w_q, w_k, w_v, w_o):
        freq = ROPE_BASE ** (-np.arange(HALF) * 2.0 / HD)
        steps, starts = np.arange(TOK)[:, None] * freq, (np.arange(NL * NL) * TOK)[:, None] * freq
        trig = jnp.asarray(np.stack([np.cos(steps), np.sin(steps)]), F32)
        base = jnp.asarray(np.stack([np.cos(starts), np.sin(starts)]), F32)
        vm, hbm = pl.BlockSpec(memory_space=pltpu.VMEM), pl.BlockSpec(memory_space=pl.ANY)
        dma = pltpu.SemaphoreType.DMA
        return pl.pallas_call(
            body,
            out_shape=jax.ShapeDtypeStruct((TOK, DM), BF),
            in_specs=[hbm] * 7,
            out_specs=vm,
            scratch_shapes=[
                pltpu.VMEM((2, TOK, HALF), F32), pltpu.VMEM((2, NL * NL, HALF), F32),
                pltpu.VMEM((TOK, DM), BF), pltpu.VMEM((DM, 2 * NL, HD), BF), pltpu.VMEM((DM, NL, HD), BF),
                pltpu.VMEM((DM, NL, HD), BF), pltpu.VMEM((2 * NL * HD, DM), BF),
                pltpu.VMEM((NL, TOK, HD), BF), pltpu.VMEM((NL, TOK, HD), BF), pltpu.VMEM((NL, 2, TOK, HD), BF),
                pltpu.VMEM((16 * TOK, HD), BF), pltpu.VMEM((16 * TOK, HD), BF),
                pltpu.VMEM((2, NL, 2, TOK, HD), BF), pltpu.VMEM((TOK, 2 * NL * HD), BF),
                pltpu.VMEM((2, NL, TOK, 2 * HD), BF), pltpu.VMEM((NL, 2, TOK, HD), F32),
                pltpu.VMEM((NL, 2, TOK, 1), F32), pltpu.VMEM((NL, 2, TOK, 1), F32),
                dma((2,)), dma(()), dma((KCUT,)), dma((KCUT,)), dma((QCUT,)), dma(()),
                dma((16,)), dma((16,)), dma((16,)), dma((16,)), dma((NL,)),
                dma((NL,)), dma((NL,)), dma((NL,)), dma((2, NL)), dma((2, NL)), dma((NL,)),
                pltpu.SemaphoreType.REGULAR,
            ],
            compiler_params=pltpu.CompilerParams(collective_id=0, has_side_effects=True,
                                                 vmem_limit_bytes=63 * 2 ** 20),
        )(trig, base, hidden, w_q, w_k, w_v, w_o.reshape(2 * NL * HD, DM))

    return jax.shard_map(local_fn, mesh=mesh,
                         in_specs=(P(("dp", "cpo", "cpi"), None), P(), P(), P(), P()),
                         out_specs=P(("dp", "cpo", "cpi"), None), check_vma=False)
```

```python
import jax
import jax.numpy as jnp
import numpy as np
from jax import lax
from jax.experimental import pallas as pl
from jax.experimental.pallas import tpu as pltpu
from jax.sharding import PartitionSpec as P

WINDOW = 2048
ROPE_BASE = 10000.0
MESH = pl.DeviceIdType.MESH
NL = 4
TOK = 192
LVL = NL * TOK
DM = 2560
HD = 256
HALF = HD // 2
LANES = 128
YCOLS = 512
NEG = -1e30
SCALE = HD ** -0.5 * 1.4426950408889634
KCUT = 2
QCUT = 4
OWN_KEYS = (256, 384, 640, 768)
F32, BF = jnp.float32, jnp.bfloat16


def body(trig_hbm, base_hbm, x_hbm, wq_hbm, wk_hbm, wv_hbm, wo_hbm, y_ref,
         trig, base, x, wq, wk, wv, wo, ko, vo, qo, kb, vb, qb, ob, osend, acc, m_s, l_s, y_acc, y_tile,
         tsem, xsem, wksem, wvsem, wqsem, wosem, krecv, vrecv, kfs, vfs, qfs, ksend, vsend, qsend, qrecv,
         os_sem, orecv, ysem, go):
    d, a, b = lax.axis_index("dp"), lax.axis_index("cpo"), lax.axis_index("cpi")
    shard = a * NL + b
    odd = lax.rem(b, 2)
    even = odd == 0
    partner = b + 1 - 2 * odd
    far = lax.rem(b + 2, NL)
    far2 = lax.rem(partner + 2, NL)
    near0 = b - odd
    away0 = 2 - near0
    donor = (a == 3) & even
    host = (a == 2) & even
    feeds = (a < 2) | ((a == 2) & (odd == 1))

    def cut(src, dst, sem, n, c):
        r = DM // n
        return pltpu.make_async_copy(src.at[pl.ds(c * r, r)], dst.at[pl.ds(c * r, r)], sem.at[c])

    xcopy = pltpu.make_async_copy(x_hbm, x, xsem)
    xcopy.start()
    cut(wk_hbm, wk, wksem, KCUT, 0).start()
    trig_copy = pltpu.make_async_copy(trig_hbm, trig, tsem.at[0])
    base_copy = pltpu.make_async_copy(base_hbm, base, tsem.at[1])

    bar = pltpu.get_barrier_semaphore()

    def greet(level, other):
        pl.semaphore_signal(bar, inc=1, device_id=(d, level, other), device_id_type=MESH)

    for j in (partner, far, far2):
        greet(a, j)

    @pl.when(a > 0)
    def _():
        greet(a - 1, b)

    @pl.when(a < NL - 1)
    def _():
        greet(a + 1, b)

    @pl.when(host)
    def _():
        for j in (partner, far, far2):
            greet(3, j)

    @pl.when(a == 3)
    def _():
        greet(2, lax.rem(b + 2 - odd, NL))

    @pl.when((a == 3) & (odd == 1))
    def _():
        greet(2, b - 1)

    def one(p):
        return p.astype(jnp.int32)

    def project(w, n, copies, heads, between):
        total = None
        for c in range(n):
            copies[c].wait()
            r = DM // n
            part = jnp.dot(x[:, c * r:(c + 1) * r], w[pl.ds(c * r, r)].reshape(r, heads * HD),
                           preferred_element_type=F32)
            total = part if total is None else total + part
            if c in between:
                between[c]()
        return total

    def rotate(t, h, cos, sin):
        lo, hi = t[:, h * HD:h * HD + HALF], t[:, h * HD + HALF:(h + 1) * HD]
        return (lo * cos - hi * sin).astype(BF), (hi * cos + lo * sin).astype(BF)

    def rows(s):
        return pl.ds(pl.multiple_of(s * TOK, TOK), TOK)

    def remote(src, dst, ss, rs, dev):
        return pltpu.make_async_remote_copy(src_ref=src, dst_ref=dst, send_sem=ss, recv_sem=rs,
                                            device_id=dev, device_id_type=MESH)

    def exchange(h, what):
        dev = (d, a, h)
        if what == "k":
            return remote(ko.at[h], kb.at[rows(shard)], ksend.at[h], krecv.at[shard], dev)
        if what == "v":
            return remote(vo.at[h], vb.at[rows(shard)], vsend.at[h], vrecv.at[shard], dev)
        return remote(qo.at[h], qb.at[0, b], qsend.at[h], qrecv.at[0, b], dev)

    def send(what, heads):
        for h in heads:
            @pl.when(b != h)
            def _():
                exchange(h, what).start()

    def hop(s, what, level):
        dev = (d, level, b)
        if what == "k":
            return remote(kb.at[rows(s)], kb.at[rows(s)], kfs.at[s], krecv.at[s], dev)
        return remote(vb.at[rows(s)], vb.at[rows(s)], vfs.at[s], vrecv.at[s], dev)

    def wait_piece(s):
        hop(s, "k", a).wait_recv()
        hop(s, "v", a).wait_recv()

    def needed(s, level):
        return s >= NL * level - 11

    def pass_on(s, whats=("k", "v")):
        @pl.when(feeds & needed(s, a + 1))
        def _():
            for what in whats:
                hop(s, what, a + 1).start()

        @pl.when(donor)
        def _():
            for what in whats:
                hop(s, what, 2).start()

    def q_down(j):
        return remote(qb.at[0, j], qb.at[1, j], qfs.at[j], qrecv.at[1, j], (d, 2, b))

    def wait_q(slot, j):
        remote(qo.at[0], qb.at[slot, j], qsend.at[0], qrecv.at[slot, j], (d, a, b)).wait_recv()

    first_user = even | (a >= 2)

    xcopy.wait()
    for c in range(1, KCUT):
        cut(wk_hbm, wk, wksem, KCUT, c).start()
    trig_copy.start()
    base_copy.start()
    for c in range(KCUT):
        cut(wv_hbm, wv, wvsem, KCUT, c).start()
    with jax.named_scope("k_proj"):
        k_f = project(wk, KCUT, [cut(wk_hbm, wk, wksem, KCUT, c) for c in range(KCUT)], NL, {})
    for c in range(QCUT):
        cut(wq_hbm, wq, wqsem, QCUT, c).start()
    wo_copy = pltpu.make_async_copy(wo_hbm, wo, wosem)
    wo_copy.start()
    trig_copy.wait()
    base_copy.wait()
    cb, sb = base[0, pl.ds(shard, 1), :], base[1, pl.ds(shard, 1), :]
    cos = cb * trig[0] - sb * trig[1]
    sin = sb * trig[0] + cb * trig[1]
    for h in range(NL):
        ko[h, :, :HALF], ko[h, :, HALF:] = rotate(k_f, h, cos, sin)
    kb[rows(shard), :] = ko[b]
    with jax.named_scope("barrier"):
        pl.semaphore_wait(bar, 3 + one(a > 0) + one(a < NL - 1) + 3 * one(host) + one(a == 3)
                          + one((a == 3) & (odd == 1)))
    send("k", (0, 2, 1, 3))

    @pl.when(first_user)
    def _():
        pass_on(shard, ("k",))

    with jax.named_scope("v_proj"):
        v_f = project(wv, KCUT, [cut(wv_hbm, wv, wvsem, KCUT, c) for c in range(KCUT)], NL, {})
    for h in range(NL):
        vo[h] = v_f[:, h * HD:(h + 1) * HD].astype(BF)
    vb[rows(shard), :] = vo[b]
    send("v", (0, 2, 1, 3))

    @pl.when(first_user)
    def _():
        pass_on(shard, ("v",))

    def relay_partner():
        @pl.when(even)
        def _():
            wait_piece(a * NL + partner)
            pass_on(a * NL + partner)

    with jax.named_scope("q_proj"):
        q_f = project(wq, QCUT, [cut(wq_hbm, wq, wqsem, QCUT, c) for c in range(QCUT)], 2 * NL, {1: relay_partner})
    for h in range(2 * NL):
        qo[h // 2, h % 2, :, :HALF], qo[h // 2, h % 2, :, HALF:] = rotate(q_f, h, cos, sin)
    qb[0, b] = qo[b]
    send("q", (0, 2, 1, 3))

    def wide(t, n):
        return jnp.concatenate([t] * (n // LANES), axis=1)

    def attend(slot, i, level, key0, n, masked, first=False, last=False):
        keys = pl.ds(pl.multiple_of(key0, 64), n)
        k, v = kb[keys, :], vb[keys, :]
        scores = []
        for g in range(2):
            s = lax.dot_general(qb[slot, i, g], k, (((1,), (1,)), ((), ())), preferred_element_type=F32)
            if masked:
                gap = (lax.broadcasted_iota(jnp.int32, (TOK, n), 0) - lax.broadcasted_iota(jnp.int32, (TOK, n), 1)
                       + (level * LVL + i * TOK - key0))
                s = jnp.where((gap >= 0) & (gap < WINDOW), s, NEG)
            scores.append(s)
        for g, s in enumerate(scores):
            top = jnp.max(s, axis=-1, keepdims=True)
            if first:
                new = jnp.broadcast_to(top, (TOK, LANES))
            else:
                old = m_s[i, g]
                new = jnp.maximum(old, top)
                fix = jnp.exp2((old - new) * SCALE)
            p = jnp.exp2((s - wide(new, n)) * SCALE)
            total = jnp.broadcast_to(jnp.sum(p, axis=-1, keepdims=True), (TOK, LANES))
            out = jnp.dot(p.astype(BF), v, preferred_element_type=F32)
            if not first:
                total = total + l_s[i, g] * fix
                out = out + acc[i, g] * wide(fix, HD)
            if last:
                osend[slot, i, :, g * HD:(g + 1) * HD] = (out * wide(1.0 / total, HD)).astype(BF)
            else:
                m_s[i, g] = new
                l_s[i, g] = total
                acc[i, g] = out
        if last:
            give(slot, i)

    def loop(lo, hi, fn):
        def step(i, carry):
            fn(i)
            return carry
        lax.fori_loop(lo, hi, step, 0)

    def head_cols():
        return pl.ds(pl.multiple_of(b * 2 * HD, 2 * HD), 2 * HD)

    def back_to(slot, i):
        return remote(osend.at[slot, i], ob.at[:, head_cols()], os_sem.at[slot, i], orecv.at[b], (d, a + slot, i))

    def give(slot, i):
        if slot == 1:
            back_to(1, i).start()
            return

        @pl.when(b != i)
        def _():
            back_to(0, i).start()

        @pl.when(b == i)
        def _():
            ob[:, head_cols()] = osend[0, i]

    def finish(slot, i):
        for g in range(2):
            osend[slot, i, :, g * HD:(g + 1) * HD] = (acc[i, g] * wide(1.0 / l_s[i, g], HD)).astype(BF)
        give(slot, i)

    def turn(t):
        return lax.rem(away0 + t, NL)

    low = (a - 1) * NL

    def own_block(slot):
        with jax.named_scope("own_att"):
            for i in range(NL):
                attend(slot, i, a + slot, (a + slot) * LVL, OWN_KEYS[i], True, first=True)

    def take(s):
        wait_piece(s)
        pass_on(s)

    @pl.when(even)
    def _():
        with jax.named_scope("own_pieces"):
            for j in (far, far2):
                take(a * NL + j)

    @pl.when((odd == 1) & (a >= 2))
    def _():
        with jax.named_scope("own_pieces"):
            for j in (partner, far, far2):
                take(a * NL + j)

    @pl.when(even & (a == 1))
    def _():
        with jax.named_scope("take_low"):
            for j in (b, partner, far, far2):
                take(low + j)
            for s in (shard, NL + partner, NL + far, NL + far2, b, partner):
                hop(s, "k", 2).wait_send()
                hop(s, "v", 2).wait_send()

    @pl.when(even & (a < 2))
    def _():
        pl.semaphore_signal(go, inc=1, device_id=(d, a, partner), device_id_type=MESH)

    @pl.when((odd == 1) & (a < 2))
    def _():
        with jax.named_scope("go_wait"):
            pl.semaphore_wait(go, 1)
        pass_on(shard)
        for j in (partner, far, far2):
            take(a * NL + j)

        @pl.when(a == 1)
        def _():
            with jax.named_scope("take_low"):
                for j in (3, 2, 1, 0):
                    take(low + j)

    with jax.named_scope("own_q"):
        for j in (partner, far, far2):
            @pl.when(jnp.logical_not(donor))
            def _():
                wait_q(0, j)

    @pl.when(donor)
    def _():
        q_down(b).start()
        for j in (partner, far, far2):
            wait_q(0, j)
            q_down(j).start()

    @pl.when(jnp.logical_not(donor))
    def _():
        own_block(0)

        @pl.when(a == 0)
        def _():
            loop(0, NL, lambda t: finish(0, turn(t)))

        @pl.when(a > 0)
        def _():
            @pl.when(a >= 2)
            def _():
                with jax.named_scope("take1"):
                    for j in (b, partner, far, far2):
                        take(low + j)

            @pl.when(a == 1)
            def _():
                loop(0, NL, lambda t: attend(0, turn(t), a, 0, LVL, False, last=True))

            @pl.when(a > 1)
            def _():
                with jax.named_scope("att1"):
                    loop(0, NL, lambda i: attend(0, i, a, (a - 1) * LVL, LVL, False))

        @pl.when(host)
        def _():
            with jax.named_scope("take2"):
                for j in (b, partner, far, far2):
                    take(j)
            with jax.named_scope("att2"):
                loop(0, NL, lambda t: attend(0, turn(t), a, 0, LVL, True, last=True))

        @pl.when((a >= 2) & (odd == 1))
        def _():
            lvl2 = (a - 2) * NL
            with jax.named_scope("take2a"):
                take(lvl2 + 3)
                take(lvl2 + 2)
            with jax.named_scope("att2a"):
                loop(0, 2, lambda i: attend(0, i, a, lvl2 * TOK + 2 * TOK, 2 * TOK, False))
            with jax.named_scope("take2b"):
                take(lvl2 + 1)
            with jax.named_scope("att2b"):
                loop(2, NL, lambda i: attend(0, i, a, lvl2 * TOK + 2 * TOK, 2 * TOK, False))
            with jax.named_scope("take2c"):
                take(lvl2)

        @pl.when((a == 2) & (odd == 1))
        def _():
            with jax.named_scope("att2c"):
                loop(0, NL, lambda t: attend(0, turn(t), a, 0, 2 * TOK, True, last=True))

        @pl.when((a == 3) & (odd == 1))
        def _():
            with jax.named_scope("att2c"):
                loop(0, NL, lambda i: attend(0, i, a, LVL, 2 * TOK, True))
            finish(0, NL - 1)
            with jax.named_scope("take3"):
                wait_piece(3)
                wait_piece(2)
            with jax.named_scope("att3"):
                attend(0, 2, a, 2 * TOK, 2 * TOK, True, last=True)
                attend(0, 1, a, 2 * TOK, 2 * TOK, True, last=True)
                attend(0, 0, a, 2 * TOK, 2 * TOK, True)
            with jax.named_scope("take3b"):
                wait_piece(1)
            with jax.named_scope("att3b"):
                attend(0, 0, a, 256, 128, True, last=True)

    @pl.when(host)
    def _():
        with jax.named_scope("host_wait"):
            for j in range(NL):
                wait_piece(3 * NL + j)
            for j in range(NL):
                wait_q(1, j)
        own_block(1)

        def each(i):
            attend(1, i, 3, 2 * LVL, LVL, False)

            @pl.when(i < NL - 1)
            def _():
                attend(1, i, 3, 256, 512, True)
            attend(1, i, 3, LVL, LVL, True, last=True)
        with jax.named_scope("host_att"):
            loop(0, NL, each)

    def take_o(h):
        @pl.when((b != h) | ((a == 3) & (h % 2 == 0)))
        def _():
            remote(osend.at[0, 0], ob.at[:, pl.ds(h * 2 * HD, 2 * HD)], os_sem.at[0, 0], orecv.at[h], (d, a, b)).wait_recv()

    def project_o(h, cols):
        return jnp.dot(ob[:, h * 2 * HD:(h + 1) * 2 * HD], wo[pl.ds(h * 2 * HD, 2 * HD), cols],
                       preferred_element_type=F32)

    tiles = [pl.ds(t * YCOLS, YCOLS) for t in range(DM // YCOLS)]
    with jax.named_scope("o_even"):
        take_o(0)
        take_o(2)
    wo_copy.wait()
    for cols in tiles:
        y_acc[:, cols] = project_o(0, cols) + project_o(2, cols)
    with jax.named_scope("o_odd"):
        take_o(1)
        take_o(3)
    y_copies = []
    with jax.named_scope("y_out"):
        for t, cols in enumerate(tiles):
            y_tile[:, cols] = (y_acc[:, cols] + project_o(1, cols) + project_o(3, cols)).astype(BF)
            y_copies.append(pltpu.make_async_copy(y_tile.at[:, cols], y_ref.at[:, cols], ysem.at[t]))
            y_copies[-1].start()

    for h in range(NL):
        @pl.when(b != h)
        def _():
            for what in ("k", "v", "q"):
                exchange(h, what).wait_send()

        @pl.when((b != h) & jnp.logical_not(donor))
        def _():
            back_to(0, h).wait_send()

        @pl.when(host)
        def _():
            back_to(1, h).wait_send()

        @pl.when(donor)
        def _():
            q_down(h).wait_send()
            for what in ("k", "v"):
                hop(3 * NL + h, what, 2).wait_send()

    for s in range(12):
        waited = even & (a == 1) & ((s >= NL) | (s // 2 == b // 2))

        @pl.when(feeds & (s < NL * (a + 1)) & needed(s, a + 1) & jnp.logical_not(waited))
        def _():
            for what in ("k", "v"):
                hop(s, what, a + 1).wait_send()
    for c in y_copies:
        c.wait()


def solution(mesh):
    def local_fn(hidden, w_q, w_k, w_v, w_o):
        freq = ROPE_BASE ** (-np.arange(HALF) * 2.0 / HD)
        steps, starts = np.arange(TOK)[:, None] * freq, (np.arange(NL * NL) * TOK)[:, None] * freq
        trig = jnp.asarray(np.stack([np.cos(steps), np.sin(steps)]), F32)
        base = jnp.asarray(np.stack([np.cos(starts), np.sin(starts)]), F32)
        hbm = pl.BlockSpec(memory_space=pl.ANY)
        dma = pltpu.SemaphoreType.DMA
        return pl.pallas_call(
            body,
            out_shape=jax.ShapeDtypeStruct((TOK, DM), BF),
            in_specs=[hbm] * 7,
            out_specs=hbm,
            scratch_shapes=[
                pltpu.VMEM((2, TOK, HALF), F32), pltpu.VMEM((2, NL * NL, HALF), F32),
                pltpu.VMEM((TOK, DM), BF), pltpu.VMEM((DM, 2 * NL, HD), BF), pltpu.VMEM((DM, NL, HD), BF),
                pltpu.VMEM((DM, NL, HD), BF), pltpu.VMEM((2 * NL * HD, DM), BF),
                pltpu.VMEM((NL, TOK, HD), BF), pltpu.VMEM((NL, TOK, HD), BF), pltpu.VMEM((NL, 2, TOK, HD), BF),
                pltpu.VMEM((16 * TOK, HD), BF), pltpu.VMEM((16 * TOK, HD), BF),
                pltpu.VMEM((2, NL, 2, TOK, HD), BF), pltpu.VMEM((TOK, 2 * NL * HD), BF),
                pltpu.VMEM((2, NL, TOK, 2 * HD), BF), pltpu.VMEM((NL, 2, TOK, HD), F32),
                pltpu.VMEM((NL, 2, TOK, LANES), F32), pltpu.VMEM((NL, 2, TOK, LANES), F32),
                pltpu.VMEM((TOK, DM), F32), pltpu.VMEM((TOK, DM), BF),
                dma((2,)), dma(()), dma((KCUT,)), dma((KCUT,)), dma((QCUT,)), dma(()),
                dma((16,)), dma((16,)), dma((16,)), dma((16,)), dma((NL,)),
                dma((NL,)), dma((NL,)), dma((NL,)), dma((2, NL)), dma((2, NL)), dma((NL,)), dma((DM // YCOLS,)),
                pltpu.SemaphoreType.REGULAR,
            ],
            compiler_params=pltpu.CompilerParams(collective_id=0, has_side_effects=True,
                                                 vmem_limit_bytes=63 * 2 ** 20),
        )(trig, base, hidden, w_q, w_k, w_v, w_o.reshape(2 * NL * HD, DM))

    return jax.shard_map(local_fn, mesh=mesh,
                         in_specs=(P(("dp", "cpo", "cpi"), None), P(), P(), P(), P()),
                         out_specs=P(("dp", "cpo", "cpi"), None), check_vma=False)
```

```python
import jax
import jax.numpy as jnp
import numpy as np
from jax import lax
from jax.experimental import pallas as pl
from jax.experimental.pallas import tpu as pltpu
from jax.sharding import PartitionSpec as P

WINDOW = 2048
ROPE_BASE = 10000.0
MESH = pl.DeviceIdType.MESH
NL = 4
TOK = 192
LVL = NL * TOK
DM = 2560
HD = 256
HALF = HD // 2
LANES = 128
YCOLS = 512
NEG = -1e30
SCALE = HD ** -0.5 * 1.4426950408889634
KCUT = 4
QCUT = 4
OWN_KEYS = (256, 384, 640, 768)
F32, BF = jnp.float32, jnp.bfloat16


def body(trig_hbm, base_hbm, x_hbm, wq_hbm, wk_hbm, wv_hbm, wo_hbm, y_ref,
         trig, base, x, wq, wk, wv, wo, ko, vo, qo, kb, vb, qb, ob, osend, acc, m_s, l_s, y_acc, y_tile,
         tsem, xsem, wksem, wvsem, wqsem, wosem, krecv, vrecv, kfs, vfs, qfs, ksend, vsend, qsend, qrecv,
         os_sem, orecv, ysem, go):
    d, a, b = lax.axis_index("dp"), lax.axis_index("cpo"), lax.axis_index("cpi")
    shard = a * NL + b
    odd = lax.rem(b, 2)
    even = odd == 0
    partner = b + 1 - 2 * odd
    far = lax.rem(b + 2, NL)
    far2 = lax.rem(partner + 2, NL)
    near0 = b - odd
    away0 = 2 - near0
    donor = (a == 3) & even
    host = (a == 2) & even
    feeds = (a < 2) | ((a == 2) & (odd == 1))

    def cut(src, dst, sem, n, c):
        r = DM // n
        return pltpu.make_async_copy(src.at[pl.ds(c * r, r)], dst.at[pl.ds(c * r, r)], sem.at[c])

    xcopy = pltpu.make_async_copy(x_hbm, x, xsem)
    xcopy.start()
    for c in range(KCUT):
        cut(wk_hbm, wk, wksem, KCUT, c).start()
    trig_copy = pltpu.make_async_copy(trig_hbm, trig, tsem.at[0])
    base_copy = pltpu.make_async_copy(base_hbm, base, tsem.at[1])

    bar = pltpu.get_barrier_semaphore()

    def greet(level, other):
        pl.semaphore_signal(bar, inc=1, device_id=(d, level, other), device_id_type=MESH)

    for j in (partner, far, far2):
        greet(a, j)

    @pl.when(a > 0)
    def _():
        greet(a - 1, b)

    @pl.when(a < NL - 1)
    def _():
        greet(a + 1, b)

    @pl.when(host)
    def _():
        for j in (partner, far, far2):
            greet(3, j)

    @pl.when(a == 3)
    def _():
        greet(2, lax.rem(b + 2 - odd, NL))

    @pl.when((a == 3) & (odd == 1))
    def _():
        greet(2, b - 1)

    def one(p):
        return p.astype(jnp.int32)

    def project(w, n, copies, heads, fetch, between):
        total = None
        for c in range(n):
            copies[c].wait()
            if c in fetch:
                fetch[c]()
            r = DM // n
            part = jnp.dot(x[:, c * r:(c + 1) * r], w[pl.ds(c * r, r)].reshape(r, heads * HD),
                           preferred_element_type=F32)
            total = part if total is None else total + part
            if c in between:
                between[c]()
        return total

    def rotate(t, h, cos, sin):
        lo, hi = t[:, h * HD:h * HD + HALF], t[:, h * HD + HALF:(h + 1) * HD]
        return (lo * cos - hi * sin).astype(BF), (hi * cos + lo * sin).astype(BF)

    def rows(s):
        return pl.ds(pl.multiple_of(s * TOK, TOK), TOK)

    def remote(src, dst, ss, rs, dev):
        return pltpu.make_async_remote_copy(src_ref=src, dst_ref=dst, send_sem=ss, recv_sem=rs,
                                            device_id=dev, device_id_type=MESH)

    def exchange(h, what):
        dev = (d, a, h)
        if what == "k":
            return remote(ko.at[h], kb.at[rows(shard)], ksend.at[h], krecv.at[shard], dev)
        if what == "v":
            return remote(vo.at[h], vb.at[rows(shard)], vsend.at[h], vrecv.at[shard], dev)
        return remote(qo.at[h], qb.at[0, b], qsend.at[h], qrecv.at[0, b], dev)

    def send(what, heads):
        for h in heads:
            @pl.when(b != h)
            def _():
                exchange(h, what).start()

    def hop(s, what, level):
        dev = (d, level, b)
        if what == "k":
            return remote(kb.at[rows(s)], kb.at[rows(s)], kfs.at[s], krecv.at[s], dev)
        return remote(vb.at[rows(s)], vb.at[rows(s)], vfs.at[s], vrecv.at[s], dev)

    def wait_piece(s):
        hop(s, "k", a).wait_recv()
        hop(s, "v", a).wait_recv()

    def needed(s, level):
        return s >= NL * level - 11

    def pass_on(s, whats=("k", "v")):
        @pl.when(feeds & needed(s, a + 1))
        def _():
            for what in whats:
                hop(s, what, a + 1).start()

        @pl.when(donor)
        def _():
            for what in whats:
                hop(s, what, 2).start()

    def q_down(j):
        return remote(qb.at[0, j], qb.at[1, j], qfs.at[j], qrecv.at[1, j], (d, 2, b))

    def wait_q(slot, j):
        remote(qo.at[0], qb.at[slot, j], qsend.at[0], qrecv.at[slot, j], (d, a, b)).wait_recv()

    first_user = even | (a >= 1)

    xcopy.wait()

    def start_v():
        trig_copy.start()
        base_copy.start()
        for c in range(KCUT):
            cut(wv_hbm, wv, wvsem, KCUT, c).start()

    def start_q():
        for c in range(QCUT):
            cut(wq_hbm, wq, wqsem, QCUT, c).start()

    with jax.named_scope("k_proj"):
        k_f = project(wk, KCUT, [cut(wk_hbm, wk, wksem, KCUT, c) for c in range(KCUT)], NL, {1: start_v}, {})
    wo_copy = pltpu.make_async_copy(wo_hbm, wo, wosem)
    trig_copy.wait()
    base_copy.wait()
    cb, sb = base[0, pl.ds(shard, 1), :], base[1, pl.ds(shard, 1), :]
    cos = cb * trig[0] - sb * trig[1]
    sin = sb * trig[0] + cb * trig[1]
    for h in range(NL):
        ko[h, :, :HALF], ko[h, :, HALF:] = rotate(k_f, h, cos, sin)
    kb[rows(shard), :] = ko[b]
    with jax.named_scope("barrier"):
        pl.semaphore_wait(bar, 3 + one(a > 0) + one(a < NL - 1) + 3 * one(host) + one(a == 3)
                          + one((a == 3) & (odd == 1)))
    send("k", (0, 2))

    def relay(who, whats, js):
        @pl.when(who)
        def _():
            for j in js:
                for what in whats:
                    hop(a * NL + j, what, a).wait_recv()
                pass_on(a * NL + j, whats)

    @pl.when(first_user)
    def _():
        pass_on(shard, ("k",))

    with jax.named_scope("v_proj"):
        v_f = project(wv, KCUT, [cut(wv_hbm, wv, wvsem, KCUT, c) for c in range(KCUT)], NL, {1: start_q},
                      {2: lambda: relay(even, ("k",), (partner,))})
    for h in range(NL):
        vo[h] = v_f[:, h * HD:(h + 1) * HD].astype(BF)
    vb[rows(shard), :] = vo[b]
    send("v", (0, 2))
    send("k", (1, 3))
    send("v", (1, 3))

    @pl.when(first_user)
    def _():
        pass_on(shard, ("v",))

    def relay_1():
        relay(even, ("v",), (partner,))
        relay(even, ("k",), (far, far2))
        relay((odd == 1) & (a >= 1), ("k", "v"), (partner,))

    with jax.named_scope("q_proj"):
        q_f = project(wq, QCUT, [cut(wq_hbm, wq, wqsem, QCUT, c) for c in range(QCUT)], 2 * NL,
                      {1: wo_copy.start}, {1: relay_1})
    for h in range(2 * NL):
        qo[h // 2, h % 2, :, :HALF], qo[h // 2, h % 2, :, HALF:] = rotate(q_f, h, cos, sin)
    qb[0, b] = qo[b]
    send("q", (0, 2, 1, 3))

    def wide(t, n):
        return jnp.concatenate([t] * (n // LANES), axis=1)

    def attend(slot, i, level, key0, n, masked, first=False, last=False):
        keys = pl.ds(pl.multiple_of(key0, 64), n)
        k, v = kb[keys, :], vb[keys, :]
        scores = []
        for g in range(2):
            s = lax.dot_general(qb[slot, i, g], k, (((1,), (1,)), ((), ())), preferred_element_type=F32)
            if masked:
                gap = (lax.broadcasted_iota(jnp.int32, (TOK, n), 0) - lax.broadcasted_iota(jnp.int32, (TOK, n), 1)
                       + (level * LVL + i * TOK - key0))
                s = jnp.where((gap >= 0) & (gap < WINDOW), s, NEG)
            scores.append(s)
        for g, s in enumerate(scores):
            top = jnp.max(s, axis=-1, keepdims=True)
            if first:
                new = jnp.broadcast_to(top, (TOK, LANES))
            else:
                old = m_s[slot, i, g]
                new = jnp.maximum(old, top)
                fix = jnp.exp2((old - new) * SCALE)
            p = jnp.exp2((s - wide(new, n)) * SCALE)
            total = jnp.broadcast_to(jnp.sum(p, axis=-1, keepdims=True), (TOK, LANES))
            out = jnp.dot(p.astype(BF), v, preferred_element_type=F32)
            if not first:
                total = total + l_s[slot, i, g] * fix
                out = out + acc[slot, i, g] * wide(fix, HD)
            if last:
                osend[slot, i, :, g * HD:(g + 1) * HD] = (out * wide(1.0 / total, HD)).astype(BF)
            else:
                m_s[slot, i, g] = new
                l_s[slot, i, g] = total
                acc[slot, i, g] = out
        if last:
            give(slot, i)

    def loop(lo, hi, fn):
        def step(i, carry):
            fn(i)
            return carry
        lax.fori_loop(lo, hi, step, 0)

    def head_cols():
        return pl.ds(pl.multiple_of(b * 2 * HD, 2 * HD), 2 * HD)

    def back_to(slot, i):
        return remote(osend.at[slot, i], ob.at[:, head_cols()], os_sem.at[slot, i], orecv.at[b], (d, a + slot, i))

    def give(slot, i):
        if slot == 1:
            back_to(1, i).start()
            return

        @pl.when(b != i)
        def _():
            back_to(0, i).start()

        @pl.when(b == i)
        def _():
            ob[:, head_cols()] = osend[0, i]

    def finish(slot, i):
        for g in range(2):
            osend[slot, i, :, g * HD:(g + 1) * HD] = (acc[slot, i, g] * wide(1.0 / l_s[slot, i, g], HD)).astype(BF)
        give(slot, i)

    def turn(t):
        return lax.rem(away0 + t, NL)

    low = (a - 1) * NL

    def own_block(slot):
        with jax.named_scope("own_att"):
            for i in range(NL):
                attend(slot, i, a + slot, (a + slot) * LVL, OWN_KEYS[i], True, first=True)

    def take(s):
        wait_piece(s)
        pass_on(s)

    relay(even, ("v",), (far, far2))

    @pl.when(even & (a == 0))
    def _():
        pl.semaphore_signal(go, inc=1, device_id=(d, a, partner), device_id_type=MESH)

    @pl.when((odd == 1) & (a == 0))
    def _():
        with jax.named_scope("go_wait"):
            pl.semaphore_wait(go, 1)
        pass_on(shard)
        take(a * NL + partner)

    relay(odd == 1, ("k", "v"), (far, far2))

    @pl.when((even & (a == 1)) | ((odd == 1) & (a >= 2)))
    def _():
        with jax.named_scope("take_low"):
            for j in (b, partner, far, far2):
                take(low + j)

    with jax.named_scope("own_q"):
        for j in (partner, far, far2):
            @pl.when(jnp.logical_not(donor))
            def _():
                wait_q(0, j)

    @pl.when(donor)
    def _():
        q_down(b).start()
        for j in (partner, far, far2):
            wait_q(0, j)
            q_down(j).start()

    @pl.when(jnp.logical_not(donor))
    def _():
        own_block(0)

        @pl.when(a == 0)
        def _():
            loop(0, NL, lambda t: finish(0, turn(t)))

        @pl.when(a > 0)
        def _():
            @pl.when(host)
            def _():
                with jax.named_scope("take1"):
                    for j in (b, partner, far, far2):
                        take(low + j)

            @pl.when((a == 1) & (odd == 1))
            def _():
                with jax.named_scope("go_wait"):
                    pl.semaphore_wait(go, 1)
                with jax.named_scope("take_low"):
                    for j in (3, 2, 1, 0):
                        take(low + j)

            @pl.when(a == 1)
            def _():
                loop(0, NL, lambda t: attend(0, turn(t), a, 0, LVL, False, last=True))

                @pl.when(even)
                def _():
                    for j in (shard, NL + partner, NL + far, NL + far2, b, partner):
                        for what in ("k", "v"):
                            hop(j, what, 2).wait_send()
                    pl.semaphore_signal(go, inc=1, device_id=(d, a, partner), device_id_type=MESH)

            @pl.when(a > 1)
            def _():
                with jax.named_scope("att1"):
                    loop(0, NL, lambda i: attend(0, i, a, (a - 1) * LVL, LVL, False))

        @pl.when(host)
        def _():
            with jax.named_scope("host_wait"):
                for j in range(NL):
                    wait_piece(3 * NL + j)
                for j in range(NL):
                    wait_q(1, j)
            own_block(1)
            with jax.named_scope("host_att"):
                loop(0, NL, lambda i: attend(1, i, 3, 2 * LVL, LVL, False))
                loop(0, NL, lambda i: attend(1, i, 3, LVL, LVL, True))
            with jax.named_scope("take2"):
                for j in (b, partner, far, far2):
                    take(j)
            with jax.named_scope("att2"):
                loop(0, NL, lambda t: attend(0, turn(t), a, 0, LVL, True, last=True))
            with jax.named_scope("host_last"):
                finish(1, NL - 1)
                loop(0, NL - 1, lambda i: attend(1, i, 3, 256, 512, True, last=True))

        @pl.when((a >= 2) & (odd == 1))
        def _():
            lvl2 = (a - 2) * NL
            with jax.named_scope("take2a"):
                take(lvl2 + 3)
                take(lvl2 + 2)
            with jax.named_scope("att2a"):
                loop(0, 2, lambda i: attend(0, i, a, lvl2 * TOK + 2 * TOK, 2 * TOK, False))
            with jax.named_scope("take2b"):
                take(lvl2 + 1)
            with jax.named_scope("att2b"):
                loop(2, NL, lambda i: attend(0, i, a, lvl2 * TOK + 2 * TOK, 2 * TOK, False))
            with jax.named_scope("take2c"):
                take(lvl2)

        @pl.when((a == 2) & (odd == 1))
        def _():
            with jax.named_scope("att2c"):
                loop(0, NL, lambda t: attend(0, turn(t), a, 0, 2 * TOK, True, last=True))

        @pl.when((a == 3) & (odd == 1))
        def _():
            with jax.named_scope("att2c"):
                loop(0, NL, lambda i: attend(0, i, a, LVL, 2 * TOK, True))
            finish(0, NL - 1)
            with jax.named_scope("take3"):
                wait_piece(3)
                wait_piece(2)
            with jax.named_scope("att3"):
                attend(0, 2, a, 2 * TOK, 2 * TOK, True, last=True)
                attend(0, 1, a, 2 * TOK, 2 * TOK, True, last=True)
                attend(0, 0, a, 2 * TOK, 2 * TOK, True)
            with jax.named_scope("take3b"):
                wait_piece(1)
            with jax.named_scope("att3b"):
                attend(0, 0, a, 256, 128, True, last=True)

    def take_o(h):
        @pl.when((b != h) | ((a == 3) & (h % 2 == 0)))
        def _():
            remote(osend.at[0, 0], ob.at[:, pl.ds(h * 2 * HD, 2 * HD)], os_sem.at[0, 0], orecv.at[h], (d, a, b)).wait_recv()

    def project_o(h, cols):
        return jnp.dot(ob[:, h * 2 * HD:(h + 1) * 2 * HD], wo[pl.ds(h * 2 * HD, 2 * HD), cols],
                       preferred_element_type=F32)

    tiles = [pl.ds(t * YCOLS, YCOLS) for t in range(DM // YCOLS)]
    with jax.named_scope("o_even"):
        take_o(0)
        take_o(2)
    wo_copy.wait()
    for cols in tiles:
        y_acc[:, cols] = project_o(0, cols) + project_o(2, cols)
    with jax.named_scope("o_odd"):
        for h in (1, 3):
            @pl.when(b // 2 == h // 2)
            def _():
                take_o(h)
                for cols in tiles:
                    y_acc[:, cols] += project_o(h, cols)
        for h in (1, 3):
            @pl.when(b // 2 != h // 2)
            def _():
                take_o(h)
                for t, cols in enumerate(tiles):
                    y_tile[:, cols] = (y_acc[:, cols] + project_o(h, cols)).astype(BF)
                    pltpu.make_async_copy(y_tile.at[:, cols], y_ref.at[:, cols], ysem.at[t]).start()
    y_copies = [pltpu.make_async_copy(y_tile.at[:, cols], y_ref.at[:, cols], ysem.at[t]) for t, cols in enumerate(tiles)]

    for h in range(NL):
        @pl.when(b != h)
        def _():
            for what in ("k", "v", "q"):
                exchange(h, what).wait_send()

        @pl.when((b != h) & jnp.logical_not(donor))
        def _():
            back_to(0, h).wait_send()

        @pl.when(host)
        def _():
            back_to(1, h).wait_send()

        @pl.when(donor)
        def _():
            q_down(h).wait_send()
            for what in ("k", "v"):
                hop(3 * NL + h, what, 2).wait_send()

    for s in range(12):
        waited = even & (a == 1) & ((s >= NL) | (s // 2 == b // 2))

        @pl.when(feeds & (s < NL * (a + 1)) & needed(s, a + 1) & jnp.logical_not(waited))
        def _():
            for what in ("k", "v"):
                hop(s, what, a + 1).wait_send()
    for c in y_copies:
        c.wait()


def solution(mesh):
    def local_fn(hidden, w_q, w_k, w_v, w_o):
        freq = ROPE_BASE ** (-np.arange(HALF) * 2.0 / HD)
        steps, starts = np.arange(TOK)[:, None] * freq, (np.arange(NL * NL) * TOK)[:, None] * freq
        trig = jnp.asarray(np.stack([np.cos(steps), np.sin(steps)]), F32)
        base = jnp.asarray(np.stack([np.cos(starts), np.sin(starts)]), F32)
        hbm = pl.BlockSpec(memory_space=pl.ANY)
        dma = pltpu.SemaphoreType.DMA
        return pl.pallas_call(
            body,
            out_shape=jax.ShapeDtypeStruct((TOK, DM), BF),
            in_specs=[hbm] * 7,
            out_specs=hbm,
            scratch_shapes=[
                pltpu.VMEM((2, TOK, HALF), F32), pltpu.VMEM((2, NL * NL, HALF), F32),
                pltpu.VMEM((TOK, DM), BF), pltpu.VMEM((DM, 2 * NL, HD), BF), pltpu.VMEM((DM, NL, HD), BF),
                pltpu.VMEM((DM, NL, HD), BF), pltpu.VMEM((2 * NL * HD, DM), BF),
                pltpu.VMEM((NL, TOK, HD), BF), pltpu.VMEM((NL, TOK, HD), BF), pltpu.VMEM((NL, 2, TOK, HD), BF),
                pltpu.VMEM((16 * TOK, HD), BF), pltpu.VMEM((16 * TOK, HD), BF),
                pltpu.VMEM((2, NL, 2, TOK, HD), BF), pltpu.VMEM((TOK, 2 * NL * HD), BF),
                pltpu.VMEM((2, NL, TOK, 2 * HD), BF), pltpu.VMEM((2, NL, 2, TOK, HD), F32),
                pltpu.VMEM((2, NL, 2, TOK, LANES), F32), pltpu.VMEM((2, NL, 2, TOK, LANES), F32),
                pltpu.VMEM((TOK, DM), F32), pltpu.VMEM((TOK, DM), BF),
                dma((2,)), dma(()), dma((KCUT,)), dma((KCUT,)), dma((QCUT,)), dma(()),
                dma((16,)), dma((16,)), dma((16,)), dma((16,)), dma((NL,)),
                dma((NL,)), dma((NL,)), dma((NL,)), dma((2, NL)), dma((2, NL)), dma((NL,)), dma((DM // YCOLS,)),
                pltpu.SemaphoreType.REGULAR,
            ],
            compiler_params=pltpu.CompilerParams(collective_id=0, has_side_effects=True,
                                                 vmem_limit_bytes=63 * 2 ** 20),
        )(trig, base, hidden, w_q, w_k, w_v, w_o.reshape(2 * NL * HD, DM))

    return jax.shard_map(local_fn, mesh=mesh,
                         in_specs=(P(("dp", "cpo", "cpi"), None), P(), P(), P(), P()),
                         out_specs=P(("dp", "cpo", "cpi"), None), check_vma=False)
```

```python
import jax
import jax.numpy as jnp
import numpy as np
from jax import lax
from jax.experimental import pallas as pl
from jax.experimental.pallas import tpu as pltpu
from jax.sharding import PartitionSpec as P

WINDOW = 2048
ROPE_BASE = 10000.0
MESH = pl.DeviceIdType.MESH
NL = 4
TOK = 192
LVL = NL * TOK
DM = 2560
HD = 256
HALF = HD // 2
LANES = 128
YCOLS = 512
NEG = -1e30
SCALE = HD ** -0.5 * 1.4426950408889634
KCUT = 4
QCUT = 4
OWN_KEYS = (256, 384, 640, 768)
F32, BF = jnp.float32, jnp.bfloat16


def body(trig_hbm, base_hbm, x_hbm, wq_hbm, wk_hbm, wv_hbm, wo_hbm, y_ref,
         trig, base, x, wq, wk, wv, wo, ko, vo, qo, kb, vb, qb, ob, osend, acc, m_s, l_s, y_acc,
         tsem, xsem, wksem, wvsem, wqsem, wosem, krecv, vrecv, kfs, vfs, qfs, ksend, vsend, qsend, qrecv,
         os_sem, orecv, go):
    d, a, b = lax.axis_index("dp"), lax.axis_index("cpo"), lax.axis_index("cpi")
    shard = a * NL + b
    odd = lax.rem(b, 2)
    even = odd == 0
    partner = b + 1 - 2 * odd
    far = lax.rem(b + 2, NL)
    far2 = lax.rem(partner + 2, NL)
    near0 = b - odd
    away0 = 2 - near0
    donor = (a == 3) & even
    host = (a == 2) & even
    feeds = (a < 2) | ((a == 2) & (odd == 1))

    def cut(src, dst, sem, n, c):
        r = DM // n
        return pltpu.make_async_copy(src.at[pl.ds(c * r, r)], dst.at[pl.ds(c * r, r)], sem.at[c])

    xcopy = pltpu.make_async_copy(x_hbm, x, xsem)
    xcopy.start()
    cut(wk_hbm, wk, wksem, KCUT, 0).start()
    trig_copy = pltpu.make_async_copy(trig_hbm, trig, tsem.at[0])
    base_copy = pltpu.make_async_copy(base_hbm, base, tsem.at[1])

    bar = pltpu.get_barrier_semaphore()

    def greet(level, other):
        pl.semaphore_signal(bar, inc=1, device_id=(d, level, other), device_id_type=MESH)

    for j in (partner, far, far2):
        greet(a, j)

    @pl.when(a > 0)
    def _():
        greet(a - 1, b)

    @pl.when(a < NL - 1)
    def _():
        greet(a + 1, b)

    @pl.when(host)
    def _():
        for j in (partner, far, far2):
            greet(3, j)

    @pl.when(a == 3)
    def _():
        greet(2, lax.rem(b + 2 - odd, NL))

    @pl.when((a == 3) & (odd == 1))
    def _():
        greet(2, b - 1)

    def one(p):
        return p.astype(jnp.int32)

    def project(w, n, copies, heads, fetch, between):
        total = None
        for c in range(n):
            copies[c].wait()
            if c in fetch:
                fetch[c]()
            r = DM // n
            part = jnp.dot(x[:, c * r:(c + 1) * r], w[pl.ds(c * r, r)].reshape(r, heads * HD),
                           preferred_element_type=F32)
            total = part if total is None else total + part
            if c in between:
                between[c]()
        return total

    def rotate(t, h, cos, sin):
        lo, hi = t[:, h * HD:h * HD + HALF], t[:, h * HD + HALF:(h + 1) * HD]
        return (lo * cos - hi * sin).astype(BF), (hi * cos + lo * sin).astype(BF)

    def rows(s):
        return pl.ds(pl.multiple_of(s * TOK, TOK), TOK)

    def remote(src, dst, ss, rs, dev):
        return pltpu.make_async_remote_copy(src_ref=src, dst_ref=dst, send_sem=ss, recv_sem=rs,
                                            device_id=dev, device_id_type=MESH)

    def exchange(h, what):
        dev = (d, a, h)
        if what == "k":
            return remote(ko.at[h], kb.at[rows(shard)], ksend.at[h], krecv.at[shard], dev)
        if what == "v":
            return remote(vo.at[h], vb.at[rows(shard)], vsend.at[h], vrecv.at[shard], dev)
        return remote(qo.at[h], qb.at[0, b], qsend.at[h], qrecv.at[0, b], dev)

    def send(what, early=True, late=True):
        for h in (0, 2, 1, 3):
            soon = (partner == h) | (h % 2 == 0)
            if early:
                @pl.when((b != h) & soon)
                def _():
                    exchange(h, what).start()
            if late:
                @pl.when((b != h) & jnp.logical_not(soon))
                def _():
                    exchange(h, what).start()

    def hop(s, what, level):
        dev = (d, level, b)
        if what == "k":
            return remote(kb.at[rows(s)], kb.at[rows(s)], kfs.at[s], krecv.at[s], dev)
        return remote(vb.at[rows(s)], vb.at[rows(s)], vfs.at[s], vrecv.at[s], dev)

    def wait_piece(s):
        hop(s, "k", a).wait_recv()
        hop(s, "v", a).wait_recv()

    def needed(s, level):
        return s >= NL * level - 11

    def pass_on(s, whats=("k", "v")):
        @pl.when(feeds & needed(s, a + 1))
        def _():
            for what in whats:
                hop(s, what, a + 1).start()

        @pl.when(donor)
        def _():
            for what in whats:
                hop(s, what, 2).start()

    def q_down(j):
        return remote(qb.at[0, j], qb.at[1, j], qfs.at[j], qrecv.at[1, j], (d, 2, b))

    def wait_q(slot, j):
        remote(qo.at[0], qb.at[slot, j], qsend.at[0], qrecv.at[slot, j], (d, a, b)).wait_recv()

    first_user = even | (a >= 1)

    xcopy.wait()
    for c in range(1, KCUT):
        cut(wk_hbm, wk, wksem, KCUT, c).start()

    def start_v():
        trig_copy.start()
        base_copy.start()
        for c in range(KCUT):
            cut(wv_hbm, wv, wvsem, KCUT, c).start()

    def start_q():
        for c in range(QCUT):
            cut(wq_hbm, wq, wqsem, QCUT, c).start()

    with jax.named_scope("k_proj"):
        k_f = project(wk, KCUT, [cut(wk_hbm, wk, wksem, KCUT, c) for c in range(KCUT)], NL, {1: start_v}, {})
    wo_copy = pltpu.make_async_copy(wo_hbm, wo, wosem)
    trig_copy.wait()
    base_copy.wait()
    cb, sb = base[0, pl.ds(shard, 1), :], base[1, pl.ds(shard, 1), :]
    cos = cb * trig[0] - sb * trig[1]
    sin = sb * trig[0] + cb * trig[1]
    for h in range(NL):
        ko[h, :, :HALF], ko[h, :, HALF:] = rotate(k_f, h, cos, sin)
    kb[rows(shard), :] = ko[b]
    with jax.named_scope("barrier"):
        pl.semaphore_wait(bar, 3 + one(a > 0) + one(a < NL - 1) + 3 * one(host) + one(a == 3)
                          + one((a == 3) & (odd == 1)))
    send("k", late=False)

    def relay(who, whats, js):
        @pl.when(who)
        def _():
            for j in js:
                for what in whats:
                    hop(a * NL + j, what, a).wait_recv()
                pass_on(a * NL + j, whats)

    @pl.when(first_user)
    def _():
        pass_on(shard, ("k",))

    with jax.named_scope("v_proj"):
        v_f = project(wv, KCUT, [cut(wv_hbm, wv, wvsem, KCUT, c) for c in range(KCUT)], NL, {1: start_q},
                      {2: lambda: relay(even | (a >= 1), ("k",), (partner,))})
    for h in range(NL):
        vo[h] = v_f[:, h * HD:(h + 1) * HD].astype(BF)
    vb[rows(shard), :] = vo[b]
    send("v", late=False)
    send("k", early=False)
    send("v", early=False)

    @pl.when(first_user)
    def _():
        pass_on(shard, ("v",))

    def relay_1():
        relay(even, ("v",), (partner,))
        relay(even, ("k",), (far, far2))
        relay((odd == 1) & (a >= 1), ("v",), (partner,))

    with jax.named_scope("q_proj"):
        q_f = project(wq, QCUT, [cut(wq_hbm, wq, wqsem, QCUT, c) for c in range(QCUT)], 2 * NL,
                      {1: wo_copy.start}, {1: relay_1})
    for h in range(2 * NL):
        qo[h // 2, h % 2, :, :HALF], qo[h // 2, h % 2, :, HALF:] = rotate(q_f, h, cos, sin)
    qb[0, b] = qo[b]
    send("q")

    def wide(t, n):
        return jnp.concatenate([t] * (n // LANES), axis=1)

    def attend(slot, i, level, key0, n, masked, first=False, last=False):
        keys = pl.ds(pl.multiple_of(key0, 64), n)
        k, v = kb[keys, :], vb[keys, :]
        scores = []
        for g in range(2):
            s = lax.dot_general(qb[slot, i, g], k, (((1,), (1,)), ((), ())), preferred_element_type=F32)
            if masked:
                gap = (lax.broadcasted_iota(jnp.int32, (TOK, n), 0) - lax.broadcasted_iota(jnp.int32, (TOK, n), 1)
                       + (level * LVL + i * TOK - key0))
                s = jnp.where((gap >= 0) & (gap < WINDOW), s, NEG)
            scores.append(s)
        for g, s in enumerate(scores):
            top = jnp.max(s, axis=-1, keepdims=True)
            if first:
                new = jnp.broadcast_to(top, (TOK, LANES))
            else:
                old = m_s[slot, i, g]
                new = jnp.maximum(old, top)
                fix = jnp.exp2((old - new) * SCALE)
            p = jnp.exp2((s - wide(new, n)) * SCALE)
            total = jnp.broadcast_to(jnp.sum(p, axis=-1, keepdims=True), (TOK, LANES))
            out = jnp.dot(p.astype(BF), v, preferred_element_type=F32)
            if not first:
                total = total + l_s[slot, i, g] * fix
                out = out + acc[slot, i, g] * wide(fix, HD)
            if last:
                osend[slot, i, :, g * HD:(g + 1) * HD] = (out * wide(1.0 / total, HD)).astype(BF)
            else:
                m_s[slot, i, g] = new
                l_s[slot, i, g] = total
                acc[slot, i, g] = out
        if last:
            give(slot, i)

    def loop(lo, hi, fn):
        def step(i, carry):
            fn(i)
            return carry
        lax.fori_loop(lo, hi, step, 0)

    def head_cols():
        return pl.ds(pl.multiple_of(b * 2 * HD, 2 * HD), 2 * HD)

    def back_to(slot, i):
        return remote(osend.at[slot, i], ob.at[:, head_cols()], os_sem.at[slot, i], orecv.at[b], (d, a + slot, i))

    def give(slot, i):
        if slot == 1:
            back_to(1, i).start()
            return

        @pl.when(b != i)
        def _():
            back_to(0, i).start()

        @pl.when(b == i)
        def _():
            ob[:, head_cols()] = osend[0, i]

    def finish(slot, i):
        for g in range(2):
            osend[slot, i, :, g * HD:(g + 1) * HD] = (acc[slot, i, g] * wide(1.0 / l_s[slot, i, g], HD)).astype(BF)
        give(slot, i)

    def turn(t):
        return lax.rem(away0 + t, NL)

    low = (a - 1) * NL

    def own_block(slot):
        with jax.named_scope("own_att"):
            for i in range(NL):
                attend(slot, i, a + slot, (a + slot) * LVL, OWN_KEYS[i], True, first=True)

    def take(s):
        wait_piece(s)
        pass_on(s)

    relay(even, ("v",), (far, far2))

    @pl.when(even & (a == 0))
    def _():
        pl.semaphore_signal(go, inc=1, device_id=(d, a, partner), device_id_type=MESH)

    @pl.when((odd == 1) & (a == 0))
    def _():
        with jax.named_scope("go_wait"):
            pl.semaphore_wait(go, 1)
        pass_on(shard)
        take(a * NL + partner)

    relay(odd == 1, ("k", "v"), (far, far2))

    @pl.when((even & (a == 1)) | ((odd == 1) & (a >= 2)))
    def _():
        with jax.named_scope("take_low"):
            for j in (b, partner, far, far2):
                take(low + j)

    with jax.named_scope("own_q"):
        @pl.when(jnp.logical_not(donor))
        def _():
            wait_q(0, partner)

        @pl.when(jnp.logical_not(donor | host))
        def _():
            wait_q(0, far)
            wait_q(0, far2)

    @pl.when(donor)
    def _():
        q_down(b).start()
        for j in (partner, far, far2):
            wait_q(0, j)
            q_down(j).start()

    def chip_block(slot, here):
        for i in range(0, NL, 2):
            @pl.when((near0 == i) == here)
            def _():
                for j in (i, i + 1):
                    attend(slot, j, a + slot, (a + slot) * LVL, OWN_KEYS[j], True, first=True)

    def pair(start, fn):
        loop(0, 2, lambda t: fn(start + t))

    @pl.when(host)
    def _():
        with jax.named_scope("take1"):
            for j in (b, partner, far, far2):
                take(low + j)
        for here in (True, False):
            first = near0 if here else away0
            with jax.named_scope("hq0"):
                if not here:
                    wait_q(0, far)
                    wait_q(0, far2)
            with jax.named_scope("job0"):
                chip_block(0, here)
                pair(first, lambda i: attend(0, i, a, (a - 1) * LVL, LVL, False))
            with jax.named_scope("hq1"):
                if here:
                    for j in range(NL):
                        wait_piece(3 * NL + j)
                for j in ((b, partner) if here else (far, far2)):
                    wait_q(1, j)
            with jax.named_scope("job1"):
                chip_block(1, here)
                pair(first, lambda i: attend(1, i, 3, 2 * LVL, LVL, False))
                pair(first, lambda i: attend(1, i, 3, LVL, LVL, True))
        with jax.named_scope("take2"):
            for j in (b, partner, far, far2):
                take(j)
        with jax.named_scope("host_last"):
            finish(1, NL - 1)
            loop(0, NL - 1, lambda i: attend(1, i, 3, 256, 512, True, last=True))
        with jax.named_scope("att2"):
            loop(0, NL, lambda t: attend(0, turn(t), a, 0, LVL, True, last=True))

    @pl.when(jnp.logical_not(donor | host))
    def _():
        own_block(0)

        @pl.when(a == 0)
        def _():
            loop(0, NL, lambda t: finish(0, turn(t)))

        @pl.when(a > 0)
        def _():
            @pl.when((a == 1) & (odd == 1))
            def _():
                with jax.named_scope("go_wait"):
                    pl.semaphore_wait(go, 1)
                with jax.named_scope("take_low"):
                    for j in (3, 2, 1, 0):
                        take(low + j)

            @pl.when(a == 1)
            def _():
                loop(0, NL, lambda t: attend(0, turn(t), a, 0, LVL, False, last=True))

                @pl.when(even)
                def _():
                    for j in (shard, NL + partner, NL + far, NL + far2, b, partner):
                        for what in ("k", "v"):
                            hop(j, what, 2).wait_send()
                    pl.semaphore_signal(go, inc=1, device_id=(d, a, partner), device_id_type=MESH)

            @pl.when(a > 1)
            def _():
                with jax.named_scope("att1"):
                    loop(0, NL, lambda i: attend(0, i, a, (a - 1) * LVL, LVL, False))

        @pl.when((a >= 2) & (odd == 1))
        def _():
            lvl2 = (a - 2) * NL
            with jax.named_scope("take2a"):
                take(lvl2 + 3)
                take(lvl2 + 2)
            with jax.named_scope("att2a"):
                loop(0, 2, lambda i: attend(0, i, a, lvl2 * TOK + 2 * TOK, 2 * TOK, False))
            with jax.named_scope("take2b"):
                take(lvl2 + 1)
            with jax.named_scope("att2b"):
                loop(2, NL, lambda i: attend(0, i, a, lvl2 * TOK + 2 * TOK, 2 * TOK, False))
            with jax.named_scope("take2c"):
                take(lvl2)

        @pl.when((a == 2) & (odd == 1))
        def _():
            with jax.named_scope("att2c"):
                loop(0, NL, lambda t: attend(0, turn(t), a, 0, 2 * TOK, True, last=True))

        @pl.when((a == 3) & (odd == 1))
        def _():
            with jax.named_scope("att2c"):
                loop(0, NL, lambda i: attend(0, i, a, LVL, 2 * TOK, True))
            finish(0, NL - 1)
            with jax.named_scope("take3"):
                wait_piece(3)
                wait_piece(2)
            with jax.named_scope("att3"):
                attend(0, 2, a, 2 * TOK, 2 * TOK, True, last=True)
                attend(0, 1, a, 2 * TOK, 2 * TOK, True, last=True)
                attend(0, 0, a, 2 * TOK, 2 * TOK, True)
            with jax.named_scope("take3b"):
                wait_piece(1)
            with jax.named_scope("att3b"):
                attend(0, 0, a, 256, 128, True, last=True)

    def take_o(h):
        @pl.when((b != h) | ((a == 3) & (h % 2 == 0)))
        def _():
            remote(osend.at[0, 0], ob.at[:, pl.ds(h * 2 * HD, 2 * HD)], os_sem.at[0, 0], orecv.at[h], (d, a, b)).wait_recv()

    def project_o(h, cols):
        return jnp.dot(ob[:, h * 2 * HD:(h + 1) * 2 * HD], wo[pl.ds(h * 2 * HD, 2 * HD), cols],
                       preferred_element_type=F32)

    tiles = [pl.ds(t * YCOLS, YCOLS) for t in range(DM // YCOLS)]
    with jax.named_scope("o_even"):
        take_o(0)
        take_o(2)
    wo_copy.wait()
    for cols in tiles:
        y_acc[:, cols] = project_o(0, cols) + project_o(2, cols)
    with jax.named_scope("o_odd"):
        for h in (1, 3):
            @pl.when(b // 2 == h // 2)
            def _():
                take_o(h)
                for cols in tiles:
                    y_acc[:, cols] += project_o(h, cols)
        for h in (1, 3):
            @pl.when(b // 2 != h // 2)
            def _():
                take_o(h)
                for cols in tiles:
                    y_ref[:, cols] = (y_acc[:, cols] + project_o(h, cols)).astype(BF)

    for h in range(NL):
        @pl.when(b != h)
        def _():
            for what in ("k", "v", "q"):
                exchange(h, what).wait_send()

        @pl.when((b != h) & jnp.logical_not(donor))
        def _():
            back_to(0, h).wait_send()

        @pl.when(host)
        def _():
            back_to(1, h).wait_send()

        @pl.when(donor)
        def _():
            q_down(h).wait_send()
            for what in ("k", "v"):
                hop(3 * NL + h, what, 2).wait_send()

    for s in range(12):
        waited = even & (a == 1) & ((s >= NL) | (s // 2 == b // 2))

        @pl.when(feeds & (s < NL * (a + 1)) & needed(s, a + 1) & jnp.logical_not(waited))
        def _():
            for what in ("k", "v"):
                hop(s, what, a + 1).wait_send()


def solution(mesh):
    def local_fn(hidden, w_q, w_k, w_v, w_o):
        freq = ROPE_BASE ** (-np.arange(HALF) * 2.0 / HD)
        steps, starts = np.arange(TOK)[:, None] * freq, (np.arange(NL * NL) * TOK)[:, None] * freq
        trig = jnp.asarray(np.stack([np.cos(steps), np.sin(steps)]), F32)
        base = jnp.asarray(np.stack([np.cos(starts), np.sin(starts)]), F32)
        hbm = pl.BlockSpec(memory_space=pl.ANY)
        dma = pltpu.SemaphoreType.DMA
        return pl.pallas_call(
            body,
            out_shape=jax.ShapeDtypeStruct((TOK, DM), BF),
            in_specs=[hbm] * 7,
            out_specs=pl.BlockSpec(memory_space=pltpu.VMEM),
            scratch_shapes=[
                pltpu.VMEM((2, TOK, HALF), F32), pltpu.VMEM((2, NL * NL, HALF), F32),
                pltpu.VMEM((TOK, DM), BF), pltpu.VMEM((DM, 2 * NL, HD), BF), pltpu.VMEM((DM, NL, HD), BF),
                pltpu.VMEM((DM, NL, HD), BF), pltpu.VMEM((2 * NL * HD, DM), BF),
                pltpu.VMEM((NL, TOK, HD), BF), pltpu.VMEM((NL, TOK, HD), BF), pltpu.VMEM((NL, 2, TOK, HD), BF),
                pltpu.VMEM((16 * TOK, HD), BF), pltpu.VMEM((16 * TOK, HD), BF),
                pltpu.VMEM((2, NL, 2, TOK, HD), BF), pltpu.VMEM((TOK, 2 * NL * HD), BF),
                pltpu.VMEM((2, NL, TOK, 2 * HD), BF), pltpu.VMEM((2, NL, 2, TOK, HD), F32),
                pltpu.VMEM((2, NL, 2, TOK, LANES), F32), pltpu.VMEM((2, NL, 2, TOK, LANES), F32),
                pltpu.VMEM((TOK, DM), F32),
                dma((2,)), dma(()), dma((KCUT,)), dma((KCUT,)), dma((QCUT,)), dma(()),
                dma((16,)), dma((16,)), dma((16,)), dma((16,)), dma((NL,)),
                dma((NL,)), dma((NL,)), dma((NL,)), dma((2, NL)), dma((2, NL)), dma((NL,)),
                pltpu.SemaphoreType.REGULAR,
            ],
            compiler_params=pltpu.CompilerParams(collective_id=0, has_side_effects=True,
                                                 vmem_limit_bytes=63 * 2 ** 20),
        )(trig, base, hidden, w_q, w_k, w_v, w_o.reshape(2 * NL * HD, DM))

    return jax.shard_map(local_fn, mesh=mesh,
                         in_specs=(P(("dp", "cpo", "cpi"), None), P(), P(), P(), P()),
                         out_specs=P(("dp", "cpo", "cpi"), None), check_vma=False)
```

```python
import jax
import jax.numpy as jnp
import numpy as np
from jax import lax
from jax.experimental import pallas as pl
from jax.experimental.pallas import tpu as pltpu
from jax.sharding import PartitionSpec as P

WINDOW = 2048
ROPE_BASE = 10000.0
MESH = pl.DeviceIdType.MESH
NL = 4
TOK = 192
LVL = NL * TOK
DM = 2560
HD = 256
HALF = HD // 2
LANES = 128
NEG = -1e30
SCALE = HD ** -0.5 * 1.4426950408889634
KCUT = 4
QCUT = 4
OWN_KEYS = (256, 384, 640, 768)
F32, BF = jnp.float32, jnp.bfloat16


def body(trig_hbm, base_hbm, x_hbm, wq_hbm, wk_hbm, wv_hbm, wo_hbm, y_ref,
         trig, base, x, wq, wk, wv, wo, ko, vo, qo, kb, vb, qb, ob, osend, acc, m_s, l_s,
         tsem, xsem, wksem, wvsem, wqsem, wosem, krecv, vrecv, kfs, vfs, qfs, ksend, vsend, qsend, qrecv,
         os_sem, orecv, go):
    d, a, b = lax.axis_index("dp"), lax.axis_index("cpo"), lax.axis_index("cpi")
    shard = a * NL + b
    odd = lax.rem(b, 2)
    even = odd == 0
    partner = b + 1 - 2 * odd
    far = lax.rem(b + 2, NL)
    far2 = lax.rem(partner + 2, NL)
    near0 = b - odd
    away0 = 2 - near0
    donor = (a == 3) & even
    host = (a == 2) & even
    feeds = (a < 2) | ((a == 2) & (odd == 1))

    def cut(src, dst, sem, n, c):
        r = DM // n
        return pltpu.make_async_copy(src.at[pl.ds(c * r, r)], dst.at[pl.ds(c * r, r)], sem.at[c])

    xcopy = pltpu.make_async_copy(x_hbm, x, xsem)
    xcopy.start()
    cut(wk_hbm, wk, wksem, KCUT, 0).start()
    trig_copy = pltpu.make_async_copy(trig_hbm, trig, tsem.at[0])
    base_copy = pltpu.make_async_copy(base_hbm, base, tsem.at[1])

    bar = pltpu.get_barrier_semaphore()

    def greet(level, other):
        pl.semaphore_signal(bar, inc=1, device_id=(d, level, other), device_id_type=MESH)

    for j in (partner, far, far2):
        greet(a, j)

    @pl.when(a > 0)
    def _():
        greet(a - 1, b)

    @pl.when(a < NL - 1)
    def _():
        greet(a + 1, b)

    @pl.when(host)
    def _():
        for j in (partner, far, far2):
            greet(3, j)

    @pl.when(a == 3)
    def _():
        greet(2, lax.rem(b + 2 - odd, NL))

    @pl.when((a == 3) & (odd == 1))
    def _():
        greet(2, b - 1)

    def one(p):
        return p.astype(jnp.int32)

    def project(w, n, copies, heads, fetch, between):
        total = None
        for c in range(n):
            copies[c].wait()
            if c in fetch:
                fetch[c]()
            r = DM // n
            at = c * r % w.shape[0]
            part = jnp.dot(x[:, c * r:(c + 1) * r], w[pl.ds(at, r)].reshape(r, heads * HD),
                           preferred_element_type=F32)
            total = part if total is None else total + part
            if c in between:
                between[c]()
        return total

    def rotate(t, h, cos, sin):
        lo, hi = t[:, h * HD:h * HD + HALF], t[:, h * HD + HALF:(h + 1) * HD]
        return (lo * cos - hi * sin).astype(BF), (hi * cos + lo * sin).astype(BF)

    def rows(s):
        return pl.ds(pl.multiple_of(s * TOK, TOK), TOK)

    def remote(src, dst, ss, rs, dev):
        return pltpu.make_async_remote_copy(src_ref=src, dst_ref=dst, send_sem=ss, recv_sem=rs,
                                            device_id=dev, device_id_type=MESH)

    def exchange(h, what):
        dev = (d, a, h)
        if what == "k":
            return remote(ko.at[h], kb.at[rows(shard)], ksend.at[h], krecv.at[shard], dev)
        if what == "v":
            return remote(vo.at[h], vb.at[rows(shard)], vsend.at[h], vrecv.at[shard], dev)
        return remote(qo.at[h], qb.at[0, b], qsend.at[h], qrecv.at[0, b], dev)

    def send(what, early=True, late=True):
        for h in (0, 2, 1, 3):
            soon = (partner == h) | (h % 2 == 0)
            if early:
                @pl.when((b != h) & soon)
                def _():
                    exchange(h, what).start()
            if late:
                @pl.when((b != h) & jnp.logical_not(soon))
                def _():
                    exchange(h, what).start()

    def hop(s, what, level):
        dev = (d, level, b)
        if what == "k":
            return remote(kb.at[rows(s)], kb.at[rows(s)], kfs.at[s], krecv.at[s], dev)
        return remote(vb.at[rows(s)], vb.at[rows(s)], vfs.at[s], vrecv.at[s], dev)

    def wait_piece(s):
        hop(s, "k", a).wait_recv()
        hop(s, "v", a).wait_recv()

    def needed(s, level):
        return s >= NL * level - 11

    def pass_on(s, whats=("k", "v")):
        @pl.when(feeds & needed(s, a + 1))
        def _():
            for what in whats:
                hop(s, what, a + 1).start()

        @pl.when(donor)
        def _():
            for what in whats:
                hop(s, what, 2).start()

    def q_down(j):
        return remote(qb.at[0, j], qb.at[1, j], qfs.at[j], qrecv.at[1, j], (d, 2, b))

    def wait_q(slot, j):
        remote(qo.at[0], qb.at[slot, j], qsend.at[0], qrecv.at[slot, j], (d, a, b)).wait_recv()

    first_user = even | (a >= 1)

    xcopy.wait()
    for c in range(1, KCUT):
        cut(wk_hbm, wk, wksem, KCUT, c).start()

    def start_v():
        trig_copy.start()
        base_copy.start()
        for c in range(KCUT):
            cut(wv_hbm, wv, wvsem, KCUT, c).start()

    def cut_q(c):
        r = DM // QCUT
        return pltpu.make_async_copy(wq_hbm.at[pl.ds(c * r, r)], wq.at[pl.ds(c % 2 * r, r)], wqsem.at[c])

    def start_q():
        cut_q(0).start()
        cut_q(1).start()

    with jax.named_scope("k_proj"):
        k_f = project(wk, KCUT, [cut(wk_hbm, wk, wksem, KCUT, c) for c in range(KCUT)], NL, {1: start_v}, {})
    wo_copy = pltpu.make_async_copy(wo_hbm, wo, wosem)
    trig_copy.wait()
    base_copy.wait()
    cb, sb = base[0, pl.ds(shard, 1), :], base[1, pl.ds(shard, 1), :]
    cos = cb * trig[0] - sb * trig[1]
    sin = sb * trig[0] + cb * trig[1]
    for h in range(NL):
        ko[h, :, :HALF], ko[h, :, HALF:] = rotate(k_f, h, cos, sin)
    kb[rows(shard), :] = ko[b]
    with jax.named_scope("barrier"):
        pl.semaphore_wait(bar, 3 + one(a > 0) + one(a < NL - 1) + 3 * one(host) + one(a == 3)
                          + one((a == 3) & (odd == 1)))
    send("k", late=False)

    def relay(who, whats, js):
        @pl.when(who)
        def _():
            for j in js:
                for what in whats:
                    hop(a * NL + j, what, a).wait_recv()
                pass_on(a * NL + j, whats)

    @pl.when(first_user)
    def _():
        pass_on(shard, ("k",))

    with jax.named_scope("v_proj"):
        v_f = project(wv, KCUT, [cut(wv_hbm, wv, wvsem, KCUT, c) for c in range(KCUT)], NL, {1: start_q},
                      {2: lambda: relay(even | (a >= 1), ("k",), (partner,))})
    for h in range(NL):
        vo[h] = v_f[:, h * HD:(h + 1) * HD].astype(BF)
    vb[rows(shard), :] = vo[b]
    send("v", late=False)
    send("k", early=False)
    send("v", early=False)

    @pl.when(first_user)
    def _():
        pass_on(shard, ("v",))

    def relay_1():
        cut_q(3).start()
        relay(even, ("v",), (partner,))
        relay(even, ("k",), (far, far2))
        relay((odd == 1) & (a >= 1), ("v",), (partner,))

    with jax.named_scope("q_proj"):
        q_f = project(wq, QCUT, [cut_q(c) for c in range(QCUT)], 2 * NL,
                      {3: wo_copy.start}, {0: cut_q(2).start, 1: relay_1})
    for h in range(2 * NL):
        qo[h // 2, h % 2, :, :HALF], qo[h // 2, h % 2, :, HALF:] = rotate(q_f, h, cos, sin)
    qb[0, b] = qo[b]
    send("q")

    def wide(t, n):
        return jnp.concatenate([t] * (n // LANES), axis=1)

    def attend(slot, i, level, key0, n, masked, first=False, last=False):
        keys = pl.ds(pl.multiple_of(key0, 64), n)
        k, v = kb[keys, :], vb[keys, :]
        scores = []
        for g in range(2):
            s = lax.dot_general(qb[slot, i, g], k, (((1,), (1,)), ((), ())), preferred_element_type=F32)
            if masked:
                gap = (lax.broadcasted_iota(jnp.int32, (TOK, n), 0) - lax.broadcasted_iota(jnp.int32, (TOK, n), 1)
                       + (level * LVL + i * TOK - key0))
                s = jnp.where((gap >= 0) & (gap < WINDOW), s, NEG)
            scores.append(s)
        for g, s in enumerate(scores):
            top = jnp.max(s, axis=-1, keepdims=True)
            if first:
                new = jnp.broadcast_to(top, (TOK, LANES))
            else:
                old = m_s[slot, i, g]
                new = jnp.maximum(old, top)
                fix = jnp.exp2((old - new) * SCALE)
            p = jnp.exp2((s - wide(new, n)) * SCALE)
            total = jnp.broadcast_to(jnp.sum(p, axis=-1, keepdims=True), (TOK, LANES))
            out = jnp.dot(p.astype(BF), v, preferred_element_type=F32)
            if not first:
                total = total + l_s[slot, i, g] * fix
                out = out + acc[slot, i, g] * wide(fix, HD)
            if last:
                osend[slot, i, :, g * HD:(g + 1) * HD] = (out * wide(1.0 / total, HD)).astype(BF)
            else:
                m_s[slot, i, g] = new
                l_s[slot, i, g] = total
                acc[slot, i, g] = out
        if last:
            give(slot, i)

    def loop(lo, hi, fn):
        def step(i, carry):
            fn(i)
            return carry
        lax.fori_loop(lo, hi, step, 0)

    def head_cols():
        return pl.ds(pl.multiple_of(b * 2 * HD, 2 * HD), 2 * HD)

    def back_to(slot, i):
        return remote(osend.at[slot, i], ob.at[:, head_cols()], os_sem.at[slot, i], orecv.at[b], (d, a + slot, i))

    def give(slot, i):
        if slot == 1:
            back_to(1, i).start()
            return

        @pl.when(b != i)
        def _():
            back_to(0, i).start()

        @pl.when(b == i)
        def _():
            ob[:, head_cols()] = osend[0, i]

    def finish(slot, i):
        for g in range(2):
            osend[slot, i, :, g * HD:(g + 1) * HD] = (acc[slot, i, g] * wide(1.0 / l_s[slot, i, g], HD)).astype(BF)
        give(slot, i)

    def turn(t):
        return lax.rem(away0 + t, NL)

    low = (a - 1) * NL

    def own_block(slot):
        with jax.named_scope("own_att"):
            for i in range(NL):
                attend(slot, i, a + slot, (a + slot) * LVL, OWN_KEYS[i], True, first=True)

    def take(s):
        wait_piece(s)
        pass_on(s)

    relay(even, ("v",), (far, far2))

    @pl.when(even & (a == 0))
    def _():
        pl.semaphore_signal(go, inc=1, device_id=(d, a, partner), device_id_type=MESH)

    @pl.when((odd == 1) & (a == 0))
    def _():
        with jax.named_scope("go_wait"):
            pl.semaphore_wait(go, 1)
        pass_on(shard)
        take(a * NL + partner)

    relay(odd == 1, ("k", "v"), (far, far2))

    @pl.when((even & (a == 1)) | ((odd == 1) & (a >= 2)))
    def _():
        with jax.named_scope("take_low"):
            for j in (b, partner, far, far2):
                take(low + j)

    with jax.named_scope("own_q"):
        @pl.when(jnp.logical_not(donor))
        def _():
            wait_q(0, partner)

        @pl.when(jnp.logical_not(donor | host))
        def _():
            wait_q(0, far)
            wait_q(0, far2)

    @pl.when(donor)
    def _():
        q_down(b).start()
        for j in (partner, far, far2):
            wait_q(0, j)
            q_down(j).start()

    def chip_block(slot, here):
        for i in range(0, NL, 2):
            @pl.when((near0 == i) == here)
            def _():
                for j in (i, i + 1):
                    attend(slot, j, a + slot, (a + slot) * LVL, OWN_KEYS[j], True, first=True)

    def pair(start, fn):
        loop(0, 2, lambda t: fn(start + t))

    @pl.when(host)
    def _():
        def low_0(start):
            pair(start, lambda i: attend(0, i, a, (a - 1) * LVL, LVL, False))

        def low_1(start):
            pair(start, lambda i: attend(1, i, 3, LVL, LVL, True))

        def top_1(here, start):
            with jax.named_scope("hq1"):
                for j in ((b, partner) if here else (far, far2)):
                    wait_q(1, j)
            with jax.named_scope("top_1"):
                chip_block(1, here)
                pair(start, lambda i: attend(1, i, 3, 2 * LVL, LVL, False))

        with jax.named_scope("job0"):
            chip_block(0, True)
        with jax.named_scope("take1"):
            for j in (b, partner, far, far2):
                take(low + j)
        low_0(near0)
        with jax.named_scope("hq0"):
            wait_q(0, far)
            wait_q(0, far2)
        with jax.named_scope("job0"):
            chip_block(0, False)
            low_0(away0)
        with jax.named_scope("hkv1"):
            for j in range(NL):
                wait_piece(3 * NL + j)
        top_1(True, near0)
        low_1(near0)

        @pl.when(near0 == 2)
        def _():
            finish(1, NL - 1)

        top_1(False, away0)
        low_1(away0)

        @pl.when(near0 == 0)
        def _():
            finish(1, NL - 1)

        with jax.named_scope("take2"):
            for j in (b, partner, far, far2):
                take(j)
        with jax.named_scope("att2"):
            loop(0, NL, lambda t: attend(0, turn(t), a, 0, LVL, True, last=True))
        with jax.named_scope("host_last"):
            loop(0, NL - 1, lambda i: attend(1, i, 3, 256, 512, True, last=True))

    @pl.when(jnp.logical_not(donor | host))
    def _():
        own_block(0)

        @pl.when(a == 0)
        def _():
            loop(0, NL, lambda t: finish(0, turn(t)))

        @pl.when(a > 0)
        def _():
            @pl.when((a == 1) & (odd == 1))
            def _():
                with jax.named_scope("go_wait"):
                    pl.semaphore_wait(go, 1)
                with jax.named_scope("take_low"):
                    for j in (3, 2, 1, 0):
                        take(low + j)

            @pl.when(a == 1)
            def _():
                loop(0, NL, lambda t: attend(0, turn(t), a, 0, LVL, False, last=True))

                @pl.when(even)
                def _():
                    for j in (shard, NL + partner, NL + far, NL + far2, b, partner):
                        for what in ("k", "v"):
                            hop(j, what, 2).wait_send()
                    pl.semaphore_signal(go, inc=1, device_id=(d, a, partner), device_id_type=MESH)

            @pl.when(a > 1)
            def _():
                with jax.named_scope("att1"):
                    loop(0, NL, lambda i: attend(0, i, a, (a - 1) * LVL, LVL, False))

        @pl.when((a >= 2) & (odd == 1))
        def _():
            lvl2 = (a - 2) * NL
            with jax.named_scope("take2a"):
                take(lvl2 + 3)
                take(lvl2 + 2)
            with jax.named_scope("att2a"):
                loop(0, 2, lambda i: attend(0, i, a, lvl2 * TOK + 2 * TOK, 2 * TOK, False))
            with jax.named_scope("take2b"):
                take(lvl2 + 1)
            with jax.named_scope("att2b"):
                loop(2, NL, lambda i: attend(0, i, a, lvl2 * TOK + 2 * TOK, 2 * TOK, False))
            with jax.named_scope("take2c"):
                take(lvl2)

        @pl.when((a == 2) & (odd == 1))
        def _():
            with jax.named_scope("att2c"):
                loop(0, NL, lambda t: attend(0, turn(t), a, 0, 2 * TOK, True, last=True))

        @pl.when((a == 3) & (odd == 1))
        def _():
            with jax.named_scope("att2c"):
                loop(0, NL, lambda i: attend(0, i, a, LVL, 2 * TOK, True))
            finish(0, NL - 1)
            with jax.named_scope("take3"):
                wait_piece(3)
                wait_piece(2)
            with jax.named_scope("att3"):
                attend(0, 2, a, 2 * TOK, 2 * TOK, True, last=True)
                attend(0, 1, a, 2 * TOK, 2 * TOK, True, last=True)
                attend(0, 0, a, 2 * TOK, 2 * TOK, True)
            with jax.named_scope("take3b"):
                wait_piece(1)
            with jax.named_scope("att3b"):
                attend(0, 0, a, 256, 128, True, last=True)

    def take_o(h):
        @pl.when((b != h) | ((a == 3) & (h % 2 == 0)))
        def _():
            remote(osend.at[0, 0], ob.at[:, pl.ds(h * 2 * HD, 2 * HD)], os_sem.at[0, 0], orecv.at[h], (d, a, b)).wait_recv()

    def project_o(h, cols):
        return jnp.dot(ob[:, h * 2 * HD:(h + 1) * 2 * HD], wo[pl.ds(h * 2 * HD, 2 * HD), cols],
                       preferred_element_type=F32)

    tiles = [(pl.ds(t * HD, HD), (t // (2 * NL), t // 2 % NL, t % 2)) for t in range(DM // HD)]
    with jax.named_scope("o_even"):
        take_o(0)
        take_o(2)
    wo_copy.wait()
    for cols, at in tiles:
        acc[at] = project_o(0, cols) + project_o(2, cols)
    with jax.named_scope("o_odd"):
        for h in (1, 3):
            @pl.when(b // 2 == h // 2)
            def _():
                take_o(h)
                for cols, at in tiles:
                    acc[at] += project_o(h, cols)
        for h in (1, 3):
            @pl.when(b // 2 != h // 2)
            def _():
                take_o(h)
                for cols, at in tiles:
                    y_ref[:, cols] = (acc[at] + project_o(h, cols)).astype(BF)

    for h in range(NL):
        @pl.when(b != h)
        def _():
            for what in ("k", "v", "q"):
                exchange(h, what).wait_send()

        @pl.when((b != h) & jnp.logical_not(donor))
        def _():
            back_to(0, h).wait_send()

        @pl.when(host)
        def _():
            back_to(1, h).wait_send()

        @pl.when(donor)
        def _():
            q_down(h).wait_send()
            for what in ("k", "v"):
                hop(3 * NL + h, what, 2).wait_send()

    for s in range(12):
        waited = even & (a == 1) & ((s >= NL) | (s // 2 == b // 2))

        @pl.when(feeds & (s < NL * (a + 1)) & needed(s, a + 1) & jnp.logical_not(waited))
        def _():
            for what in ("k", "v"):
                hop(s, what, a + 1).wait_send()


def solution(mesh):
    def local_fn(hidden, w_q, w_k, w_v, w_o):
        freq = ROPE_BASE ** (-np.arange(HALF) * 2.0 / HD)
        steps, starts = np.arange(TOK)[:, None] * freq, (np.arange(NL * NL) * TOK)[:, None] * freq
        trig = jnp.asarray(np.stack([np.cos(steps), np.sin(steps)]), F32)
        base = jnp.asarray(np.stack([np.cos(starts), np.sin(starts)]), F32)
        hbm = pl.BlockSpec(memory_space=pltpu.HBM)
        dma = pltpu.SemaphoreType.DMA
        return pl.pallas_call(
            body,
            out_shape=jax.ShapeDtypeStruct((TOK, DM), BF),
            in_specs=[hbm] * 7,
            out_specs=pl.BlockSpec(memory_space=pltpu.VMEM),
            scratch_shapes=[
                pltpu.VMEM((2, TOK, HALF), F32), pltpu.VMEM((2, NL * NL, HALF), F32),
                pltpu.VMEM((TOK, DM), BF), pltpu.VMEM((DM // 2, 2 * NL, HD), BF), pltpu.VMEM((DM, NL, HD), BF),
                pltpu.VMEM((DM, NL, HD), BF), pltpu.VMEM((2 * NL * HD, DM), BF),
                pltpu.VMEM((NL, TOK, HD), BF), pltpu.VMEM((NL, TOK, HD), BF), pltpu.VMEM((NL, 2, TOK, HD), BF),
                pltpu.VMEM((16 * TOK, HD), BF), pltpu.VMEM((16 * TOK, HD), BF),
                pltpu.VMEM((2, NL, 2, TOK, HD), BF), pltpu.VMEM((TOK, 2 * NL * HD), BF),
                pltpu.VMEM((2, NL, TOK, 2 * HD), BF), pltpu.VMEM((2, NL, 2, TOK, HD), F32),
                pltpu.VMEM((2, NL, 2, TOK, LANES), F32), pltpu.VMEM((2, NL, 2, TOK, LANES), F32),
                dma((2,)), dma(()), dma((KCUT,)), dma((KCUT,)), dma((QCUT,)), dma(()),
                dma((16,)), dma((16,)), dma((16,)), dma((16,)), dma((NL,)),
                dma((NL,)), dma((NL,)), dma((NL,)), dma((2, NL)), dma((2, NL)), dma((NL,)),
                pltpu.SemaphoreType.REGULAR,
            ],
            compiler_params=pltpu.CompilerParams(collective_id=0, has_side_effects=True,
                                                 vmem_limit_bytes=51 * 2 ** 20),
        )(trig, base, hidden, w_q, w_k, w_v, w_o.reshape(2 * NL * HD, DM))

    return jax.shard_map(local_fn, mesh=mesh,
                         in_specs=(P(("dp", "cpo", "cpi"), None), P(), P(), P(), P()),
                         out_specs=P(("dp", "cpo", "cpi"), None), check_vma=False)
```

```python
import jax
import jax.numpy as jnp
from jax import lax
from jax.experimental import pallas as pl
from jax.experimental.pallas import tpu as pltpu
from jax.sharding import PartitionSpec as P

WINDOW = 2048
ROPE_BASE = 10000.0
MESH = pl.DeviceIdType.MESH
NL = 4
TOK = 192
LVL = NL * TOK
DM = 2560
HD = 256
HALF = HD // 2
LANES = 128
FINE = 16
NEG = -1e30
SCALE = HD ** -0.5 * 1.4426950408889634
KCUT = 4
QCUT = 4
OWN_KEYS = (256, 384, 640, 768)
F32, BF = jnp.float32, jnp.bfloat16


def body(freq_ref, x, wq_hbm, wk_hbm, wv_hbm, wo_hbm, y_ref,
         wq, wk, wv, wo, ko, vo, qo, kb, vb, qb, ob, osend, acc, m_s, l_s,
         wksem, wvsem, wqsem, wosem, krecv, vrecv, kfs, vfs, qfs, ksend, vsend, qsend, qrecv,
         os_sem, orecv, go):
    d, a, b = lax.axis_index("dp"), lax.axis_index("cpo"), lax.axis_index("cpi")
    shard = a * NL + b
    odd = lax.rem(b, 2)
    even = odd == 0
    partner = b + 1 - 2 * odd
    far = lax.rem(b + 2, NL)
    far2 = lax.rem(partner + 2, NL)
    near0 = b - odd
    away0 = 2 - near0
    donor = (a == 3) & even
    host = (a == 2) & even
    feeds = (a < 2) | ((a == 2) & (odd == 1))

    def cut(src, dst, sem, n, c):
        r = DM // n
        return pltpu.make_async_copy(src.at[pl.ds(c * r, r)], dst.at[pl.ds(c * r, r)], sem.at[c])

    for c in range(KCUT):
        cut(wk_hbm, wk, wksem, KCUT, c).start()

    bar = pltpu.get_barrier_semaphore()

    def greet(level, other):
        pl.semaphore_signal(bar, inc=1, device_id=(d, level, other), device_id_type=MESH)

    for j in (partner, far, far2):
        greet(a, j)

    @pl.when(a > 0)
    def _():
        greet(a - 1, b)

    @pl.when(a < NL - 1)
    def _():
        greet(a + 1, b)

    @pl.when(host)
    def _():
        for j in (partner, far, far2):
            greet(3, j)

    @pl.when(a == 3)
    def _():
        greet(2, lax.rem(b + 2 - odd, NL))

    @pl.when((a == 3) & (odd == 1))
    def _():
        greet(2, b - 1)

    def one(p):
        return p.astype(jnp.int32)

    step = lax.broadcasted_iota(jnp.int32, (FINE, HALF), 0)
    fine = step.astype(F32) * freq_ref[...]
    coarse = (step * FINE + shard * TOK).astype(F32) * freq_ref[...]
    cf, sf = jnp.cos(fine)[None], jnp.sin(fine)[None]
    cc, sc = jnp.cos(coarse)[:TOK // FINE, None], jnp.sin(coarse)[:TOK // FINE, None]
    cos = (cc * cf - sc * sf).reshape(TOK, HALF)
    sin = (sc * cf + cc * sf).reshape(TOK, HALF)

    def project(w, n, copies, heads, fetch, between):
        total = None
        for c in range(n):
            copies[c].wait()
            if c in fetch:
                fetch[c]()
            r = DM // n
            at = c * r % w.shape[0]
            part = jnp.dot(x[:, c * r:(c + 1) * r], w[pl.ds(at, r)].reshape(r, heads * HD),
                           preferred_element_type=F32)
            total = part if total is None else total + part
            if c in between:
                between[c]()
        return total

    def rotate(t, h, cos, sin):
        lo, hi = t[:, h * HD:h * HD + HALF], t[:, h * HD + HALF:(h + 1) * HD]
        return (lo * cos - hi * sin).astype(BF), (hi * cos + lo * sin).astype(BF)

    def rows(s):
        return pl.ds(pl.multiple_of(s * TOK, TOK), TOK)

    def remote(src, dst, ss, rs, dev):
        return pltpu.make_async_remote_copy(src_ref=src, dst_ref=dst, send_sem=ss, recv_sem=rs,
                                            device_id=dev, device_id_type=MESH)

    def exchange(h, what):
        dev = (d, a, h)
        if what == "k":
            return remote(ko.at[h], kb.at[rows(shard)], ksend.at[h], krecv.at[shard], dev)
        if what == "v":
            return remote(vo.at[h], vb.at[rows(shard)], vsend.at[h], vrecv.at[shard], dev)
        return remote(qo.at[h], qb.at[0, b], qsend.at[h], qrecv.at[0, b], dev)

    def send(what, early=True, late=True):
        for h in (0, 2, 1, 3):
            soon = (partner == h) | (h % 2 == 0)
            if early:
                @pl.when((b != h) & soon)
                def _():
                    exchange(h, what).start()
            if late:
                @pl.when((b != h) & jnp.logical_not(soon))
                def _():
                    exchange(h, what).start()

    def hop(s, what, level):
        dev = (d, level, b)
        if what == "k":
            return remote(kb.at[rows(s)], kb.at[rows(s)], kfs.at[s], krecv.at[s], dev)
        return remote(vb.at[rows(s)], vb.at[rows(s)], vfs.at[s], vrecv.at[s], dev)

    def wait_piece(s):
        hop(s, "k", a).wait_recv()
        hop(s, "v", a).wait_recv()

    def needed(s, level):
        return s >= NL * level - 11

    def pass_on(s, whats=("k", "v")):
        @pl.when(feeds & needed(s, a + 1))
        def _():
            for what in whats:
                hop(s, what, a + 1).start()

        @pl.when(donor)
        def _():
            for what in whats:
                hop(s, what, 2).start()

    def q_down(j):
        return remote(qb.at[0, j], qb.at[1, j], qfs.at[j], qrecv.at[1, j], (d, 2, b))

    def wait_q(slot, j):
        remote(qo.at[0], qb.at[slot, j], qsend.at[0], qrecv.at[slot, j], (d, a, b)).wait_recv()

    first_user = even | (a >= 1)


    def start_v():
        for c in range(KCUT):
            cut(wv_hbm, wv, wvsem, KCUT, c).start()

    def cut_q(c):
        r = DM // QCUT
        return pltpu.make_async_copy(wq_hbm.at[pl.ds(c * r, r)], wq.at[pl.ds(c % 2 * r, r)], wqsem.at[c])

    def start_q():
        cut_q(0).start()
        cut_q(1).start()

    with jax.named_scope("k_proj"):
        k_f = project(wk, KCUT, [cut(wk_hbm, wk, wksem, KCUT, c) for c in range(KCUT)], NL, {1: start_v}, {})
    wo_copy = pltpu.make_async_copy(wo_hbm, wo, wosem)
    for h in range(NL):
        ko[h, :, :HALF], ko[h, :, HALF:] = rotate(k_f, h, cos, sin)
    kb[rows(shard), :] = ko[b]
    with jax.named_scope("barrier"):
        pl.semaphore_wait(bar, 3 + one(a > 0) + one(a < NL - 1) + 3 * one(host) + one(a == 3)
                          + one((a == 3) & (odd == 1)))
    send("k", late=False)

    def relay(who, whats, js):
        @pl.when(who)
        def _():
            for j in js:
                for what in whats:
                    hop(a * NL + j, what, a).wait_recv()
                pass_on(a * NL + j, whats)

    @pl.when(first_user)
    def _():
        pass_on(shard, ("k",))

    with jax.named_scope("v_proj"):
        v_f = project(wv, KCUT, [cut(wv_hbm, wv, wvsem, KCUT, c) for c in range(KCUT)], NL, {1: start_q},
                      {2: lambda: relay(even | (a >= 1), ("k",), (partner,))})
    for h in range(NL):
        vo[h] = v_f[:, h * HD:(h + 1) * HD].astype(BF)
    vb[rows(shard), :] = vo[b]
    send("v", late=False)
    send("k", early=False)
    send("v", early=False)

    @pl.when(first_user)
    def _():
        pass_on(shard, ("v",))

    def relay_1():
        cut_q(3).start()
        relay(even, ("v",), (partner,))
        relay(even, ("k",), (far, far2))
        relay((odd == 1) & (a >= 1), ("v",), (partner,))

    with jax.named_scope("q_proj"):
        q_f = project(wq, QCUT, [cut_q(c) for c in range(QCUT)], 2 * NL,
                      {3: wo_copy.start}, {0: cut_q(2).start, 1: relay_1})
    for h in range(2 * NL):
        qo[h // 2, h % 2, :, :HALF], qo[h // 2, h % 2, :, HALF:] = rotate(q_f, h, cos, sin)
    qb[0, b] = qo[b]
    send("q")

    def wide(t, n):
        return jnp.concatenate([t] * (n // LANES), axis=1)

    def attend(slot, i, level, key0, n, masked, first=False, last=False):
        keys = pl.ds(pl.multiple_of(key0, 64), n)
        k, v = kb[keys, :], vb[keys, :]
        scores = []
        for g in range(2):
            s = lax.dot_general(qb[slot, i, g], k, (((1,), (1,)), ((), ())), preferred_element_type=F32)
            if masked:
                gap = (lax.broadcasted_iota(jnp.int32, (TOK, n), 0) - lax.broadcasted_iota(jnp.int32, (TOK, n), 1)
                       + (level * LVL + i * TOK - key0))
                s = jnp.where((gap >= 0) & (gap < WINDOW), s, NEG)
            scores.append(s)
        for g, s in enumerate(scores):
            top = jnp.max(s, axis=-1, keepdims=True)
            if first:
                new = jnp.broadcast_to(top, (TOK, LANES))
            else:
                old = m_s[slot, i, g]
                new = jnp.maximum(old, top)
                fix = jnp.exp2((old - new) * SCALE)
            p = jnp.exp2((s - wide(new, n)) * SCALE)
            total = jnp.broadcast_to(jnp.sum(p, axis=-1, keepdims=True), (TOK, LANES))
            out = jnp.dot(p.astype(BF), v, preferred_element_type=F32)
            if not first:
                total = total + l_s[slot, i, g] * fix
                out = out + acc[slot, i, g] * wide(fix, HD)
            if last:
                osend[slot, i, :, g * HD:(g + 1) * HD] = (out * wide(1.0 / total, HD)).astype(BF)
            else:
                m_s[slot, i, g] = new
                l_s[slot, i, g] = total
                acc[slot, i, g] = out
        if last:
            give(slot, i)

    def loop(lo, hi, fn):
        def step(i, carry):
            fn(i)
            return carry
        lax.fori_loop(lo, hi, step, 0)

    def head_cols():
        return pl.ds(pl.multiple_of(b * 2 * HD, 2 * HD), 2 * HD)

    def back_to(slot, i):
        return remote(osend.at[slot, i], ob.at[:, head_cols()], os_sem.at[slot, i], orecv.at[b], (d, a + slot, i))

    def give(slot, i):
        if slot == 1:
            back_to(1, i).start()
            return

        @pl.when(b != i)
        def _():
            back_to(0, i).start()

        @pl.when(b == i)
        def _():
            ob[:, head_cols()] = osend[0, i]

    def finish(slot, i):
        for g in range(2):
            osend[slot, i, :, g * HD:(g + 1) * HD] = (acc[slot, i, g] * wide(1.0 / l_s[slot, i, g], HD)).astype(BF)
        give(slot, i)

    def turn(t):
        return lax.rem(away0 + t, NL)

    low = (a - 1) * NL

    def own_block(slot):
        with jax.named_scope("own_att"):
            for i in range(NL):
                attend(slot, i, a + slot, (a + slot) * LVL, OWN_KEYS[i], True, first=True)

    def take(s):
        wait_piece(s)
        pass_on(s)

    relay(even, ("v",), (far, far2))

    @pl.when(even & (a == 0))
    def _():
        pl.semaphore_signal(go, inc=1, device_id=(d, a, partner), device_id_type=MESH)

    @pl.when((odd == 1) & (a == 0))
    def _():
        with jax.named_scope("go_wait"):
            pl.semaphore_wait(go, 1)
        pass_on(shard)
        take(a * NL + partner)

    relay(odd == 1, ("k", "v"), (far, far2))

    @pl.when((even & (a == 1)) | ((odd == 1) & (a >= 2)))
    def _():
        with jax.named_scope("take_low"):
            for j in (b, partner, far, far2):
                take(low + j)

    with jax.named_scope("own_q"):
        @pl.when(jnp.logical_not(donor))
        def _():
            wait_q(0, partner)

        @pl.when(jnp.logical_not(donor | host))
        def _():
            wait_q(0, far)
            wait_q(0, far2)

    @pl.when(donor)
    def _():
        q_down(b).start()
        for j in (partner, far, far2):
            wait_q(0, j)
            q_down(j).start()

    def chip_block(slot, here):
        for i in range(0, NL, 2):
            @pl.when((near0 == i) == here)
            def _():
                for j in (i, i + 1):
                    attend(slot, j, a + slot, (a + slot) * LVL, OWN_KEYS[j], True, first=True)

    def pair(start, fn):
        loop(0, 2, lambda t: fn(start + t))

    @pl.when(host)
    def _():
        def low_0(start):
            pair(start, lambda i: attend(0, i, a, (a - 1) * LVL, LVL, False))

        def low_1(start):
            pair(start, lambda i: attend(1, i, 3, LVL, LVL, True))

        def top_1(here, start):
            with jax.named_scope("hq1"):
                for j in ((b, partner) if here else (far, far2)):
                    wait_q(1, j)
            with jax.named_scope("top_1"):
                chip_block(1, here)
                pair(start, lambda i: attend(1, i, 3, 2 * LVL, LVL, False))

        with jax.named_scope("job0"):
            chip_block(0, True)
        with jax.named_scope("take1"):
            for j in (b, partner, far, far2):
                take(low + j)
        low_0(near0)
        with jax.named_scope("hq0"):
            wait_q(0, far)
            wait_q(0, far2)
        with jax.named_scope("job0"):
            chip_block(0, False)
            low_0(away0)
        with jax.named_scope("hkv1"):
            for j in range(NL):
                wait_piece(3 * NL + j)
        top_1(True, near0)
        low_1(near0)

        @pl.when(near0 == 2)
        def _():
            finish(1, NL - 1)

        top_1(False, away0)
        low_1(away0)

        @pl.when(near0 == 0)
        def _():
            finish(1, NL - 1)

        with jax.named_scope("take2"):
            for j in (b, partner, far, far2):
                take(j)
        with jax.named_scope("att2"):
            loop(0, NL, lambda t: attend(0, turn(t), a, 0, LVL, True, last=True))
        with jax.named_scope("host_last"):
            loop(0, NL - 1, lambda i: attend(1, i, 3, 256, 512, True, last=True))

    @pl.when(jnp.logical_not(donor | host))
    def _():
        own_block(0)

        @pl.when(a == 0)
        def _():
            loop(0, NL, lambda t: finish(0, turn(t)))

        @pl.when(a > 0)
        def _():
            @pl.when((a == 1) & (odd == 1))
            def _():
                with jax.named_scope("go_wait"):
                    pl.semaphore_wait(go, 1)
                with jax.named_scope("take_low"):
                    for j in (3, 2, 1, 0):
                        take(low + j)

            @pl.when(a == 1)
            def _():
                loop(0, NL, lambda t: attend(0, turn(t), a, 0, LVL, False, last=True))

                @pl.when(even)
                def _():
                    for j in (shard, NL + partner, NL + far, NL + far2, b, partner):
                        for what in ("k", "v"):
                            hop(j, what, 2).wait_send()
                    pl.semaphore_signal(go, inc=1, device_id=(d, a, partner), device_id_type=MESH)

            @pl.when(a > 1)
            def _():
                with jax.named_scope("att1"):
                    loop(0, NL, lambda i: attend(0, i, a, (a - 1) * LVL, LVL, False))

        @pl.when((a >= 2) & (odd == 1))
        def _():
            lvl2 = (a - 2) * NL
            with jax.named_scope("take2a"):
                take(lvl2 + 3)
                take(lvl2 + 2)
            with jax.named_scope("att2a"):
                loop(0, 2, lambda i: attend(0, i, a, lvl2 * TOK + 2 * TOK, 2 * TOK, False))
            with jax.named_scope("take2b"):
                take(lvl2 + 1)
            with jax.named_scope("att2b"):
                loop(2, NL, lambda i: attend(0, i, a, lvl2 * TOK + 2 * TOK, 2 * TOK, False))
            with jax.named_scope("take2c"):
                take(lvl2)

        @pl.when((a == 2) & (odd == 1))
        def _():
            with jax.named_scope("att2c"):
                loop(0, NL, lambda t: attend(0, turn(t), a, 0, 2 * TOK, True, last=True))

        @pl.when((a == 3) & (odd == 1))
        def _():
            with jax.named_scope("att2c"):
                loop(0, NL, lambda i: attend(0, i, a, LVL, 2 * TOK, True))
            finish(0, NL - 1)
            with jax.named_scope("take3"):
                wait_piece(3)
                wait_piece(2)
            with jax.named_scope("att3"):
                attend(0, 2, a, 2 * TOK, 2 * TOK, True, last=True)
                attend(0, 1, a, 2 * TOK, 2 * TOK, True, last=True)
                attend(0, 0, a, 2 * TOK, 2 * TOK, True)
            with jax.named_scope("take3b"):
                wait_piece(1)
            with jax.named_scope("att3b"):
                attend(0, 0, a, 256, 128, True, last=True)

    def take_o(h):
        @pl.when((b != h) | ((a == 3) & (h % 2 == 0)))
        def _():
            remote(osend.at[0, 0], ob.at[:, pl.ds(h * 2 * HD, 2 * HD)], os_sem.at[0, 0], orecv.at[h], (d, a, b)).wait_recv()

    def project_o(h, cols):
        return jnp.dot(ob[:, h * 2 * HD:(h + 1) * 2 * HD], wo[pl.ds(h * 2 * HD, 2 * HD), cols],
                       preferred_element_type=F32)

    tiles = [(pl.ds(t * HD, HD), (t // (2 * NL), t // 2 % NL, t % 2)) for t in range(DM // HD)]
    with jax.named_scope("o_even"):
        take_o(0)
        take_o(2)
    wo_copy.wait()
    for cols, at in tiles:
        acc[at] = project_o(0, cols) + project_o(2, cols)
    with jax.named_scope("o_odd"):
        for h in (1, 3):
            @pl.when(b // 2 == h // 2)
            def _():
                take_o(h)
                for cols, at in tiles:
                    acc[at] += project_o(h, cols)
        for h in (1, 3):
            @pl.when(b // 2 != h // 2)
            def _():
                take_o(h)
                for cols, at in tiles:
                    y_ref[:, cols] = (acc[at] + project_o(h, cols)).astype(BF)

    for h in range(NL):
        @pl.when(b != h)
        def _():
            for what in ("k", "v", "q"):
                exchange(h, what).wait_send()

        @pl.when((b != h) & jnp.logical_not(donor))
        def _():
            back_to(0, h).wait_send()

        @pl.when(host)
        def _():
            back_to(1, h).wait_send()

        @pl.when(donor)
        def _():
            q_down(h).wait_send()
            for what in ("k", "v"):
                hop(3 * NL + h, what, 2).wait_send()

    for s in range(12):
        waited = even & (a == 1) & ((s >= NL) | (s // 2 == b // 2))

        @pl.when(feeds & (s < NL * (a + 1)) & needed(s, a + 1) & jnp.logical_not(waited))
        def _():
            for what in ("k", "v"):
                hop(s, what, a + 1).wait_send()


def solution(mesh):
    def local_fn(hidden, w_q, w_k, w_v, w_o):
        freq = (ROPE_BASE ** (-jnp.arange(HALF, dtype=F32) * 2.0 / HD)).reshape(1, HALF)
        hbm = pl.BlockSpec(memory_space=pltpu.HBM)
        dma = pltpu.SemaphoreType.DMA
        return pl.pallas_call(
            body,
            out_shape=jax.ShapeDtypeStruct((TOK, DM), BF),
            in_specs=[pl.BlockSpec(memory_space=pltpu.VMEM)] * 2 + [hbm] * 4,
            out_specs=pl.BlockSpec(memory_space=pltpu.VMEM),
            scratch_shapes=[
                pltpu.VMEM((DM // 2, 2 * NL, HD), BF), pltpu.VMEM((DM, NL, HD), BF),
                pltpu.VMEM((DM, NL, HD), BF), pltpu.VMEM((2 * NL * HD, DM), BF),
                pltpu.VMEM((NL, TOK, HD), BF), pltpu.VMEM((NL, TOK, HD), BF), pltpu.VMEM((NL, 2, TOK, HD), BF),
                pltpu.VMEM((16 * TOK, HD), BF), pltpu.VMEM((16 * TOK, HD), BF),
                pltpu.VMEM((2, NL, 2, TOK, HD), BF), pltpu.VMEM((TOK, 2 * NL * HD), BF),
                pltpu.VMEM((2, NL, TOK, 2 * HD), BF), pltpu.VMEM((2, NL, 2, TOK, HD), F32),
                pltpu.VMEM((2, NL, 2, TOK, LANES), F32), pltpu.VMEM((2, NL, 2, TOK, LANES), F32),
                dma((KCUT,)), dma((KCUT,)), dma((QCUT,)), dma(()),
                dma((16,)), dma((16,)), dma((16,)), dma((16,)), dma((NL,)),
                dma((NL,)), dma((NL,)), dma((NL,)), dma((2, NL)), dma((2, NL)), dma((NL,)),
                pltpu.SemaphoreType.REGULAR,
            ],
            compiler_params=pltpu.CompilerParams(collective_id=0, has_side_effects=True,
                                                 vmem_limit_bytes=51 * 2 ** 20),
        )(freq, hidden, w_q, w_k, w_v, w_o.reshape(2 * NL * HD, DM))

    return jax.shard_map(local_fn, mesh=mesh,
                         in_specs=(P(("dp", "cpo", "cpi"), None), P(), P(), P(), P()),
                         out_specs=P(("dp", "cpo", "cpi"), None), check_vma=False)
```

```python
import jax
import jax.numpy as jnp
from jax import lax
from jax.experimental import pallas as pl
from jax.experimental.pallas import tpu as pltpu
from jax.sharding import PartitionSpec as P

WINDOW = 2048
ROPE_BASE = 10000.0
MESH = pl.DeviceIdType.MESH
NL = 4
TOK = 192
LVL = NL * TOK
DM = 2560
HD = 256
HALF = HD // 2
LANES = 128
FINE = 16
NEG = -1e30
SCALE = HD ** -0.5 * 1.4426950408889634
KCUT = 4
QCUT = 4
OWN_KEYS = (256, 384, 640, 768)
F32, BF = jnp.float32, jnp.bfloat16


def body(freq_ref, x, wq_hbm, wk_hbm, wv_hbm, wo_hbm, y_ref,
         wq, wk, wv, wo, ko, vo, qo, kb, vb, qb, ob, osend, acc, m_s, l_s,
         wksem, wvsem, wqsem, wosem, krecv, vrecv, kfs, vfs, qfs, ksend, vsend, qsend, qrecv,
         os_sem, orecv, go):
    d, a, b = lax.axis_index("dp"), lax.axis_index("cpo"), lax.axis_index("cpi")
    shard = a * NL + b
    odd = lax.rem(b, 2)
    even = odd == 0
    partner = b + 1 - 2 * odd
    far = lax.rem(b + 2, NL)
    far2 = lax.rem(partner + 2, NL)
    near0 = b - odd
    away0 = 2 - near0
    donor = (a == 3) & even
    host = (a == 2) & even
    feeds = (a < 2) | ((a == 2) & (odd == 1))

    def cut(src, dst, sem, n, c):
        r = DM // n
        return pltpu.make_async_copy(src.at[pl.ds(c * r, r)], dst.at[pl.ds(c * r, r)], sem.at[c])

    for c in range(KCUT):
        cut(wk_hbm, wk, wksem, KCUT, c).start()

    bar = pltpu.get_barrier_semaphore()

    def greet(level, other):
        pl.semaphore_signal(bar, inc=1, device_id=(d, level, other), device_id_type=MESH)

    for j in (partner, far, far2):
        greet(a, j)

    @pl.when(a > 0)
    def _():
        greet(a - 1, b)

    @pl.when(a < NL - 1)
    def _():
        greet(a + 1, b)

    @pl.when(host)
    def _():
        for j in (partner, far, far2):
            greet(3, j)

    @pl.when(a == 3)
    def _():
        greet(2, lax.rem(b + 2 - odd, NL))

    @pl.when((a == 3) & (odd == 1))
    def _():
        greet(2, b - 1)

    def one(p):
        return p.astype(jnp.int32)

    step = lax.broadcasted_iota(jnp.int32, (FINE, HALF), 0)
    fine = step.astype(F32) * freq_ref[...]
    coarse = (step * FINE + shard * TOK).astype(F32) * freq_ref[...]
    cf, sf = jnp.cos(fine)[None], jnp.sin(fine)[None]
    cc, sc = jnp.cos(coarse)[:TOK // FINE, None], jnp.sin(coarse)[:TOK // FINE, None]
    cos = (cc * cf - sc * sf).reshape(TOK, HALF)
    sin = (sc * cf + cc * sf).reshape(TOK, HALF)

    def project(w, n, copies, heads, fetch, between):
        total = None
        for c in range(n):
            copies[c].wait()
            if c in fetch:
                fetch[c]()
            r = DM // n
            at = c * r % w.shape[0]
            part = jnp.dot(x[:, c * r:(c + 1) * r], w[pl.ds(at, r)].reshape(r, heads * HD),
                           preferred_element_type=F32)
            total = part if total is None else total + part
            if c in between:
                between[c]()
        return total

    def rotate(t, h, cos, sin):
        lo, hi = t[:, h * HD:h * HD + HALF], t[:, h * HD + HALF:(h + 1) * HD]
        return (lo * cos - hi * sin).astype(BF), (hi * cos + lo * sin).astype(BF)

    def rows(s):
        return pl.ds(pl.multiple_of(s * TOK, TOK), TOK)

    def remote(src, dst, ss, rs, dev):
        return pltpu.make_async_remote_copy(src_ref=src, dst_ref=dst, send_sem=ss, recv_sem=rs,
                                            device_id=dev, device_id_type=MESH)

    def exchange(h, what):
        dev = (d, a, h)
        if what == "k":
            return remote(ko.at[h], kb.at[rows(shard)], ksend.at[h], krecv.at[shard], dev)
        if what == "v":
            return remote(vo.at[h], vb.at[rows(shard)], vsend.at[h], vrecv.at[shard], dev)
        return remote(qo.at[h], qb.at[0, b], qsend.at[h], qrecv.at[0, b], dev)

    def send(what, early=True, late=True):
        for h in (0, 2, 1, 3):
            soon = (partner == h) | (h % 2 == 0)
            if early:
                @pl.when((b != h) & soon)
                def _():
                    exchange(h, what).start()
            if late:
                @pl.when((b != h) & jnp.logical_not(soon))
                def _():
                    exchange(h, what).start()

    def hop(s, what, level):
        dev = (d, level, b)
        if what == "k":
            return remote(kb.at[rows(s)], kb.at[rows(s)], kfs.at[s], krecv.at[s], dev)
        return remote(vb.at[rows(s)], vb.at[rows(s)], vfs.at[s], vrecv.at[s], dev)

    def wait_piece(s):
        hop(s, "k", a).wait_recv()
        hop(s, "v", a).wait_recv()

    def needed(s, level):
        return s >= NL * level - 11

    def pass_on(s, whats=("k", "v")):
        @pl.when(feeds & needed(s, a + 1))
        def _():
            for what in whats:
                hop(s, what, a + 1).start()

        @pl.when(donor)
        def _():
            for what in whats:
                hop(s, what, 2).start()

    def q_down(j):
        return remote(qb.at[0, j], qb.at[1, j], qfs.at[j], qrecv.at[1, j], (d, 2, b))

    def wait_q(slot, j):
        remote(qo.at[0], qb.at[slot, j], qsend.at[0], qrecv.at[slot, j], (d, a, b)).wait_recv()

    first_user = even | (a >= 1)


    def start_v():
        for c in range(KCUT):
            cut(wv_hbm, wv, wvsem, KCUT, c).start()

    def cut_q(c):
        r = DM // QCUT
        return pltpu.make_async_copy(wq_hbm.at[pl.ds(c * r, r)], wq.at[pl.ds(c % 2 * r, r)], wqsem.at[c])

    def start_q():
        cut_q(0).start()
        cut_q(1).start()

    with jax.named_scope("k_proj"):
        k_f = project(wk, KCUT, [cut(wk_hbm, wk, wksem, KCUT, c) for c in range(KCUT)], NL, {1: start_v}, {})
    wo_copy = pltpu.make_async_copy(wo_hbm, wo, wosem)
    for h in range(NL):
        ko[h, :, :HALF], ko[h, :, HALF:] = rotate(k_f, h, cos, sin)
    kb[rows(shard), :] = ko[b]
    with jax.named_scope("barrier"):
        pl.semaphore_wait(bar, 3 + one(a > 0) + one(a < NL - 1) + 3 * one(host) + one(a == 3)
                          + one((a == 3) & (odd == 1)))
    send("k", late=False)

    def relay(who, whats, js):
        @pl.when(who)
        def _():
            for j in js:
                for what in whats:
                    hop(a * NL + j, what, a).wait_recv()
                pass_on(a * NL + j, whats)

    @pl.when(first_user)
    def _():
        pass_on(shard, ("k",))

    with jax.named_scope("v_proj"):
        v_f = project(wv, KCUT, [cut(wv_hbm, wv, wvsem, KCUT, c) for c in range(KCUT)], NL, {1: start_q},
                      {2: lambda: relay(even | (a >= 1), ("k",), (partner,))})
    for h in range(NL):
        vo[h] = v_f[:, h * HD:(h + 1) * HD].astype(BF)
    vb[rows(shard), :] = vo[b]
    send("v", late=False)
    send("k", early=False)
    send("v", early=False)

    @pl.when(first_user)
    def _():
        pass_on(shard, ("v",))

    def relay_1():
        cut_q(3).start()
        relay(even, ("v",), (partner,))
        relay(even, ("k",), (far, far2))
        relay((odd == 1) & (a >= 1), ("v",), (partner,))

    with jax.named_scope("q_proj"):
        q_f = project(wq, QCUT, [cut_q(c) for c in range(QCUT)], 2 * NL,
                      {3: wo_copy.start}, {0: cut_q(2).start, 1: relay_1})
    for h in range(2 * NL):
        qo[h // 2, h % 2, :, :HALF], qo[h // 2, h % 2, :, HALF:] = rotate(q_f, h, cos, sin)
    qb[0, b] = qo[b]
    send("q")

    def wide(t, n):
        return jnp.concatenate([t] * (n // LANES), axis=1)

    def attend(slot, i, level, key0, n, masked, first=False, last=False):
        keys = pl.ds(pl.multiple_of(key0, 64), n)
        k, v = kb[keys, :], vb[keys, :]
        scores = []
        for g in range(2):
            s = lax.dot_general(qb[slot, i, g], k, (((1,), (1,)), ((), ())), preferred_element_type=F32)
            if masked:
                gap = (lax.broadcasted_iota(jnp.int32, (TOK, n), 0) - lax.broadcasted_iota(jnp.int32, (TOK, n), 1)
                       + (level * LVL + i * TOK - key0))
                s = jnp.where((gap >= 0) & (gap < WINDOW), s, NEG)
            scores.append(s)
        for g, s in enumerate(scores):
            top = jnp.max(s, axis=-1, keepdims=True)
            if first:
                new = jnp.broadcast_to(top, (TOK, LANES))
            else:
                old = m_s[slot, i, g]
                new = jnp.maximum(old, top)
                fix = jnp.exp2((old - new) * SCALE)
            p = jnp.exp2((s - wide(new, n)) * SCALE)
            total = jnp.broadcast_to(jnp.sum(p, axis=-1, keepdims=True), (TOK, LANES))
            out = jnp.dot(p.astype(BF), v, preferred_element_type=F32)
            if not first:
                total = total + l_s[slot, i, g] * fix
                out = out + acc[slot, i, g] * wide(fix, HD)
            if last:
                osend[slot, i, :, g * HD:(g + 1) * HD] = (out * wide(1.0 / total, HD)).astype(BF)
            else:
                m_s[slot, i, g] = new
                l_s[slot, i, g] = total
                acc[slot, i, g] = out
        if last:
            give(slot, i)

    def loop(lo, hi, fn):
        def step(i, carry):
            fn(i)
            return carry
        lax.fori_loop(lo, hi, step, 0)

    def head_cols():
        return pl.ds(pl.multiple_of(b * 2 * HD, 2 * HD), 2 * HD)

    def back_to(slot, i):
        return remote(osend.at[slot, i], ob.at[:, head_cols()], os_sem.at[slot, i], orecv.at[b], (d, a + slot, i))

    def give(slot, i):
        if slot == 1:
            back_to(1, i).start()
            return

        @pl.when(b != i)
        def _():
            back_to(0, i).start()

        @pl.when(b == i)
        def _():
            ob[:, head_cols()] = osend[0, i]

    def finish(slot, i):
        for g in range(2):
            osend[slot, i, :, g * HD:(g + 1) * HD] = (acc[slot, i, g] * wide(1.0 / l_s[slot, i, g], HD)).astype(BF)
        give(slot, i)

    def turn(t):
        return lax.rem(away0 + t, NL)

    low = (a - 1) * NL

    def own_block(slot):
        with jax.named_scope("own_att"):
            for i in range(NL):
                attend(slot, i, a + slot, (a + slot) * LVL, OWN_KEYS[i], True, first=True)

    def take(s):
        wait_piece(s)
        pass_on(s)

    relay(even, ("v",), (far, far2))

    @pl.when(even & (a == 0))
    def _():
        pl.semaphore_signal(go, inc=1, device_id=(d, a, partner), device_id_type=MESH)

    @pl.when((odd == 1) & (a == 0))
    def _():
        with jax.named_scope("go_wait"):
            pl.semaphore_wait(go, 1)
        pass_on(shard)
        take(a * NL + partner)

    relay(odd == 1, ("k", "v"), (far, far2))

    @pl.when((even & (a == 1)) | ((odd == 1) & (a >= 2)))
    def _():
        with jax.named_scope("take_low"):
            for j in (b, partner, far, far2):
                take(low + j)

    @pl.when((odd == 1) & (a == 1))
    def _():
        with jax.named_scope("take_early"):
            pass

    with jax.named_scope("own_q"):
        @pl.when(jnp.logical_not(donor))
        def _():
            wait_q(0, partner)

        @pl.when(jnp.logical_not(donor | host))
        def _():
            wait_q(0, far)
            wait_q(0, far2)

    @pl.when(donor)
    def _():
        q_down(b).start()
        for j in (partner, far, far2):
            wait_q(0, j)
            q_down(j).start()

    def chip_block(slot, here):
        for i in range(0, NL, 2):
            @pl.when((near0 == i) == here)
            def _():
                for j in (i, i + 1):
                    attend(slot, j, a + slot, (a + slot) * LVL, OWN_KEYS[j], True, first=True)

    def pair(start, fn):
        loop(0, 2, lambda t: fn(start + t))

    @pl.when(host)
    def _():
        def low_0(start):
            pair(start, lambda i: attend(0, i, a, (a - 1) * LVL, LVL, False))

        def low_1(start):
            pair(start, lambda i: attend(1, i, 3, LVL, LVL, True))

        def top_1(here, start):
            with jax.named_scope("hq1"):
                for j in ((b, partner) if here else (far, far2)):
                    wait_q(1, j)
            with jax.named_scope("top_1"):
                chip_block(1, here)
                pair(start, lambda i: attend(1, i, 3, 2 * LVL, LVL, False))

        with jax.named_scope("job0"):
            chip_block(0, True)
        with jax.named_scope("take1"):
            for j in (b, partner, far, far2):
                take(low + j)
        low_0(near0)
        with jax.named_scope("hq0"):
            wait_q(0, far)
            wait_q(0, far2)
        with jax.named_scope("job0"):
            chip_block(0, False)
            low_0(away0)
        with jax.named_scope("hkv1"):
            for j in range(NL):
                wait_piece(3 * NL + j)
        top_1(True, near0)
        low_1(near0)

        @pl.when(near0 == 2)
        def _():
            finish(1, NL - 1)

        top_1(False, away0)
        low_1(away0)

        @pl.when(near0 == 0)
        def _():
            finish(1, NL - 1)

        with jax.named_scope("take2"):
            for j in (b, partner, far, far2):
                take(j)
        with jax.named_scope("host_last"):
            loop(0, NL - 1, lambda i: attend(1, i, 3, 256, 512, True, last=True))
        with jax.named_scope("att2"):
            loop(0, NL, lambda t: attend(0, turn(t), a, 0, LVL, True, last=True))

    @pl.when(jnp.logical_not(donor | host))
    def _():
        own_block(0)

        @pl.when((a == 2) & (odd == 1))
        def _():
            with jax.named_scope("take_early"):
                pass

        @pl.when(a == 0)
        def _():
            loop(0, NL, lambda t: finish(0, turn(t)))

        @pl.when(a > 0)
        def _():
            @pl.when((a == 1) & (odd == 1))
            def _():
                with jax.named_scope("go_wait"):
                    pl.semaphore_wait(go, 1)
                with jax.named_scope("take_low"):
                    for j in (3, 2, 1, 0):
                        take(low + j)

            @pl.when(a == 1)
            def _():
                loop(0, NL, lambda t: attend(0, turn(t), a, 0, LVL, False, last=True))

                @pl.when(even)
                def _():
                    for j in (shard, NL + partner, NL + far, NL + far2, b, partner):
                        for what in ("k", "v"):
                            hop(j, what, 2).wait_send()
                    pl.semaphore_signal(go, inc=1, device_id=(d, a, partner), device_id_type=MESH)

            @pl.when(a > 1)
            def _():
                with jax.named_scope("att1"):
                    loop(0, NL, lambda i: attend(0, i, a, (a - 1) * LVL, LVL, False))

        @pl.when((a >= 2) & (odd == 1))
        def _():
            lvl2 = (a - 2) * NL
            with jax.named_scope("take2a"):
                take(lvl2 + 3)
                take(lvl2 + 2)
            with jax.named_scope("att2a"):
                loop(0, 2, lambda i: attend(0, i, a, lvl2 * TOK + 2 * TOK, 2 * TOK, False))
            with jax.named_scope("take2b"):
                take(lvl2 + 1)
            with jax.named_scope("att2b"):
                loop(2, NL, lambda i: attend(0, i, a, lvl2 * TOK + 2 * TOK, 2 * TOK, False))
            with jax.named_scope("take2c"):
                take(lvl2)

        @pl.when((a == 2) & (odd == 1))
        def _():
            with jax.named_scope("att2c"):
                loop(0, NL, lambda t: attend(0, turn(t), a, 0, 2 * TOK, True, last=True))

        @pl.when((a == 3) & (odd == 1))
        def _():
            with jax.named_scope("att2c"):
                loop(0, NL, lambda i: attend(0, i, a, LVL, 2 * TOK, True))
            finish(0, NL - 1)
            with jax.named_scope("take3"):
                wait_piece(3)
                wait_piece(2)
            with jax.named_scope("att3"):
                attend(0, 2, a, 2 * TOK, 2 * TOK, True, last=True)
                attend(0, 1, a, 2 * TOK, 2 * TOK, True, last=True)
                attend(0, 0, a, 2 * TOK, 2 * TOK, True)
            with jax.named_scope("take3b"):
                wait_piece(1)
            with jax.named_scope("att3b"):
                attend(0, 0, a, 256, 128, True, last=True)

    def take_o(h):
        @pl.when((b != h) | ((a == 3) & (h % 2 == 0)))
        def _():
            remote(osend.at[0, 0], ob.at[:, pl.ds(h * 2 * HD, 2 * HD)], os_sem.at[0, 0], orecv.at[h], (d, a, b)).wait_recv()

    def project_o(h, cols):
        return jnp.dot(ob[:, h * 2 * HD:(h + 1) * 2 * HD], wo[pl.ds(h * 2 * HD, 2 * HD), cols],
                       preferred_element_type=F32)

    tiles = [(pl.ds(t * HD, HD), (t // (2 * NL), t // 2 % NL, t % 2)) for t in range(DM // HD)]
    wo_copy.wait()

    def add_head(h, here, start=False, last=False):
        @pl.when((b // 2 == h // 2) == here)
        def _():
            take_o(h)
            for cols, at in tiles:
                part = project_o(h, cols)
                if not start:
                    part = part + acc[at]
                if last:
                    y_ref[:, cols] = part.astype(BF)
                else:
                    acc[at] = part

    with jax.named_scope("o_near"):
        for h in (1, 3):
            add_head(h, True, start=True)
        for h in (0, 2):
            add_head(h, True)

    for h in range(NL):
        @pl.when(b != h)
        def _():
            for what in ("k", "v", "q"):
                exchange(h, what).wait_send()

        @pl.when(donor)
        def _():
            q_down(h).wait_send()
            for what in ("k", "v"):
                hop(3 * NL + h, what, 2).wait_send()

    for s in range(12):
        waited = even & (a == 1) & ((s >= NL) | (s // 2 == b // 2))

        @pl.when(feeds & (s < NL * (a + 1)) & needed(s, a + 1) & jnp.logical_not(waited))
        def _():
            for what in ("k", "v"):
                hop(s, what, a + 1).wait_send()

    with jax.named_scope("o_far"):
        for h in (1, 3):
            add_head(h, False)
        for h in (0, 2):
            add_head(h, False, last=True)

    for h in range(NL):
        @pl.when((b != h) & jnp.logical_not(donor))
        def _():
            back_to(0, h).wait_send()

        @pl.when(host)
        def _():
            back_to(1, h).wait_send()


def solution(mesh):
    def local_fn(hidden, w_q, w_k, w_v, w_o):
        freq = (ROPE_BASE ** (-jnp.arange(HALF, dtype=F32) * 2.0 / HD)).reshape(1, HALF)
        hbm = pl.BlockSpec(memory_space=pltpu.HBM)
        dma = pltpu.SemaphoreType.DMA
        return pl.pallas_call(
            body,
            out_shape=jax.ShapeDtypeStruct((TOK, DM), BF),
            in_specs=[pl.BlockSpec(memory_space=pltpu.VMEM)] * 2 + [hbm] * 4,
            out_specs=pl.BlockSpec(memory_space=pltpu.VMEM),
            scratch_shapes=[
                pltpu.VMEM((DM // 2, 2 * NL, HD), BF), pltpu.VMEM((DM, NL, HD), BF),
                pltpu.VMEM((DM, NL, HD), BF), pltpu.VMEM((2 * NL * HD, DM), BF),
                pltpu.VMEM((NL, TOK, HD), BF), pltpu.VMEM((NL, TOK, HD), BF), pltpu.VMEM((NL, 2, TOK, HD), BF),
                pltpu.VMEM((16 * TOK, HD), BF), pltpu.VMEM((16 * TOK, HD), BF),
                pltpu.VMEM((2, NL, 2, TOK, HD), BF), pltpu.VMEM((TOK, 2 * NL * HD), BF),
                pltpu.VMEM((2, NL, TOK, 2 * HD), BF), pltpu.VMEM((2, NL, 2, TOK, HD), F32),
                pltpu.VMEM((2, NL, 2, TOK, LANES), F32), pltpu.VMEM((2, NL, 2, TOK, LANES), F32),
                dma((KCUT,)), dma((KCUT,)), dma((QCUT,)), dma(()),
                dma((16,)), dma((16,)), dma((16,)), dma((16,)), dma((NL,)),
                dma((NL,)), dma((NL,)), dma((NL,)), dma((2, NL)), dma((2, NL)), dma((NL,)),
                pltpu.SemaphoreType.REGULAR,
            ],
            compiler_params=pltpu.CompilerParams(collective_id=0, has_side_effects=True,
                                                 vmem_limit_bytes=51 * 2 ** 20),
        )(freq, hidden, w_q, w_k, w_v, w_o.reshape(2 * NL * HD, DM))

    return jax.shard_map(local_fn, mesh=mesh,
                         in_specs=(P(("dp", "cpo", "cpi"), None), P(), P(), P(), P()),
                         out_specs=P(("dp", "cpo", "cpi"), None), check_vma=False)
```

```python
import jax
import jax.numpy as jnp
from jax import lax
from jax.experimental import pallas as pl
from jax.experimental.pallas import tpu as pltpu
from jax.sharding import PartitionSpec as P

WINDOW = 2048
ROPE_BASE = 10000.0
MESH = pl.DeviceIdType.MESH
NL = 4
TOK = 192
LVL = NL * TOK
DM = 2560
HD = 256
HALF = HD // 2
LANES = 128
FINE = 16
NEG = -1e30
SCALE = HD ** -0.5 * 1.4426950408889634
KCUT = 5
QCUT = 4
OWN_KEYS = (256, 384, 640, 768)
F32, BF = jnp.float32, jnp.bfloat16


def body(freq_ref, x, wq_hbm, wk_hbm, wv_hbm, wo_hbm, y_ref,
         wq, wk, wv, wo, ko, vo, qo, kb, vb, qb, ob, osend, acc, m_s, l_s,
         wksem, wvsem, wqsem, wosem, krecv, vrecv, kfs, vfs, qfs, ksend, vsend, qsend, qrecv,
         os_sem, orecv, go):
    d, a, b = lax.axis_index("dp"), lax.axis_index("cpo"), lax.axis_index("cpi")
    shard = a * NL + b
    odd = lax.rem(b, 2)
    even = odd == 0
    partner = b + 1 - 2 * odd
    far = lax.rem(b + 2, NL)
    far2 = lax.rem(partner + 2, NL)
    near0 = b - odd
    away0 = 2 - near0
    donor = (a == 3) & even
    host = (a == 2) & even
    feeds = (a < 2) | ((a == 2) & (odd == 1))

    def cut(src, dst, sem, n, c):
        r = DM // n
        return pltpu.make_async_copy(src.at[pl.ds(c * r, r)], dst.at[pl.ds(c * r, r)], sem.at[c])

    for c in range(KCUT):
        cut(wk_hbm, wk, wksem, KCUT, c).start()

    bar = pltpu.get_barrier_semaphore()

    def greet(level, other):
        pl.semaphore_signal(bar, inc=1, device_id=(d, level, other), device_id_type=MESH)

    for j in (partner, far, far2):
        greet(a, j)

    @pl.when(a > 0)
    def _():
        greet(a - 1, b)

    @pl.when(a < NL - 1)
    def _():
        greet(a + 1, b)

    @pl.when(host)
    def _():
        for j in (partner, far, far2):
            greet(3, j)

    @pl.when(a == 3)
    def _():
        greet(2, lax.rem(b + 2 - odd, NL))

    @pl.when((a == 3) & (odd == 1))
    def _():
        greet(2, b - 1)

    def one(p):
        return p.astype(jnp.int32)

    step = lax.broadcasted_iota(jnp.int32, (FINE, HALF), 0)
    fine = step.astype(F32) * freq_ref[...]
    coarse = (step * FINE + shard * TOK).astype(F32) * freq_ref[...]
    cf, sf = jnp.cos(fine)[None], jnp.sin(fine)[None]
    cc, sc = jnp.cos(coarse)[:TOK // FINE, None], jnp.sin(coarse)[:TOK // FINE, None]
    cos = (cc * cf - sc * sf).reshape(TOK, HALF)
    sin = (sc * cf + cc * sf).reshape(TOK, HALF)

    def project(w, n, copies, heads, fetch, between):
        total = None
        for c in range(n):
            copies[c].wait()
            if c in fetch:
                fetch[c]()
            r = DM // n
            at = c * r % w.shape[0]
            part = jnp.dot(x[:, c * r:(c + 1) * r], w[pl.ds(at, r)].reshape(r, heads * HD),
                           preferred_element_type=F32)
            total = part if total is None else total + part
            if c in between:
                between[c]()
        return total

    def rotate(t, h, cos, sin):
        lo, hi = t[:, h * HD:h * HD + HALF], t[:, h * HD + HALF:(h + 1) * HD]
        return (lo * cos - hi * sin).astype(BF), (hi * cos + lo * sin).astype(BF)

    def rows(s):
        return pl.ds(pl.multiple_of(s * TOK, TOK), TOK)

    def remote(src, dst, ss, rs, dev):
        return pltpu.make_async_remote_copy(src_ref=src, dst_ref=dst, send_sem=ss, recv_sem=rs,
                                            device_id=dev, device_id_type=MESH)

    def exchange(h, what):
        dev = (d, a, h)
        if what == "k":
            return remote(ko.at[h], kb.at[rows(shard)], ksend.at[h], krecv.at[shard], dev)
        if what == "v":
            return remote(vo.at[h], vb.at[rows(shard)], vsend.at[h], vrecv.at[shard], dev)
        return remote(qo.at[h], qb.at[0, b], qsend.at[h], qrecv.at[0, b], dev)

    def send(what, early=True, late=True):
        for h in (0, 2, 1, 3):
            soon = (partner == h) | (h % 2 == 0)
            if early:
                @pl.when((b != h) & soon)
                def _():
                    exchange(h, what).start()
            if late:
                @pl.when((b != h) & jnp.logical_not(soon))
                def _():
                    exchange(h, what).start()

    def hop(s, what, level):
        dev = (d, level, b)
        if what == "k":
            return remote(kb.at[rows(s)], kb.at[rows(s)], kfs.at[s], krecv.at[s], dev)
        return remote(vb.at[rows(s)], vb.at[rows(s)], vfs.at[s], vrecv.at[s], dev)

    def wait_piece(s):
        hop(s, "k", a).wait_recv()
        hop(s, "v", a).wait_recv()

    def needed(s, level):
        return s >= NL * level - 11

    def pass_on(s, whats=("k", "v")):
        @pl.when(feeds & needed(s, a + 1))
        def _():
            for what in whats:
                hop(s, what, a + 1).start()

        @pl.when(donor)
        def _():
            for what in whats:
                hop(s, what, 2).start()

    def q_down(j):
        return remote(qb.at[0, j], qb.at[1, j], qfs.at[j], qrecv.at[1, j], (d, 2, b))

    def wait_q(slot, j):
        remote(qo.at[0], qb.at[slot, j], qsend.at[0], qrecv.at[slot, j], (d, a, b)).wait_recv()

    first_user = even | (a >= 1)


    def start_v():
        for c in range(KCUT):
            cut(wv_hbm, wv, wvsem, KCUT, c).start()

    def cut_q(c):
        r = DM // QCUT
        return pltpu.make_async_copy(wq_hbm.at[pl.ds(c * r, r)], wq.at[pl.ds(c % 2 * r, r)], wqsem.at[c])

    def start_q():
        cut_q(0).start()
        cut_q(1).start()

    with jax.named_scope("k_proj"):
        k_f = project(wk, KCUT, [cut(wk_hbm, wk, wksem, KCUT, c) for c in range(KCUT)], NL, {1: start_v}, {})
    wo_copy = pltpu.make_async_copy(wo_hbm, wo, wosem)
    for h in range(NL):
        ko[h, :, :HALF], ko[h, :, HALF:] = rotate(k_f, h, cos, sin)
    kb[rows(shard), :] = ko[b]
    with jax.named_scope("barrier"):
        pl.semaphore_wait(bar, 3 + one(a > 0) + one(a < NL - 1) + 3 * one(host) + one(a == 3)
                          + one((a == 3) & (odd == 1)))
    send("k", late=False)

    def relay(who, whats, js):
        @pl.when(who)
        def _():
            for j in js:
                for what in whats:
                    hop(a * NL + j, what, a).wait_recv()
                pass_on(a * NL + j, whats)

    @pl.when(first_user)
    def _():
        pass_on(shard, ("k",))

    with jax.named_scope("v_proj"):
        v_f = project(wv, KCUT, [cut(wv_hbm, wv, wvsem, KCUT, c) for c in range(KCUT)], NL, {1: start_q},
                      {2: lambda: relay(even | (a >= 1), ("k",), (partner,))})
    for h in range(NL):
        vo[h] = v_f[:, h * HD:(h + 1) * HD].astype(BF)
    vb[rows(shard), :] = vo[b]
    send("v", late=False)
    send("k", early=False)
    send("v", early=False)

    @pl.when(first_user)
    def _():
        pass_on(shard, ("v",))

    def relay_1():
        cut_q(3).start()
        relay(even, ("v",), (partner,))
        relay(even, ("k",), (far, far2))
        relay((odd == 1) & (a >= 1), ("v",), (partner,))

    with jax.named_scope("q_proj"):
        q_f = project(wq, QCUT, [cut_q(c) for c in range(QCUT)], 2 * NL,
                      {3: wo_copy.start}, {0: cut_q(2).start, 1: relay_1})
    for h in range(2 * NL):
        qo[h // 2, h % 2, :, :HALF], qo[h // 2, h % 2, :, HALF:] = rotate(q_f, h, cos, sin)
    qb[0, b] = qo[b]
    send("q")

    def wide(t, n):
        return jnp.concatenate([t] * (n // LANES), axis=1)

    def attend(slot, i, level, key0, n, masked, first=False, last=False):
        keys = pl.ds(pl.multiple_of(key0, 64), n)
        k, v = kb[keys, :], vb[keys, :]
        scores = []
        for g in range(2):
            s = lax.dot_general(qb[slot, i, g], k, (((1,), (1,)), ((), ())), preferred_element_type=F32)
            if masked:
                gap = (lax.broadcasted_iota(jnp.int32, (TOK, n), 0) - lax.broadcasted_iota(jnp.int32, (TOK, n), 1)
                       + (level * LVL + i * TOK - key0))
                s = jnp.where((gap >= 0) & (gap < WINDOW), s, NEG)
            scores.append(s)
        for g, s in enumerate(scores):
            top = jnp.max(s, axis=-1, keepdims=True)
            if first:
                new = jnp.broadcast_to(top, (TOK, LANES))
            else:
                old = m_s[slot, i, g]
                new = jnp.maximum(old, top)
                fix = jnp.exp2((old - new) * SCALE)
            p = jnp.exp2((s - wide(new, n)) * SCALE)
            total = jnp.broadcast_to(jnp.sum(p, axis=-1, keepdims=True), (TOK, LANES))
            out = jnp.dot(p.astype(BF), v, preferred_element_type=F32)
            if not first:
                total = total + l_s[slot, i, g] * fix
                out = out + acc[slot, i, g] * wide(fix, HD)
            if last:
                osend[slot, i, :, g * HD:(g + 1) * HD] = (out * wide(1.0 / total, HD)).astype(BF)
            else:
                m_s[slot, i, g] = new
                l_s[slot, i, g] = total
                acc[slot, i, g] = out
        if last:
            give(slot, i)

    def loop(lo, hi, fn):
        def step(i, carry):
            fn(i)
            return carry
        lax.fori_loop(lo, hi, step, 0)

    def head_cols():
        return pl.ds(pl.multiple_of(b * 2 * HD, 2 * HD), 2 * HD)

    def back_to(slot, i):
        return remote(osend.at[slot, i], ob.at[:, head_cols()], os_sem.at[slot, i], orecv.at[b], (d, a + slot, i))

    def give(slot, i):
        if slot == 1:
            back_to(1, i).start()
            return

        @pl.when(b != i)
        def _():
            back_to(0, i).start()

        @pl.when(b == i)
        def _():
            ob[:, head_cols()] = osend[0, i]

    def finish(slot, i):
        for g in range(2):
            osend[slot, i, :, g * HD:(g + 1) * HD] = (acc[slot, i, g] * wide(1.0 / l_s[slot, i, g], HD)).astype(BF)
        give(slot, i)

    def turn(t):
        return lax.rem(away0 + t, NL)

    low = (a - 1) * NL

    def own_block(slot):
        with jax.named_scope("own_att"):
            for i in range(NL):
                attend(slot, i, a + slot, (a + slot) * LVL, OWN_KEYS[i], True, first=True)

    def take(s):
        wait_piece(s)
        pass_on(s)

    relay(even, ("v",), (far, far2))

    @pl.when(even & (a == 0))
    def _():
        pl.semaphore_signal(go, inc=1, device_id=(d, a, partner), device_id_type=MESH)

    @pl.when((odd == 1) & (a == 0))
    def _():
        with jax.named_scope("go_wait"):
            pl.semaphore_wait(go, 1)
        pass_on(shard)
        take(a * NL + partner)

    relay(odd == 1, ("k", "v"), (far, far2))

    @pl.when((even & (a == 1)) | ((odd == 1) & (a >= 2)))
    def _():
        with jax.named_scope("take_low"):
            for j in (b, partner, far, far2):
                take(low + j)

    @pl.when((odd == 1) & (a == 1))
    def _():
        with jax.named_scope("take_early"):
            pass

    with jax.named_scope("own_q"):
        @pl.when(jnp.logical_not(donor))
        def _():
            wait_q(0, partner)

        @pl.when(jnp.logical_not(donor | host))
        def _():
            wait_q(0, far)
            wait_q(0, far2)

    @pl.when(donor)
    def _():
        q_down(b).start()
        for j in (partner, far, far2):
            wait_q(0, j)
            q_down(j).start()

    def chip_block(slot, here):
        for i in range(0, NL, 2):
            @pl.when((near0 == i) == here)
            def _():
                for j in (i, i + 1):
                    attend(slot, j, a + slot, (a + slot) * LVL, OWN_KEYS[j], True, first=True)

    def pair(start, fn):
        loop(0, 2, lambda t: fn(start + t))

    @pl.when(host)
    def _():
        def low_0(start):
            pair(start, lambda i: attend(0, i, a, (a - 1) * LVL, LVL, False))

        def low_1(start):
            pair(start, lambda i: attend(1, i, 3, LVL, LVL, True))

        def top_1(here, start):
            with jax.named_scope("hq1"):
                for j in ((b, partner) if here else (far, far2)):
                    wait_q(1, j)
            with jax.named_scope("top_1"):
                chip_block(1, here)
                pair(start, lambda i: attend(1, i, 3, 2 * LVL, LVL, False))

        with jax.named_scope("job0"):
            chip_block(0, True)
        with jax.named_scope("take1"):
            for j in (b, partner, far, far2):
                take(low + j)
        low_0(near0)
        with jax.named_scope("hq0"):
            wait_q(0, far)
            wait_q(0, far2)
        with jax.named_scope("job0"):
            chip_block(0, False)
            low_0(away0)
        with jax.named_scope("hkv1"):
            for j in range(NL):
                wait_piece(3 * NL + j)
        top_1(True, near0)
        low_1(near0)

        @pl.when(near0 == 2)
        def _():
            finish(1, NL - 1)

        top_1(False, away0)
        low_1(away0)

        @pl.when(near0 == 0)
        def _():
            finish(1, NL - 1)

        with jax.named_scope("take2"):
            for j in (b, partner, far, far2):
                take(j)
        with jax.named_scope("host_last"):
            loop(0, NL - 1, lambda i: attend(1, i, 3, 256, 512, True, last=True))
        with jax.named_scope("att2"):
            loop(0, NL, lambda t: attend(0, turn(t), a, 0, LVL, True, last=True))

    @pl.when(jnp.logical_not(donor | host))
    def _():
        own_block(0)

        @pl.when((a == 2) & (odd == 1))
        def _():
            with jax.named_scope("take_early"):
                pass

        @pl.when(a == 0)
        def _():
            loop(0, NL, lambda t: finish(0, turn(t)))

        @pl.when(a > 0)
        def _():
            @pl.when((a == 1) & (odd == 1))
            def _():
                with jax.named_scope("go_wait"):
                    pl.semaphore_wait(go, 1)
                with jax.named_scope("take_low"):
                    for j in (3, 2, 1, 0):
                        take(low + j)

            @pl.when(a == 1)
            def _():
                loop(0, NL, lambda t: attend(0, turn(t), a, 0, LVL, False, last=True))

                @pl.when(even)
                def _():
                    for j in (shard, NL + partner, NL + far, NL + far2, b, partner):
                        for what in ("k", "v"):
                            hop(j, what, 2).wait_send()
                    pl.semaphore_signal(go, inc=1, device_id=(d, a, partner), device_id_type=MESH)

            @pl.when(a > 1)
            def _():
                with jax.named_scope("att1"):
                    loop(0, NL, lambda i: attend(0, i, a, (a - 1) * LVL, LVL, False))

        @pl.when((a >= 2) & (odd == 1))
        def _():
            lvl2 = (a - 2) * NL
            with jax.named_scope("take2a"):
                take(lvl2 + 3)
                take(lvl2 + 2)
            with jax.named_scope("att2a"):
                loop(0, 2, lambda i: attend(0, i, a, lvl2 * TOK + 2 * TOK, 2 * TOK, False))
            with jax.named_scope("take2b"):
                take(lvl2 + 1)
            with jax.named_scope("att2b"):
                loop(2, NL, lambda i: attend(0, i, a, lvl2 * TOK + 2 * TOK, 2 * TOK, False))
            with jax.named_scope("take2c"):
                take(lvl2)

        @pl.when((a == 2) & (odd == 1))
        def _():
            with jax.named_scope("att2c"):
                loop(0, NL, lambda t: attend(0, turn(t), a, 0, 2 * TOK, True, last=True))

        @pl.when((a == 3) & (odd == 1))
        def _():
            with jax.named_scope("att2c"):
                loop(0, NL, lambda i: attend(0, i, a, LVL, 2 * TOK, True))
            finish(0, NL - 1)
            with jax.named_scope("take3"):
                wait_piece(3)
                wait_piece(2)
            with jax.named_scope("att3"):
                attend(0, 2, a, 2 * TOK, 2 * TOK, True, last=True)
                attend(0, 1, a, 2 * TOK, 2 * TOK, True, last=True)
                attend(0, 0, a, 2 * TOK, 2 * TOK, True)
            with jax.named_scope("take3b"):
                wait_piece(1)
            with jax.named_scope("att3b"):
                attend(0, 0, a, 256, 128, True, last=True)

    def take_o(h):
        @pl.when((b != h) | ((a == 3) & (h % 2 == 0)))
        def _():
            remote(osend.at[0, 0], ob.at[:, pl.ds(h * 2 * HD, 2 * HD)], os_sem.at[0, 0], orecv.at[h], (d, a, b)).wait_recv()

    def project_o(h, cols):
        return jnp.dot(ob[:, h * 2 * HD:(h + 1) * 2 * HD], wo[pl.ds(h * 2 * HD, 2 * HD), cols],
                       preferred_element_type=F32)

    tiles = [(pl.ds(t * HD, HD), (t // (2 * NL), t // 2 % NL, t % 2)) for t in range(DM // HD)]
    wo_copy.wait()

    def add_head(h, here, start=False, last=False):
        @pl.when((b // 2 == h // 2) == here)
        def _():
            take_o(h)
            for cols, at in tiles:
                part = project_o(h, cols)
                if not start:
                    part = part + acc[at]
                if last:
                    y_ref[:, cols] = part.astype(BF)
                else:
                    acc[at] = part

    with jax.named_scope("o_near"):
        for h in (1, 3):
            add_head(h, True, start=True)
        for h in (0, 2):
            add_head(h, True)

    for h in range(NL):
        @pl.when(b != h)
        def _():
            for what in ("k", "v", "q"):
                exchange(h, what).wait_send()

        @pl.when(donor)
        def _():
            q_down(h).wait_send()
            for what in ("k", "v"):
                hop(3 * NL + h, what, 2).wait_send()

    for s in range(12):
        waited = even & (a == 1) & ((s >= NL) | (s // 2 == b // 2))

        @pl.when(feeds & (s < NL * (a + 1)) & needed(s, a + 1) & jnp.logical_not(waited))
        def _():
            for what in ("k", "v"):
                hop(s, what, a + 1).wait_send()

    with jax.named_scope("o_far"):
        for h in (1, 3):
            add_head(h, False)
        for h in (0, 2):
            add_head(h, False, last=True)

    for h in range(NL):
        @pl.when((b != h) & jnp.logical_not(donor))
        def _():
            back_to(0, h).wait_send()

        @pl.when(host)
        def _():
            back_to(1, h).wait_send()


def solution(mesh):
    def local_fn(hidden, w_q, w_k, w_v, w_o):
        freq = (ROPE_BASE ** (-jnp.arange(HALF, dtype=F32) * 2.0 / HD)).reshape(1, HALF)
        hbm = pl.BlockSpec(memory_space=pltpu.HBM)
        dma = pltpu.SemaphoreType.DMA
        return pl.pallas_call(
            body,
            out_shape=jax.ShapeDtypeStruct((TOK, DM), BF),
            in_specs=[pl.BlockSpec(memory_space=pltpu.VMEM)] * 2 + [hbm] * 4,
            out_specs=pl.BlockSpec(memory_space=pltpu.VMEM),
            scratch_shapes=[
                pltpu.VMEM((DM // 2, 2 * NL, HD), BF), pltpu.VMEM((DM, NL, HD), BF),
                pltpu.VMEM((DM, NL, HD), BF), pltpu.VMEM((2 * NL * HD, DM), BF),
                pltpu.VMEM((NL, TOK, HD), BF), pltpu.VMEM((NL, TOK, HD), BF), pltpu.VMEM((NL, 2, TOK, HD), BF),
                pltpu.VMEM((16 * TOK, HD), BF), pltpu.VMEM((16 * TOK, HD), BF),
                pltpu.VMEM((2, NL, 2, TOK, HD), BF), pltpu.VMEM((TOK, 2 * NL * HD), BF),
                pltpu.VMEM((2, NL, TOK, 2 * HD), BF), pltpu.VMEM((2, NL, 2, TOK, HD), F32),
                pltpu.VMEM((2, NL, 2, TOK, LANES), F32), pltpu.VMEM((2, NL, 2, TOK, LANES), F32),
                dma((KCUT,)), dma((KCUT,)), dma((QCUT,)), dma(()),
                dma((16,)), dma((16,)), dma((16,)), dma((16,)), dma((NL,)),
                dma((NL,)), dma((NL,)), dma((NL,)), dma((2, NL)), dma((2, NL)), dma((NL,)),
                pltpu.SemaphoreType.REGULAR,
            ],
            compiler_params=pltpu.CompilerParams(collective_id=0, has_side_effects=True,
                                                 vmem_limit_bytes=51 * 2 ** 20),
        )(freq, hidden, w_q, w_k, w_v, w_o.reshape(2 * NL * HD, DM))

    return jax.shard_map(local_fn, mesh=mesh,
                         in_specs=(P(("dp", "cpo", "cpi"), None), P(), P(), P(), P()),
                         out_specs=P(("dp", "cpo", "cpi"), None), check_vma=False)
```
